32 devices in a mesh: seq: 16 (over z, y, core), head: 2 (over x).
Axes of the slice: x: 2, y: 2, z: 4, core: 2. Of those that a mesh axis runs over, the one named last changes fastest.
Arguments:
- tokens: bfloat16 [8192, 1024], P('seq'), may hold values from -24 to 24
- norm_attn: float32 [1024], replicated, may hold values from 0.5 to 1.5
- self_qkv: bfloat16 [3, 1024, 1024], P(None, None, 'head'), may hold values from -4 to 4
- self_out: bfloat16 [1024, 1024], P('head'), may hold values from -0.1875 to 0.1875
- norm_ffn: float32 [1024], replicated, may hold values from 0.5 to 1.5
- ffn_in: bfloat16 [2, 1024, 2816], P(None, None, 'head'), may hold values from -0.1875 to 0.1875
- ffn_out: bfloat16 [2816, 1024], P('head'), may hold values from -0.109375 to 0.109375
- norm_final: float32 [1024], replicated, may hold values from 0.5 to 1.5
- pad_lengths: int32 [16], replicated, may hold values from 64 to 512
- targets: bfloat16 [512, 1024], replicated, may hold values from -8 to 8
- target_lengths: int32 [4], replicated, may hold values from 32 to 128
- norm_cross: float32 [1024], replicated, may hold values from 0.1 to 1.9
- cross_query: bfloat16 [1024, 1024], P(None, 'head'), may hold values from -4 to 4
- cross_kv: bfloat16 [2, 1024, 1024], P(None, None, 'head'), may hold values from -4 to 4
- cross_out: bfloat16 [1024, 1024], P('head'), may hold values from -4 to 4
Outputs:
- encoded: bfloat16 [8192, 1024], P('seq')
- decoded: bfloat16 [512, 1024], replicated
The draws below stay inside these ranges and needn't reach their ends.
All inputs are finite; a program needn't handle non-finite values.
Results may differ from the reference program's by a relative error of at most 0.033.
Values may be sent and summed in bfloat16 or wider, within the bound.
A program may use at most 128 MiB of HBM per device.

```python
import math
import jax
import jax.numpy as jnp
from jax import lax

D = 1024
HEADS = 16
HD = 64
FF = 2816
TOK_DEV = 512
TGT_SEQS = 4
TGT_LEN = 128
TOKENS = 8192
TGT = 512
BLOCKS = 16


def plant_strength():
    return math.sqrt(300.0 * math.sqrt(HD) / D)


def plant_vectors(seed_key):
    base_key = jax.random.fold_in(seed_key, 9001)
    direction = jax.random.normal(jax.random.fold_in(base_key, 1), (D,), jnp.float32)
    direction = direction / jnp.sqrt(jnp.sum(direction * direction))
    target_dir = jax.random.normal(jax.random.fold_in(base_key, 2), (HEADS, HD), jnp.float32)
    target_dir = target_dir / jnp.sqrt(jnp.sum(target_dir * target_dir, axis=1, keepdims=True))
    return (direction, target_dir.reshape(HEADS * HD))


def projection(seed_key, salt, planted):
    matrix = jax.random.normal(jax.random.fold_in(seed_key, salt), (planted.shape[0], D, HEADS * HD), jnp.float32) * D ** (-0.5)
    matrix = jnp.clip(matrix, -3.5, 3.5)
    direction, target_dir = plant_vectors(seed_key)
    bump = plant_strength() * jnp.outer(direction, target_dir)
    matrix = matrix + planted[:, None, None] * bump[None, :, :]
    return matrix


def draw_self_qkv(seed_key, part_index):
    return projection(seed_key, 11, jnp.array([1.0, 1.0, 0.0], jnp.float32)).astype(jnp.bfloat16)


def draw_cross_query(seed_key, part_index):
    return projection(seed_key, 12, jnp.array([1.0], jnp.float32))[0].astype(jnp.bfloat16)


def draw_cross_kv(seed_key, part_index):
    return projection(seed_key, 13, jnp.array([1.0, 0.0], jnp.float32)).astype(jnp.bfloat16)


def draw_tokens(seed_key, part_index):
    rows_drawn = jnp.clip(jax.random.normal(jax.random.fold_in(seed_key, 21), (TOKENS, D), jnp.float32), -6.0, 6.0)
    direction, target_dir = plant_vectors(seed_key)
    row_ids = jnp.arange(TOKENS, dtype=jnp.int32)[:, None]
    picked = (jax.random.randint(jax.random.fold_in(seed_key, 22), (TOKENS, 1), 0, 32) == 0) | (row_ids % (4 * TOK_DEV) == 0)
    planted_rows = 128.0 * direction[None, :] + 96.0 / math.sqrt(D) * rows_drawn
    rows_drawn = jnp.where(picked, planted_rows, rows_drawn)
    return jnp.clip(rows_drawn, -24.0, 24.0).astype(jnp.bfloat16)


def draw_targets(seed_key, part_index):
    rows_drawn = jnp.clip(jax.random.normal(jax.random.fold_in(seed_key, 31), (TGT, D), jnp.float32), -6.0, 6.0)
    direction, target_dir = plant_vectors(seed_key)
    row_ids = jnp.arange(TGT, dtype=jnp.int32)[:, None]
    picked = (jax.random.randint(jax.random.fold_in(seed_key, 32), (TGT, 1), 0, 16) == 0) | (row_ids == 0)
    rows_drawn = jnp.where(picked, 32.0 * direction[None, :], rows_drawn)
    return jnp.clip(rows_drawn, -8.0, 8.0).astype(jnp.bfloat16)


def set_ends(drawn, own_key, smallest, top_value):
    longest = drawn.shape.index(max(drawn.shape))
    spots = []
    for shift in (0, 1):
        where = [jax.random.randint(jax.random.fold_in(own_key, axis), (), 0, length) for axis, length in enumerate(drawn.shape)]
        where[longest] = (where[longest] + shift) % drawn.shape[longest]
        spots.append(tuple(where))
    return drawn.at[spots[0]].set(smallest).at[spots[1]].set(top_value)


def levels(own_key, shape, shards, least, largest):
    def one(axis_at, shards_of):
        steps = jax.random.uniform(jax.random.fold_in(jax.random.fold_in(own_key, 6), axis_at), (shards_of,), jnp.float32, least / len(shards), largest / len(shards))
        return jnp.repeat(jnp.exp(steps), shape[axis_at] // shards_of).reshape((-1,) + (1,) * (len(shape) - axis_at - 1))

    factor_of = one(*shards[0])
    for cut in shards[1:]:
        factor_of = factor_of * one(*cut)
    return factor_of


def scatter_about(stream_key, extent, scale, reach, cuts=(), held_as=jnp.bfloat16):
    loudness = levels(stream_key, extent, cuts, -0.22, 0.18) if cuts else 1.0
    values = jax.random.normal(stream_key, extent, jnp.float32) * scale * loudness
    return jnp.minimum(jnp.maximum(values, -reach), reach).astype(held_as)


def setup_inputs(seed: int = 0) -> dict:
    key_of = jax.random.split(jax.random.key(seed), 16)
    tokens = draw_tokens(jax.random.fold_in(key_of[15], 71), 0)
    norm_attn = jnp.clip(1.0 + 0.1 * jax.random.normal(key_of[1], (D,), jnp.float32), 0.5, 1.5)
    self_qkv = draw_self_qkv(jax.random.fold_in(key_of[15], 71), 0)
    self_out = scatter_about(key_of[3], (HEADS * HD, D), (HEADS * HD) ** -0.5, 0.1875, ((0, 2),))
    norm_ffn = jnp.clip(1.0 + 0.1 * jax.random.normal(key_of[4], (D,), jnp.float32), 0.5, 1.5)
    ffn_in = scatter_about(key_of[5], (2, D, FF), D ** -0.5, 0.1875, ((2, 2),))
    ffn_out = scatter_about(key_of[6], (FF, D), FF ** -0.5, 0.109375, ((0, 2),))
    norm_final = jnp.clip(1.0 + 0.1 * jax.random.normal(key_of[7], (D,), jnp.float32), 0.5, 1.5)
    pad_lengths = set_ends(jax.random.randint(key_of[8], (BLOCKS,), TOK_DEV // 8, TOK_DEV + 1), jax.random.fold_in(key_of[8], 1), TOK_DEV // 8, TOK_DEV).astype(jnp.int32)
    targets = draw_targets(jax.random.fold_in(key_of[15], 71), 0)
    target_lengths = set_ends(jax.random.randint(key_of[10], (TGT_SEQS,), TGT_LEN // 4, TGT_LEN + 1), jax.random.fold_in(key_of[10], 1), TGT_LEN // 4, TGT_LEN).astype(jnp.int32)
    norm_cross = jnp.clip(1.0 + 0.18 * jax.random.normal(key_of[11], (D,), jnp.float32), 0.1, 1.9)
    cross_query = draw_cross_query(jax.random.fold_in(key_of[15], 71), 0)
    cross_kv = draw_cross_kv(jax.random.fold_in(key_of[15], 71), 0)
    cross_out = scatter_about(key_of[14], (HEADS * HD, D), (8.0 / (HEADS * HD) ** 0.5), 4.0, ((0, 2),))
    return {"tokens": tokens, "norm_attn": norm_attn, "self_qkv": self_qkv, "self_out": self_out, "norm_ffn": norm_ffn, "ffn_in": ffn_in, "ffn_out": ffn_out, "norm_final": norm_final, "pad_lengths": pad_lengths, "targets": targets, "target_lengths": target_lengths, "norm_cross": norm_cross, "cross_query": cross_query, "cross_kv": cross_kv, "cross_out": cross_out}


epsilon = 1e-06
masked_score = -1e+30

def rms_norm(values, gain_vector):
    widened = values.astype(jnp.float32)
    return widened * lax.rsqrt(lax.optimization_barrier(jnp.mean(widened * widened, axis=-1, keepdims=True)) + epsilon) * gain_vector.astype(jnp.float32)

def attend(queries, keys, values, live_keys):
    query_count = queries.shape[0]
    key_count = keys.shape[0]
    query_heads = queries.reshape(query_count, HEADS, HD).transpose(1, 0, 2)
    key_heads = keys.reshape(key_count, HEADS, HD).transpose(1, 0, 2)
    value_heads = values.reshape(key_count, HEADS, HD).transpose(1, 0, 2)
    block_rows = math.gcd(query_count, 1024)
    scaling = HD ** (-0.5)

    def one_head(head_parts):
        head_queries, head_keys, head_values = head_parts
        blocked = head_queries.reshape(query_count // block_rows, block_rows, HD)

        def one_block(block_queries):
            scores = jnp.dot(block_queries, head_keys.T, preferred_element_type=jnp.float32) * scaling
            scores = jnp.where(live_keys[None, :], scores, masked_score)
            row_max = lax.optimization_barrier(jnp.max(scores, axis=1, keepdims=True))
            weights = jnp.where(live_keys[None, :], jnp.exp(scores - row_max), 0.0)
            weight_sum = lax.optimization_barrier(jnp.sum(weights, axis=1, keepdims=True))
            mixed_rows = jnp.dot(weights.astype(jnp.bfloat16), head_values, preferred_element_type=jnp.float32)
            return mixed_rows / weight_sum
        return lax.map(one_block, blocked).reshape(query_count, HD)
    per_head = lax.map(one_head, (query_heads, key_heads, value_heads))
    return per_head.transpose(1, 0, 2).reshape(query_count, HEADS * HD).astype(jnp.bfloat16)

def reference(tokens, norm_attn, self_qkv, self_out, norm_ffn, ffn_in, ffn_out, norm_final, pad_lengths, targets, target_lengths, norm_cross, cross_query, cross_kv, cross_out):
    normed = rms_norm(tokens, norm_attn).astype(jnp.bfloat16)
    queries = jnp.dot(normed, self_qkv[0], preferred_element_type=jnp.float32).astype(jnp.bfloat16)
    keys = jnp.dot(normed, self_qkv[1], preferred_element_type=jnp.float32).astype(jnp.bfloat16)
    values = jnp.dot(normed, self_qkv[2], preferred_element_type=jnp.float32).astype(jnp.bfloat16)
    positions = jnp.arange(TOKENS, dtype=jnp.int32)
    live = positions % TOK_DEV < jnp.repeat(pad_lengths, TOK_DEV, total_repeat_length=TOKENS)
    context = attend(queries, keys, values, live)
    hidden_in = tokens.astype(jnp.float32) + jnp.dot(context, self_out, preferred_element_type=jnp.float32)
    ffn_normed = rms_norm(hidden_in, norm_ffn).astype(jnp.bfloat16)
    gate_proj = jnp.dot(ffn_normed, ffn_in[0], preferred_element_type=jnp.float32)
    up_proj = jnp.dot(ffn_normed, ffn_in[1], preferred_element_type=jnp.float32)
    activated = (jax.nn.gelu(gate_proj, approximate=True) * up_proj).astype(jnp.bfloat16)
    final_in = hidden_in + jnp.dot(activated, ffn_out, preferred_element_type=jnp.float32)
    encoded = rms_norm(final_in, norm_final).astype(jnp.bfloat16)
    cross_normed = rms_norm(targets, norm_cross).astype(jnp.bfloat16)
    cross_queries = jnp.dot(cross_normed, cross_query, preferred_element_type=jnp.float32).astype(jnp.bfloat16)
    cross_keys = jnp.dot(encoded, cross_kv[0], preferred_element_type=jnp.float32).astype(jnp.bfloat16)
    cross_values = jnp.dot(encoded, cross_kv[1], preferred_element_type=jnp.float32).astype(jnp.bfloat16)
    cross_context = attend(cross_queries, cross_keys, cross_values, live)
    slots = jnp.arange(TGT, dtype=jnp.int32)
    target_live = slots % TGT_LEN < jnp.repeat(target_lengths, TGT_LEN, total_repeat_length=TGT)
    cross_total = jnp.dot(cross_context, cross_out, preferred_element_type=jnp.float32)
    decoded = (targets.astype(jnp.float32) + jnp.where(target_live[:, None], cross_total, 0.0)).astype(jnp.bfloat16)
    return (encoded, decoded)
```

```python
import functools
import math

import jax
import jax.numpy as jnp
from jax import lax
from jax.experimental import pallas as pl
from jax.experimental.pallas import tpu as pltpu
from jax.sharding import PartitionSpec as P

HD = 64
TGT_LEN = 128

epsilon = 1e-06
masked_score = -1e30
MESH = pl.DeviceIdType.MESH


def flip(index, other, count):
    result = 0
    weight = 1
    while weight < count:
        digit = other // weight if isinstance(other, int) else lax.div(other, weight)
        result = result + lax.rem(lax.div(index, weight) + digit, 2) * weight
        weight *= 2
    return result


def rows_at(start, size, align):
    return pl.ds(pl.multiple_of(start, align), size)


def greet_all(ring, sides):
    me = lax.axis_index("seq")
    here = lax.axis_index("head")
    barrier = pltpu.get_barrier_semaphore()

    def greet(i, carry):
        pl.semaphore_signal(
            barrier, inc=1, device_id={"seq": lax.rem(me + i, ring)}, device_id_type=MESH
        )
        return carry

    lax.fori_loop(1, ring, greet, 0)
    for k in range(1, sides):
        pl.semaphore_signal(
            barrier, inc=1, device_id={"head": lax.rem(here + k, sides)}, device_id_type=MESH
        )
    pl.semaphore_wait(barrier, ring - 1 + sides - 1)


def seq_copy(to, source, target, send_sem, recv_sem):
    return pltpu.make_async_remote_copy(
        src_ref=source,
        dst_ref=target,
        send_sem=send_sem,
        recv_sem=recv_sem,
        device_id={"seq": to},
        device_id_type=MESH,
    )


def side_copy(sides, k, source, target, send_sem, recv_sem):
    here = lax.axis_index("head")
    return pltpu.make_async_remote_copy(
        src_ref=source,
        dst_ref=target,
        send_sem=send_sem,
        recv_sem=recv_sem,
        device_id={"head": lax.rem(here + k, sides)},
        device_id_type=MESH,
    )


def norm_rows(values, gain):
    scale = lax.rsqrt(jnp.mean(values * values, axis=-1, keepdims=True) + epsilon)
    return values * scale * gain


def scatter_kernel(
    ring, share, sides, tokens_hbm, gain_hbm, qkv_hbm, out_hbm, targets_hbm, g_cross_hbm, w_cross_hbm,
    q_out, kv_out, out_all, cross_q,
    tokens, gain, qkv, targets, g_cross, w_cross, normed, q_in, kv_in,
    qs, qr, ks, kr, fs, fr, ls, os, ws, wr,
):
    me = lax.axis_index("seq")
    here = lax.axis_index("head")
    half = targets.shape[0]
    part = kv_in.shape[1]
    heads = ring // share
    slot = lax.rem(me, share)
    mine = rows_at(slot * part, part, part)
    loads = [
        pltpu.make_async_copy(source, target, ls.at[n])
        for n, (source, target) in enumerate(
            [
                (tokens_hbm, tokens),
                (gain_hbm, gain),
                (qkv_hbm.at[1], qkv.at[1]),
                (qkv_hbm.at[2], qkv.at[2]),
                (qkv_hbm.at[0], qkv.at[0]),
                (targets_hbm.at[rows_at(lax.rem(me, 2) * half, half, half)], targets),
                (g_cross_hbm, g_cross),
                (w_cross_hbm, w_cross),
            ]
        )
    ]
    for load in loads:
        load.start()
    greet_all(ring, sides)
    for k in range(1, sides):
        side_copy(sides, k, out_hbm, out_all.at[here], ws.at[k], wr.at[k]).start()

    def q_copy(i):
        to = flip(me, i, ring)
        return seq_copy(to, q_in.at[to], q_out.at[me], qs.at[i], qr.at[i])

    def kv_copy(i):
        to = flip(me, i, ring)
        rows = rows_at(lax.rem(to, share) * part, part, part)
        return seq_copy(to, kv_in.at[to], kv_out.at[me, rows], ks.at[i], kr.at[i])

    def forward(i, k):
        block = kv_out.at[flip(me, i, ring), mine]
        to = me - slot + lax.rem(slot + k, share)
        return seq_copy(to, block, block, fs.at[i, k], fr.at[i, k])

    def arrived(i, k):
        giver = me - slot + lax.rem(slot - k + share, share)
        rows = rows_at(lax.rem(giver, share) * part, part, part)
        block = kv_out.at[flip(giver, i, ring), rows]
        return seq_copy(giver, block, block, fs.at[i, k], fr.at[i, k])

    loads[0].wait()
    loads[1].wait()
    normed[...] = norm_rows(tokens[...].astype(jnp.float32), gain[...]).astype(jnp.bfloat16)
    loads[2].wait()
    loads[3].wait()
    keys = jnp.dot(normed[...], qkv[1], preferred_element_type=jnp.float32).astype(jnp.bfloat16)
    values = jnp.dot(normed[...], qkv[2], preferred_element_type=jnp.float32).astype(jnp.bfloat16)
    for h in range(heads):
        cut = slice(h * HD, (h + 1) * HD)
        both = jnp.concatenate([keys[:, cut], values[:, cut]], axis=1)
        for s in range(share):
            kv_in[h * share + s] = both[s * part : (s + 1) * part, :]

    def send_kv(i, carry):
        kv_copy(ring - i).start()
        return carry

    lax.fori_loop(1, ring, send_kv, 0)
    own_kv = pltpu.make_async_copy(kv_in.at[me], kv_out.at[me, mine], os.at[1])
    own_kv.start()
    loads[4].wait()
    queries = lax.dot_general(
        qkv[0], normed[...], (((0,), (1,)), ((), ())), preferred_element_type=jnp.float32
    ).astype(jnp.bfloat16) * jnp.bfloat16(HD ** (-0.5))
    for h in range(heads):
        for s in range(share):
            q_in[h * share + s] = queries[h * HD : (h + 1) * HD, s * part : (s + 1) * part]

    def send_q(i, carry):
        q_copy(ring - i).start()
        return carry

    lax.fori_loop(1, ring, send_q, 0)
    own_q = pltpu.make_async_copy(q_in.at[me], q_out.at[me], os.at[0])
    own_q.start()
    own_kv.wait()
    for k in range(1, share):
        forward(0, k).start()
    for load in loads[5:]:
        load.wait()
    cross_normed = norm_rows(targets[...].astype(jnp.float32), g_cross[...]).astype(jnp.bfloat16)
    cross_q[...] = jnp.dot(
        cross_normed, w_cross[...], preferred_element_type=jnp.float32
    ).astype(jnp.bfloat16) * jnp.bfloat16(HD ** (-0.5))

    def relay(i, carry):
        origin = flip(me, i, ring)
        seq_copy(origin, kv_in.at[0], kv_out.at[origin, mine], ks.at[i], kr.at[i]).wait_recv()
        for k in range(1, share):
            forward(i, k).start()
        return carry

    lax.fori_loop(1, ring, relay, 0)

    def finish(i, carry):
        origin = flip(me, i, ring)
        seq_copy(origin, q_in.at[0], q_out.at[origin], qs.at[i], qr.at[i]).wait_recv()
        q_copy(i).wait_send()
        kv_copy(i).wait_send()
        return carry

    lax.fori_loop(1, ring, finish, 0)

    def drain(i, carry):
        for k in range(1, share):
            arrived(i, k).wait_recv()
            forward(i, k).wait_send()
        return carry

    lax.fori_loop(0, ring, drain, 0)
    for k in range(1, sides):
        origin = lax.rem(here - k + sides, sides)
        side_copy(sides, k, out_hbm, out_all.at[origin], ws.at[k], wr.at[k]).wait()
    own_q.wait()


def scatter_heads(ring, share, sides, tokens, gain, qkv, w_out, targets, g_cross, w_cross):
    rows, width = tokens.shape
    heads = ring // share
    part = rows // share
    half = targets.shape[0] // 2
    bf16 = jnp.bfloat16
    vmem = pl.BlockSpec(memory_space=pltpu.VMEM)
    hbm = pl.BlockSpec(memory_space=pltpu.HBM)
    dma = pltpu.SemaphoreType.DMA
    return pl.pallas_call(
        functools.partial(scatter_kernel, ring, share, sides),
        out_shape=(
            jax.ShapeDtypeStruct((ring, HD, part), bf16),
            jax.ShapeDtypeStruct((ring, rows, 2 * HD), bf16),
            jax.ShapeDtypeStruct((sides,) + w_out.shape, bf16),
            jax.ShapeDtypeStruct((half, w_cross.shape[1]), bf16),
        ),
        in_specs=[hbm] * 7,
        out_specs=(vmem, vmem, hbm, vmem),
        scratch_shapes=[
            pltpu.VMEM((rows, width), bf16),
            pltpu.VMEM((1, width), jnp.float32),
            pltpu.VMEM(qkv.shape, bf16),
            pltpu.VMEM((half, width), bf16),
            pltpu.VMEM((1, width), jnp.float32),
            pltpu.VMEM(w_cross.shape, bf16),
            pltpu.VMEM((rows, width), bf16),
            pltpu.VMEM((heads * share, HD, part), bf16),
            pltpu.VMEM((heads * share, part, 2 * HD), bf16),
            dma((ring,)),
            dma((ring,)),
            dma((ring,)),
            dma((ring,)),
            dma((ring, share)),
            dma((ring, share)),
            dma((8,)),
            dma((2,)),
            dma((sides,)),
            dma((sides,)),
        ],
        compiler_params=pltpu.CompilerParams(
            collective_id=0, has_side_effects=True, vmem_limit_bytes=40 * 1024 * 1024
        ),
        name="scatter_heads",
    )(tokens, gain[None, :], qkv, w_out, targets, g_cross[None, :], w_cross)


def block_kernel(
    ring, share, sides, x_in, pad_lengths, target_lengths, tokens_hbm, g_ffn_hbm, g_final_hbm,
    w_own_hbm, w_all_hbm, up_hbm, down_hbm, kv_hbm, cross_q, w_cross_hbm, targets_hbm,
    encoded, decoded,
    tokens, g_ffn, g_final, w_out, context, hidden, normed, parts, up, down, w_kv, w_cross, mine,
    cross_k, cross_v, mixed, stats, got, partial, incoming,
    ls, ss, rs, fs, fr, ps, pr, cs, cr, ms, mr, xs, xr, zs, zr, ys, yr, ws, wr, hs, hr,
):
    me = lax.axis_index("seq")
    here = lax.axis_index("head")
    heads = ring // share
    rows, width = tokens.shape
    slab = mine.shape[0]
    core = lax.rem(me, 2)
    mate = flip(me, 1, ring)

    def slab_start(owner):
        return (lax.rem(owner, 2) * (ring // 2) + lax.div(owner, 2)) * slab

    loads = [
        pltpu.make_async_copy(source, target, ls.at[n])
        for n, (source, target) in enumerate(
            [
                (tokens_hbm, tokens),
                (g_ffn_hbm, g_ffn),
                (w_own_hbm, w_out.at[here]),
                (up_hbm, up),
                (down_hbm, down),
                (g_final_hbm, g_final),
                (kv_hbm, w_kv),
                (w_cross_hbm, w_cross),
                (targets_hbm.at[rows_at(slab_start(me), slab, slab)], mine),
            ]
            + [
                (w_all_hbm.at[lax.rem(here + k, sides)], w_out.at[lax.rem(here + k, sides)])
                for k in range(1, sides)
            ]
        )
    ]
    for load in loads:
        load.start()

    def place(side, origin):
        return context.at[lax.rem(origin, share), side * heads + lax.div(origin, share)]

    own = pltpu.make_async_copy(x_in.at[me], place(here, me), ls.at[len(loads)])
    own.start()
    greet_all(ring, sides)

    def outgoing(i):
        to = flip(me, i, ring)
        return seq_copy(to, x_in.at[to], place(here, me), ss.at[i], rs.at[i])

    def relay(i, k):
        block = place(here, flip(me, i, ring))
        return side_copy(sides, k, block, block, fs.at[i, k], fr.at[i, k])

    def send(i, carry):
        outgoing(ring - i).start()
        return carry

    lax.fori_loop(1, ring, send, 0)
    own.wait()
    for k in range(1, sides):
        relay(0, k).start()

    def pass_on(i, carry):
        origin = flip(me, i, ring)
        seq_copy(origin, x_in.at[0], place(here, origin), ss.at[i], rs.at[i]).wait_recv()
        for k in range(1, sides):
            relay(i, k).start()
        return carry

    lax.fori_loop(1, ring, pass_on, 0)

    def sent(i, carry):
        outgoing(i).wait_send()
        return carry

    lax.fori_loop(1, ring, sent, 0)

    def drain(i, carry):
        for k in range(1, sides):
            relay(i, k).wait_send()
            block = place(lax.rem(here - k + sides, sides), flip(me, i, ring))
            side_copy(sides, k, block, block, fs.at[i, k], fr.at[i, k]).wait_recv()
        return carry

    lax.fori_loop(0, ring, drain, 0)
    for load in loads[:3] + loads[9:]:
        load.wait()
    part = rows // share

    def project(c, carry):
        at = rows_at(c * part, part, part)
        flat = context[c].reshape(sides * heads * HD, part)
        total = tokens[at, :].astype(jnp.float32) + lax.dot_general(
            flat, w_out[...].reshape(sides * heads * HD, width), (((0,), (0,)), ((), ())),
            preferred_element_type=jnp.float32,
        )
        hidden[at, :] = total
        normed[at, :] = norm_rows(total, g_ffn[...]).astype(jnp.bfloat16)
        return carry

    lax.fori_loop(0, share, project, 0)
    for load in loads[3:6]:
        load.wait()
    chunk = math.gcd(rows, 128)
    chunks = rows // chunk

    def span(c):
        return rows_at(c * chunk, chunk, chunk)

    def swap(c, k, side):
        return side_copy(
            sides, k, parts.at[side, span(c)], parts.at[side, span(c)], ps.at[c, k], pr.at[c, k]
        )

    def feed(c, carry):
        x = normed[span(c), :]
        gate = jnp.dot(x, up[0], preferred_element_type=jnp.float32)
        lift = jnp.dot(x, up[1], preferred_element_type=jnp.float32)
        active = (jax.nn.gelu(gate, approximate=True) * lift).astype(jnp.bfloat16)
        parts[here, span(c), :] = jnp.dot(
            active, down[...], preferred_element_type=jnp.float32
        ).astype(jnp.bfloat16)
        for k in range(1, sides):
            swap(c, k, here).start()
        return carry

    lax.fori_loop(0, chunks, feed, 0)
    for load in loads[6:9]:
        load.wait()

    def pair_up(c, slot):
        return (
            seq_copy(mate, cross_k.at[slot, span(c)], cross_k.at[slot, span(c)], cs.at[c, 0], cr.at[c, 0]),
            seq_copy(mate, cross_v.at[slot, span(c)], cross_v.at[slot, span(c)], cs.at[c, 1], cr.at[c, 1]),
        )

    def close(c, carry):
        for k in range(1, sides):
            swap(c, k, here).wait_send()
            swap(c, k, lax.rem(here - k + sides, sides)).wait_recv()
        total = hidden[span(c), :]
        for side in range(sides):
            total = total + parts[side, span(c), :].astype(jnp.float32)
        done = norm_rows(total, g_final[...]).astype(jnp.bfloat16)
        encoded[span(c), :] = done
        cross_k[core, span(c), :] = jnp.dot(
            done, w_kv[0], preferred_element_type=jnp.float32
        ).astype(jnp.bfloat16)
        cross_v[core, span(c), :] = jnp.dot(
            done, w_kv[1], preferred_element_type=jnp.float32
        ).astype(jnp.bfloat16)
        for copy in pair_up(c, core):
            copy.start()
        return carry

    lax.fori_loop(0, chunks, close, 0)

    def paired(c, carry):
        for copy in pair_up(c, core):
            copy.wait_send()
        for copy in pair_up(c, 1 - core):
            copy.wait_recv()
        return carry

    lax.fori_loop(0, chunks, paired, 0)
    half = cross_q.shape[0]
    pairs = heads // 2
    peers = ring // 2
    position = lax.broadcasted_iota(jnp.int32, (1, 2 * rows), 1)
    first = me - core
    limit = jnp.where(position < rows, pad_lengths[first], rows + pad_lengths[first + 1])
    bias = jnp.where(position < limit, 0.0, masked_score)
    lane = lax.broadcasted_iota(jnp.int32, (2 * rows, 2 * HD), 1)
    out_lane = lax.broadcasted_iota(jnp.int32, (half, 2 * HD), 1)
    ones = jnp.ones((2 * rows, 2 * HD), jnp.bfloat16)
    stats[...] = jnp.where(out_lane < HD, 0.0, jnp.where(out_lane < HD + heads, 1.0, 0.0))

    def to_peer(i, j):
        to = flip(me, 2 * j, ring)
        source = mixed.at[i, rows_at(lax.div(to, 2) * slab, slab, slab)]
        return seq_copy(to, source, got.at[j, i], ms.at[j, i], mr.at[j, i])

    def to_peers(i):
        def send_one(j, carry):
            to_peer(i, peers - j).start()
            return carry

        lax.fori_loop(1, peers, send_one, 0)

    def cross_pair(i, carry):
        cut = rows_at(i * 2 * HD, 2 * HD, 2 * HD)
        q_here = cross_q[:, cut]
        k_here = cross_k[:, :, cut].reshape(2 * rows, 2 * HD)
        v_here = cross_v[:, :, cut].reshape(2 * rows, 2 * HD)
        pieces = []
        seen = stats[...]
        for h in range(2):
            own = lane < HD if h == 0 else lane >= HD
            keys = jnp.where(own, k_here, jnp.zeros_like(ones))
            values = jnp.where(own, v_here, ones)
            scores = bias + lax.dot_general(
                q_here, keys, (((1,), (1,)), ((), ())), preferred_element_type=jnp.float32
            )
            top = jnp.max(scores, axis=1, keepdims=True)
            weights = jnp.exp(scores - top).astype(jnp.bfloat16)
            piece = jnp.dot(weights, values, preferred_element_type=jnp.float32)
            total = piece[:, 2 * HD - 1 :] if h == 0 else piece[:, :1]
            seen = jnp.where(
                out_lane == 2 * i + h, top, jnp.where(out_lane == HD + 2 * i + h, total, seen)
            )
            pieces.append(piece)
        stats[...] = seen
        mixed[i] = jnp.where(out_lane < HD, pieces[0], pieces[1]).astype(jnp.bfloat16)
        to_peers(i)
        return carry

    lax.fori_loop(0, pairs, cross_pair, 0)
    seen = stats[...]
    high = seen.astype(jnp.bfloat16).astype(jnp.float32)
    rest = seen - high
    middle = rest.astype(jnp.bfloat16).astype(jnp.float32)
    mixed[pairs] = (
        high + pltpu.roll(middle, heads, 1) + pltpu.roll(rest - middle, 2 * heads, 1)
    ).astype(jnp.bfloat16)
    to_peers(pairs)
    got[0] = mixed[:, rows_at(lax.div(me, 2) * slab, slab, slab), :]

    def collect(j, carry):
        for i in range(pairs + 1):
            copy = to_peer(i, j)
            copy.wait_send()
            copy.wait_recv()
        return carry

    lax.fori_loop(1, peers, collect, 0)
    packed = got[:, pairs].astype(jnp.float32).reshape(peers * slab, 2 * HD)
    seen = packed + pltpu.roll(packed, 2 * HD - heads, 1) + pltpu.roll(packed, 2 * HD - 2 * heads, 1)
    sums = pltpu.roll(seen, HD, 1).reshape(peers, slab, 2 * HD)
    seen = seen.reshape(peers, slab, 2 * HD)
    best = jnp.max(seen, axis=0, keepdims=True)
    grow = jnp.exp(seen - best)
    weight_sum = jnp.sum(grow * sums, axis=0, keepdims=True)
    factor = (grow / weight_sum).reshape(peers * slab, 2 * HD)
    factor = jnp.where(lax.broadcasted_iota(jnp.int32, factor.shape, 1) < heads, factor, 0.0)
    column = lax.broadcasted_iota(jnp.int32, (2 * HD, heads * HD), 1)
    row = lax.broadcasted_iota(jnp.int32, (2 * HD, heads * HD), 0)
    spread = jnp.where((column >= row * HD) & (column < row * HD + HD), 1.0, 0.0)
    wide = jnp.dot(
        factor, spread, precision=lax.Precision.HIGHEST, preferred_element_type=jnp.float32
    ).reshape(peers, slab, heads * HD)
    merged = []
    for i in range(pairs):
        weighed = got[:, i].astype(jnp.float32) * wide[:, :, i * 2 * HD : (i + 1) * 2 * HD]
        merged.append(jnp.sum(weighed, axis=0).astype(jnp.bfloat16))
    product = jnp.dot(
        jnp.concatenate(merged, axis=1), w_cross[...], preferred_element_type=jnp.float32
    )
    partial[...] = product.astype(jnp.bfloat16)
    piece = incoming.shape[1]
    divided = piece < slab

    def piece_of(side):
        return rows_at(side * piece, piece, piece) if divided else pl.ds(0, piece)

    def exchange(k, side, origin):
        return side_copy(
            sides, k, partial.at[piece_of(side)], incoming.at[origin], xs.at[k], xr.at[k]
        )

    for k in range(1, sides):
        exchange(k, lax.rem(here + k, sides), here).start()
    incoming[here] = partial[piece_of(here), :]
    for k in range(1, sides):
        exchange(k, lax.rem(here + k, sides), here).wait_send()
        exchange(k, here, lax.rem(here - k + sides, sides)).wait_recv()
    total = incoming[0].astype(jnp.float32)
    for side in range(1, sides):
        total = total + incoming[side].astype(jnp.float32)

    def piece_start(owner, side):
        return slab_start(owner) + (side * piece if divided else 0)

    slot = piece_start(me, here) + lax.broadcasted_iota(jnp.int32, (piece, width), 0)
    limit = jnp.zeros((piece, width), jnp.int32)
    for n in range(target_lengths.shape[0]):
        begun = n * TGT_LEN
        limit = jnp.where(slot >= begun, begun + target_lengths[n], limit)
    decoded[rows_at(piece_start(me, here), piece, piece), :] = (
        mine[piece_of(here), :].astype(jnp.float32) + jnp.where(slot < limit, total, 0.0)
    ).astype(jnp.bfloat16)

    layers = ring // 4

    def block(owner, side):
        return decoded.at[rows_at(piece_start(owner, side), piece, piece)]

    def near(n):
        return flip(me, 2 * n, ring)

    def to_layer(m, owner):
        return seq_copy(flip(me, 4 * m, ring), block(owner, here), block(owner, here), zs.at[m], zr.at[m])

    def to_row(m, owner):
        return seq_copy(flip(me, 2, ring), block(owner, here), block(owner, here), ys.at[m], yr.at[m])

    def to_side(k, n, side):
        return side_copy(
            sides, k, block(near(n), side), block(near(n), side), ws.at[k, n], wr.at[k, n]
        )

    def to_mate(k, owner):
        def at(n):
            side = lax.rem(here - k + sides, sides)
            source = block(flip(owner, 2 * n, ring), side)
            return seq_copy(mate, source, source, hs.at[k, n], hr.at[k, n])

        return at

    given = range(1, sides) if divided else ()

    def pass_block(n):
        for k in given:
            to_side(k, n, here).start()
        to_mate(0, me)(n).start()

    for m in range(layers - 1, 0, -1):
        to_layer(m, me).start()
    to_row(0, me).start()
    pass_block(0)
    for m in range(layers):
        if m:
            to_layer(m, near(2 * m)).wait_recv()
            to_row(m, near(2 * m)).start()
            pass_block(2 * m)
        to_row(m, near(2 * m + 1)).wait_recv()
        pass_block(2 * m + 1)

    def across(n, carry):
        for k in given:
            to_side(k, n, lax.rem(here - k + sides, sides)).wait_recv()
            to_mate(k, me)(n).start()
        return carry

    lax.fori_loop(0, peers, across, 0)
    for m in range(layers):
        if m:
            to_layer(m, me).wait_send()
        to_row(m, near(2 * m)).wait_send()

    def settle(n, carry):
        for k in given:
            to_side(k, n, here).wait_send()
        for k in (0, *given):
            to_mate(k, me)(n).wait_send()
            to_mate(k, mate)(n).wait_recv()
        return carry

    lax.fori_loop(0, peers, settle, 0)


def encoder_block(
    ring, share, sides, back, pad_lengths, target_lengths, tokens, g_ffn, g_final, w_own, w_all,
    ffn_in, ffn_out, w_kv, cross_q, w_cross, targets,
):
    rows, width = tokens.shape
    heads = ring // share
    chunks = rows // math.gcd(rows, 128)
    slab = targets.shape[0] // ring
    piece = slab // sides if slab % (16 * sides) == 0 else slab
    half, lanes = cross_q.shape
    pairs = heads // 2
    peers = ring // 2
    layers = ring // 4
    bf16 = jnp.bfloat16
    vmem = pl.BlockSpec(memory_space=pltpu.VMEM)
    smem = pl.BlockSpec(memory_space=pltpu.SMEM)
    hbm = pl.BlockSpec(memory_space=pltpu.HBM)
    dma = pltpu.SemaphoreType.DMA
    return pl.pallas_call(
        functools.partial(block_kernel, ring, share, sides),
        out_shape=(
            jax.ShapeDtypeStruct((rows, width), bf16),
            jax.ShapeDtypeStruct(targets.shape, bf16),
        ),
        in_specs=[vmem, smem, smem] + [hbm] * 8 + [vmem, hbm, hbm],
        out_specs=(vmem, vmem),
        scratch_shapes=[
            pltpu.VMEM((rows, width), bf16),
            pltpu.VMEM((1, width), jnp.float32),
            pltpu.VMEM((1, width), jnp.float32),
            pltpu.VMEM((sides,) + w_own.shape, bf16),
            pltpu.VMEM((share, sides * heads, HD, rows // share), bf16),
            pltpu.VMEM((rows, width), jnp.float32),
            pltpu.VMEM((rows, width), bf16),
            pltpu.VMEM((sides, rows, width), bf16),
            pltpu.VMEM(ffn_in.shape, bf16),
            pltpu.VMEM(ffn_out.shape, bf16),
            pltpu.VMEM(w_kv.shape, bf16),
            pltpu.VMEM(w_cross.shape, bf16),
            pltpu.VMEM((slab, width), bf16),
            pltpu.VMEM((2, rows, lanes), bf16),
            pltpu.VMEM((2, rows, lanes), bf16),
            pltpu.VMEM((pairs + 1, half, 2 * HD), bf16),
            pltpu.VMEM((half, 2 * HD), jnp.float32),
            pltpu.VMEM((peers, pairs + 1, slab, 2 * HD), bf16),
            pltpu.VMEM((slab, width), bf16),
            pltpu.VMEM((sides, piece, width), bf16),
            dma((9 + sides,)),
            dma((ring,)),
            dma((ring,)),
            dma((ring, sides)),
            dma((ring, sides)),
            dma((chunks, sides)),
            dma((chunks, sides)),
            dma((chunks, 2)),
            dma((chunks, 2)),
            dma((peers, pairs + 1)),
            dma((peers, pairs + 1)),
            dma((sides,)),
            dma((sides,)),
            dma((layers,)),
            dma((layers,)),
            dma((layers,)),
            dma((layers,)),
            dma((sides, peers)),
            dma((sides, peers)),
            dma((sides, peers)),
            dma((sides, peers)),
        ],
        compiler_params=pltpu.CompilerParams(
            collective_id=1, has_side_effects=True, vmem_limit_bytes=50 * 1024 * 1024
        ),
        name="encoder_block",
    )(
        back, pad_lengths, target_lengths, tokens, g_ffn[None, :], g_final[None, :], w_own, w_all,
        ffn_in, ffn_out, w_kv, cross_q, w_cross, targets,
    )


def attend_kernel(lengths, q_ref, kv_ref, o_ref, keys, values, flipped, count):
    blocks, span, lanes = kv_ref.shape
    tile = span
    queries = q_ref.shape[1]
    group = math.gcd(queries, 256)
    ones_rows = flipped.shape[1] - HD
    lane = lax.broadcasted_iota(jnp.int32, (span, lanes), 1)
    row = lax.broadcasted_iota(jnp.int32, (span, lanes), 0)

    @pl.when(pl.program_id(0) == 0)
    def pack():
        def place(j, start):
            block = kv_ref[j]
            dead = jnp.where(row < lengths[j], 0.0, masked_score).astype(jnp.bfloat16)
            at = pl.ds(pl.multiple_of(start, 16), span)
            keys[at, :] = jnp.where(lane < HD, block, dead)
            values[at, :] = jnp.where(lane < HD, jnp.ones_like(block), block)
            return start + ((lengths[j] + 15) // 16) * 16

        stop = lax.fori_loop(0, blocks, place, 0)
        at = pl.ds(pl.multiple_of(stop, 16), span)
        keys[at, :] = jnp.where(lane < HD, 0.0, masked_score).astype(jnp.bfloat16)
        values[at, :] = jnp.zeros((span, lanes), jnp.bfloat16)
        count[0] = (stop + tile - 1) // tile

        def flip(t, carry):
            at = pl.ds(pl.multiple_of(t * tile, tile), tile)
            flipped[t] = values[at, :].T[HD - ones_rows :, :]
            return carry

        lax.fori_loop(0, count[0], flip, 0)

    spare = lax.broadcasted_iota(jnp.int32, (HD, queries), 0)
    pick = jnp.where(spare == 0, 1.0, 0.0).astype(jnp.bfloat16)
    q_wide = jnp.concatenate([q_ref[...], pick], axis=0)
    cuts = [slice(g, g + group) for g in range(0, queries, group)]

    def step(t, state):
        at = pl.ds(pl.multiple_of(t * tile, tile), tile)
        keys_here = keys[at, :]
        values_here = flipped[t]
        all_scores = [
            jnp.dot(keys_here, q_wide[:, cut], preferred_element_type=jnp.float32) for cut in cuts
        ]
        updated = []
        for scores, (top, mixed) in zip(all_scores, state):
            new_top = jnp.maximum(top, jnp.max(scores, axis=0, keepdims=True))
            weights = jnp.exp(scores - new_top).astype(jnp.bfloat16)
            part = jnp.dot(values_here, weights, preferred_element_type=jnp.float32)
            updated.append((new_top, mixed * jnp.exp(top - new_top) + part))
        return tuple(updated)

    start = tuple(
        (
            jnp.full((1, group), masked_score, jnp.float32),
            jnp.zeros((ones_rows + HD, group), jnp.float32),
        )
        for cut in cuts
    )
    ends = lax.fori_loop(0, count[0], step, start)
    for cut, (top, mixed) in zip(cuts, ends):
        o_ref[:, cut] = (mixed[ones_rows:, :] / mixed[0:1, :]).astype(jnp.bfloat16)


def attend(q_all, kv_all, pad_lengths):
    blocks, span, lanes = kv_all.shape
    total = q_all.shape[1]
    width = math.gcd(total, 2048)
    return pl.pallas_call(
        attend_kernel,
        out_shape=jax.ShapeDtypeStruct((HD, total), jnp.bfloat16),
        grid_spec=pltpu.PrefetchScalarGridSpec(
            num_scalar_prefetch=1,
            grid=(total // width,),
            in_specs=[
                pl.BlockSpec((HD, width), lambda i, lengths: (0, i)),
                pl.BlockSpec((blocks, span, lanes), lambda i, lengths: (0, 0, 0)),
            ],
            out_specs=pl.BlockSpec((HD, width), lambda i, lengths: (0, i)),
            scratch_shapes=[
                pltpu.VMEM(((blocks + 1) * span, lanes), jnp.bfloat16),
                pltpu.VMEM(((blocks + 1) * span, lanes), jnp.bfloat16),
                pltpu.VMEM((blocks + 1, HD + 16, span), jnp.bfloat16),
                pltpu.SMEM((1,), jnp.int32),
            ],
        ),
        compiler_params=pltpu.CompilerParams(
            dimension_semantics=("arbitrary",), vmem_limit_bytes=48 * 1024 * 1024
        ),
        name="attend",
    )(pad_lengths, q_all, kv_all)


def local(
    ring,
    sides,
    tokens,
    norm_attn,
    self_qkv,
    self_out,
    norm_ffn,
    ffn_in,
    ffn_out,
    norm_final,
    pad_lengths,
    targets,
    target_lengths,
    norm_cross,
    cross_query,
    cross_kv,
    cross_out,
):
    heads_here = self_qkv.shape[2] // HD
    share = ring // heads_here
    part = tokens.shape[0] // share
    q_got, kv_got, out_all, cross_q = scatter_heads(
        ring, share, sides, tokens, norm_attn, self_qkv, self_out, targets, norm_cross, cross_query
    )
    q_all = q_got.transpose(1, 0, 2).reshape(HD, ring * part)
    mixed_t = attend(q_all, kv_got, pad_lengths)
    back = mixed_t.reshape(HD, ring, part).transpose(1, 0, 2)
    return encoder_block(
        ring,
        share,
        sides,
        back,
        pad_lengths,
        target_lengths,
        tokens,
        norm_ffn,
        norm_final,
        self_out,
        out_all,
        ffn_in,
        ffn_out,
        cross_kv,
        cross_q,
        cross_out,
        targets,
    )


def solution(mesh):
    ring = mesh.shape["seq"]
    sides = mesh.shape["head"]
    placed = (
        P("seq", None),
        P(),
        P(None, None, "head"),
        P("head", None),
        P(),
        P(None, None, "head"),
        P("head", None),
        P(),
        P(),
        P(),
        P(),
        P(),
        P(None, "head"),
        P(None, None, "head"),
        P("head", None),
    )
    return jax.shard_map(
        functools.partial(local, ring, sides),
        mesh=mesh,
        in_specs=placed,
        out_specs=(P("seq", None), P()),
        check_vma=False,
    )
```

```python
import functools
import math

import jax
import jax.numpy as jnp
from jax import lax
from jax.experimental import pallas as pl
from jax.experimental.pallas import tpu as pltpu
from jax.sharding import PartitionSpec as P

HD = 64
TGT_LEN = 128

epsilon = 1e-06
masked_score = -1e30
MESH = pl.DeviceIdType.MESH


def flip(index, other, count):
    result = 0
    weight = 1
    while weight < count:
        digit = other // weight if isinstance(other, int) else lax.div(other, weight)
        result = result + lax.rem(lax.div(index, weight) + digit, 2) * weight
        weight *= 2
    return result


def rows_at(start, size, align):
    return pl.ds(pl.multiple_of(start, align), size)


def greet_all(ring, sides):
    me = lax.axis_index("seq")
    here = lax.axis_index("head")
    barrier = pltpu.get_barrier_semaphore()

    def greet(i, carry):
        pl.semaphore_signal(
            barrier, inc=1, device_id={"seq": lax.rem(me + i, ring)}, device_id_type=MESH
        )
        return carry

    lax.fori_loop(1, ring, greet, 0)
    for k in range(1, sides):
        pl.semaphore_signal(
            barrier, inc=1, device_id={"head": lax.rem(here + k, sides)}, device_id_type=MESH
        )
    pl.semaphore_wait(barrier, ring - 1 + sides - 1)


def seq_copy(to, source, target, send_sem, recv_sem):
    return pltpu.make_async_remote_copy(
        src_ref=source,
        dst_ref=target,
        send_sem=send_sem,
        recv_sem=recv_sem,
        device_id={"seq": to},
        device_id_type=MESH,
    )


def side_copy(sides, k, source, target, send_sem, recv_sem):
    here = lax.axis_index("head")
    return pltpu.make_async_remote_copy(
        src_ref=source,
        dst_ref=target,
        send_sem=send_sem,
        recv_sem=recv_sem,
        device_id={"head": lax.rem(here + k, sides)},
        device_id_type=MESH,
    )


def in_hbm(array):
    return pltpu.with_memory_space_constraint(array, pltpu.HBM)


def norm_rows(values, gain):
    scale = lax.rsqrt(jnp.mean(values * values, axis=-1, keepdims=True) + epsilon)
    return values * scale * gain


def scatter_kernel(
    ring, share, sides, tokens_hbm, gain_hbm, qkv_hbm, out_hbm, targets_hbm, g_cross_hbm, w_cross_hbm,
    q_out, kv_out, out_all, cross_q,
    tokens, gain, qkv, targets, g_cross, w_cross, normed, q_in, kv_in,
    qs, qr, ks, kr, fs, fr, ls, os, ws, wr,
):
    me = lax.axis_index("seq")
    here = lax.axis_index("head")
    half = targets.shape[0]
    part = kv_in.shape[1]
    heads = ring // share
    slot = lax.rem(me, share)
    mine = rows_at(slot * part, part, part)
    loads = [
        pltpu.make_async_copy(source, target, ls.at[n])
        for n, (source, target) in enumerate(
            [
                (tokens_hbm, tokens),
                (gain_hbm, gain),
                (qkv_hbm.at[1], qkv.at[1]),
                (qkv_hbm.at[2], qkv.at[2]),
                (qkv_hbm.at[0], qkv.at[0]),
                (targets_hbm.at[rows_at(lax.rem(me, 2) * half, half, half)], targets),
                (g_cross_hbm, g_cross),
                (w_cross_hbm, w_cross),
            ]
        )
    ]
    for load in loads:
        load.start()
    greet_all(ring, sides)
    for k in range(1, sides):
        side_copy(sides, k, out_hbm, out_all.at[here], ws.at[k], wr.at[k]).start()

    def q_copy(i):
        to = flip(me, i, ring)
        return seq_copy(to, q_in.at[to], q_out.at[me], qs.at[i], qr.at[i])

    def kv_copy(i):
        to = flip(me, i, ring)
        rows = rows_at(lax.rem(to, share) * part, part, part)
        return seq_copy(to, kv_in.at[to], kv_out.at[me, rows], ks.at[i], kr.at[i])

    def forward(i, k):
        block = kv_out.at[flip(me, i, ring), mine]
        to = me - slot + lax.rem(slot + k, share)
        return seq_copy(to, block, block, fs.at[i, k], fr.at[i, k])

    def arrived(i, k):
        giver = me - slot + lax.rem(slot - k + share, share)
        rows = rows_at(lax.rem(giver, share) * part, part, part)
        block = kv_out.at[flip(giver, i, ring), rows]
        return seq_copy(giver, block, block, fs.at[i, k], fr.at[i, k])

    loads[0].wait()
    loads[1].wait()
    normed[...] = norm_rows(tokens[...].astype(jnp.float32), gain[...]).astype(jnp.bfloat16)
    loads[2].wait()
    loads[3].wait()
    keys = jnp.dot(normed[...], qkv[1], preferred_element_type=jnp.float32).astype(jnp.bfloat16)
    values = jnp.dot(normed[...], qkv[2], preferred_element_type=jnp.float32).astype(jnp.bfloat16)
    for h in range(heads):
        cut = slice(h * HD, (h + 1) * HD)
        both = jnp.concatenate([keys[:, cut], values[:, cut]], axis=1)
        for s in range(share):
            kv_in[h * share + s] = both[s * part : (s + 1) * part, :]

    span = ring // 2
    inner = lax.rem(lax.div(me, span) + lax.div(me, ring // 4), 2)

    def send_half(copy, far):
        def send(n, carry):
            step = far * span + n

            @pl.when(step > 0)
            def away():
                copy(step).start()

            return carry

        lax.fori_loop(0, span, send, 0)

    send_half(kv_copy, inner)
    own_kv = pltpu.make_async_copy(kv_in.at[me], kv_out.at[me, mine], os.at[1])
    own_kv.start()
    loads[4].wait()
    queries = lax.dot_general(
        qkv[0], normed[...], (((0,), (1,)), ((), ())), preferred_element_type=jnp.float32
    ).astype(jnp.bfloat16) * jnp.bfloat16(HD ** (-0.5))
    for h in range(heads):
        for s in range(share):
            q_in[h * share + s] = queries[h * HD : (h + 1) * HD, s * part : (s + 1) * part]

    send_half(q_copy, 0)
    send_half(kv_copy, 1 - inner)
    send_half(q_copy, 1)
    own_q = pltpu.make_async_copy(q_in.at[me], q_out.at[me], os.at[0])
    own_q.start()
    own_kv.wait()
    for k in range(1, share):
        forward(0, k).start()
    for load in loads[5:]:
        load.wait()
    cross_normed = norm_rows(targets[...].astype(jnp.float32), g_cross[...]).astype(jnp.bfloat16)
    cross_q[...] = jnp.dot(
        cross_normed, w_cross[...], preferred_element_type=jnp.float32
    ).astype(jnp.bfloat16) * jnp.bfloat16(HD ** (-0.5))

    def relay(i, carry):
        origin = flip(me, i, ring)
        seq_copy(origin, kv_in.at[0], kv_out.at[origin, mine], ks.at[i], kr.at[i]).wait_recv()
        for k in range(1, share):
            forward(i, k).start()
        return carry

    lax.fori_loop(1, ring, relay, 0)

    def finish(i, carry):
        origin = flip(me, i, ring)
        seq_copy(origin, q_in.at[0], q_out.at[origin], qs.at[i], qr.at[i]).wait_recv()
        q_copy(i).wait_send()
        kv_copy(i).wait_send()
        return carry

    lax.fori_loop(1, ring, finish, 0)

    def drain(i, carry):
        for k in range(1, share):
            arrived(i, k).wait_recv()
            forward(i, k).wait_send()
        return carry

    lax.fori_loop(0, ring, drain, 0)
    for k in range(1, sides):
        origin = lax.rem(here - k + sides, sides)
        side_copy(sides, k, out_hbm, out_all.at[origin], ws.at[k], wr.at[k]).wait()
    own_q.wait()


def scatter_heads(ring, share, sides, tokens, gain, qkv, w_out, targets, g_cross, w_cross):
    rows, width = tokens.shape
    heads = ring // share
    part = rows // share
    half = targets.shape[0] // 2
    bf16 = jnp.bfloat16
    vmem = pl.BlockSpec(memory_space=pltpu.VMEM)
    hbm = pl.BlockSpec(memory_space=pltpu.HBM)
    dma = pltpu.SemaphoreType.DMA
    return pl.pallas_call(
        functools.partial(scatter_kernel, ring, share, sides),
        out_shape=(
            jax.ShapeDtypeStruct((ring, HD, part), bf16),
            jax.ShapeDtypeStruct((ring, rows, 2 * HD), bf16),
            jax.ShapeDtypeStruct((sides,) + w_out.shape, bf16),
            jax.ShapeDtypeStruct((half, w_cross.shape[1]), bf16),
        ),
        in_specs=[hbm] * 7,
        out_specs=(vmem, vmem, hbm, vmem),
        scratch_shapes=[
            pltpu.VMEM((rows, width), bf16),
            pltpu.VMEM((1, width), jnp.float32),
            pltpu.VMEM(qkv.shape, bf16),
            pltpu.VMEM((half, width), bf16),
            pltpu.VMEM((1, width), jnp.float32),
            pltpu.VMEM(w_cross.shape, bf16),
            pltpu.VMEM((rows, width), bf16),
            pltpu.VMEM((heads * share, HD, part), bf16),
            pltpu.VMEM((heads * share, part, 2 * HD), bf16),
            dma((ring,)),
            dma((ring,)),
            dma((ring,)),
            dma((ring,)),
            dma((ring, share)),
            dma((ring, share)),
            dma((8,)),
            dma((2,)),
            dma((sides,)),
            dma((sides,)),
        ],
        compiler_params=pltpu.CompilerParams(
            collective_id=0, has_side_effects=True, vmem_limit_bytes=40 * 1024 * 1024
        ),
        name="scatter_heads",
    )(*map(in_hbm, (tokens, gain[None, :], qkv, w_out, targets, g_cross[None, :], w_cross)))


def block_kernel(
    ring, share, sides, x_in, pad_lengths, target_lengths, tokens_hbm, g_ffn_hbm, g_final_hbm,
    w_own_hbm, w_all_hbm, up_hbm, down_hbm, kv_hbm, cross_q, w_cross_hbm, targets_hbm,
    encoded, decoded,
    tokens, g_ffn, g_final, w_out, context, hidden, normed, parts, up, down, w_kv, w_cross, mine,
    cross_k, cross_v, mixed, stats, got, partial, incoming,
    ls, ss, rs, fs, fr, ps, pr, cs, cr, ms, mr, xs, xr, zs, zr, ys, yr, ws, wr, hs, hr,
):
    me = lax.axis_index("seq")
    here = lax.axis_index("head")
    heads = ring // share
    rows, width = tokens.shape
    slab = mine.shape[0]
    core = lax.rem(me, 2)
    mate = flip(me, 1, ring)

    def slab_start(owner):
        return (lax.rem(owner, 2) * (ring // 2) + lax.div(owner, 2)) * slab

    loads = [
        pltpu.make_async_copy(source, target, ls.at[n])
        for n, (source, target) in enumerate(
            [
                (tokens_hbm, tokens),
                (g_ffn_hbm, g_ffn),
                (w_own_hbm, w_out.at[here]),
                (up_hbm, up),
                (down_hbm, down),
                (g_final_hbm, g_final),
                (kv_hbm, w_kv),
                (w_cross_hbm, w_cross),
                (targets_hbm.at[rows_at(slab_start(me), slab, slab)], mine),
            ]
            + [
                (w_all_hbm.at[lax.rem(here + k, sides)], w_out.at[lax.rem(here + k, sides)])
                for k in range(1, sides)
            ]
        )
    ]
    for load in loads:
        load.start()

    def place(side, origin):
        return context.at[lax.rem(origin, share), side * heads + lax.div(origin, share)]

    own = pltpu.make_async_copy(x_in.at[me], place(here, me), ls.at[len(loads)])
    own.start()
    greet_all(ring, sides)

    def outgoing(i):
        to = flip(me, i, ring)
        return seq_copy(to, x_in.at[to], place(here, me), ss.at[i], rs.at[i])

    def relay(i, k):
        block = place(here, flip(me, i, ring))
        return side_copy(sides, k, block, block, fs.at[i, k], fr.at[i, k])

    def send(i, carry):
        outgoing(i).start()
        return carry

    lax.fori_loop(1, ring, send, 0)
    own.wait()
    for k in range(1, sides):
        relay(0, k).start()

    def pass_on(i, carry):
        origin = flip(me, i, ring)
        seq_copy(origin, x_in.at[0], place(here, origin), ss.at[i], rs.at[i]).wait_recv()
        for k in range(1, sides):
            relay(i, k).start()
        return carry

    lax.fori_loop(1, ring, pass_on, 0)

    def sent(i, carry):
        outgoing(i).wait_send()
        return carry

    lax.fori_loop(1, ring, sent, 0)

    def drain(i, carry):
        for k in range(1, sides):
            relay(i, k).wait_send()
            block = place(lax.rem(here - k + sides, sides), flip(me, i, ring))
            side_copy(sides, k, block, block, fs.at[i, k], fr.at[i, k]).wait_recv()
        return carry

    lax.fori_loop(0, ring, drain, 0)
    for load in loads[:3] + loads[9:]:
        load.wait()
    part = rows // share

    def project(c, carry):
        at = rows_at(c * part, part, part)
        flat = context[c].reshape(sides * heads * HD, part)
        total = tokens[at, :].astype(jnp.float32) + lax.dot_general(
            flat, w_out[...].reshape(sides * heads * HD, width), (((0,), (0,)), ((), ())),
            preferred_element_type=jnp.float32,
        )
        hidden[at, :] = total
        normed[at, :] = norm_rows(total, g_ffn[...]).astype(jnp.bfloat16)
        return carry

    lax.fori_loop(0, share, project, 0)
    for load in loads[3:6]:
        load.wait()
    chunk = math.gcd(rows, 128)
    chunks = rows // chunk

    def span(c):
        return rows_at(c * chunk, chunk, chunk)

    def swap(c, k, side):
        return side_copy(
            sides, k, parts.at[side, span(c)], parts.at[side, span(c)], ps.at[c, k], pr.at[c, k]
        )

    def feed(c, carry):
        x = normed[span(c), :]
        gate = jnp.dot(x, up[0], preferred_element_type=jnp.float32)
        lift = jnp.dot(x, up[1], preferred_element_type=jnp.float32)
        active = (jax.nn.gelu(gate, approximate=True) * lift).astype(jnp.bfloat16)
        parts[here, span(c), :] = jnp.dot(
            active, down[...], preferred_element_type=jnp.float32
        ).astype(jnp.bfloat16)
        for k in range(1, sides):
            swap(c, k, here).start()
        return carry

    lax.fori_loop(0, chunks, feed, 0)
    for load in loads[6:9]:
        load.wait()

    def pair_up(c, slot):
        return (
            seq_copy(mate, cross_k.at[slot, span(c)], cross_k.at[slot, span(c)], cs.at[c, 0], cr.at[c, 0]),
            seq_copy(mate, cross_v.at[slot, span(c)], cross_v.at[slot, span(c)], cs.at[c, 1], cr.at[c, 1]),
        )

    def close(c, carry):
        for k in range(1, sides):
            swap(c, k, here).wait_send()
            swap(c, k, lax.rem(here - k + sides, sides)).wait_recv()
        total = hidden[span(c), :]
        for side in range(sides):
            total = total + parts[side, span(c), :].astype(jnp.float32)
        done = norm_rows(total, g_final[...]).astype(jnp.bfloat16)
        encoded[span(c), :] = done
        cross_k[core, span(c), :] = jnp.dot(
            done, w_kv[0], preferred_element_type=jnp.float32
        ).astype(jnp.bfloat16)
        cross_v[core, span(c), :] = jnp.dot(
            done, w_kv[1], preferred_element_type=jnp.float32
        ).astype(jnp.bfloat16)
        for copy in pair_up(c, core):
            copy.start()
        return carry

    lax.fori_loop(0, chunks, close, 0)

    def paired(c, carry):
        for copy in pair_up(c, core):
            copy.wait_send()
        for copy in pair_up(c, 1 - core):
            copy.wait_recv()
        return carry

    lax.fori_loop(0, chunks, paired, 0)
    half = cross_q.shape[0]
    pairs = heads // 2
    peers = ring // 2
    position = lax.broadcasted_iota(jnp.int32, (1, 2 * rows), 1)
    first = me - core
    limit = jnp.where(position < rows, pad_lengths[first], rows + pad_lengths[first + 1])
    bias = jnp.where(position < limit, 0.0, masked_score)
    lane = lax.broadcasted_iota(jnp.int32, (2 * rows, 2 * HD), 1)
    out_lane = lax.broadcasted_iota(jnp.int32, (half, 2 * HD), 1)
    ones = jnp.ones((2 * rows, 2 * HD), jnp.bfloat16)
    stats[...] = jnp.where(out_lane < HD, 0.0, jnp.where(out_lane < HD + heads, 1.0, 0.0))

    def to_peer(i, j):
        to = flip(me, 2 * j, ring)
        source = mixed.at[i, rows_at(lax.div(to, 2) * slab, slab, slab)]
        return seq_copy(to, source, got.at[j, i], ms.at[j, i], mr.at[j, i])

    def to_peers(i):
        def send_one(j, carry):
            to_peer(i, peers - j).start()
            return carry

        lax.fori_loop(1, peers, send_one, 0)

    def cross_pair(i, carry):
        cut = rows_at(i * 2 * HD, 2 * HD, 2 * HD)
        q_here = cross_q[:, cut]
        k_here = cross_k[:, :, cut].reshape(2 * rows, 2 * HD)
        v_here = cross_v[:, :, cut].reshape(2 * rows, 2 * HD)
        pieces = []
        seen = stats[...]
        for h in range(2):
            own = lane < HD if h == 0 else lane >= HD
            keys = jnp.where(own, k_here, jnp.zeros_like(ones))
            values = jnp.where(own, v_here, ones)
            scores = bias + lax.dot_general(
                q_here, keys, (((1,), (1,)), ((), ())), preferred_element_type=jnp.float32
            )
            top = jnp.max(scores, axis=1, keepdims=True)
            weights = jnp.exp(scores - top).astype(jnp.bfloat16)
            piece = jnp.dot(weights, values, preferred_element_type=jnp.float32)
            total = piece[:, 2 * HD - 1 :] if h == 0 else piece[:, :1]
            seen = jnp.where(
                out_lane == 2 * i + h, top, jnp.where(out_lane == HD + 2 * i + h, total, seen)
            )
            pieces.append(piece)
        stats[...] = seen
        mixed[i] = jnp.where(out_lane < HD, pieces[0], pieces[1]).astype(jnp.bfloat16)
        to_peers(i)
        return carry

    lax.fori_loop(0, pairs, cross_pair, 0)
    seen = stats[...]
    high = seen.astype(jnp.bfloat16).astype(jnp.float32)
    rest = seen - high
    middle = rest.astype(jnp.bfloat16).astype(jnp.float32)
    mixed[pairs] = (
        high + pltpu.roll(middle, heads, 1) + pltpu.roll(rest - middle, 2 * heads, 1)
    ).astype(jnp.bfloat16)
    to_peers(pairs)
    got[0] = mixed[:, rows_at(lax.div(me, 2) * slab, slab, slab), :]

    def collect(j, carry):
        for i in range(pairs + 1):
            copy = to_peer(i, j)
            copy.wait_send()
            copy.wait_recv()
        return carry

    lax.fori_loop(1, peers, collect, 0)
    packed = got[:, pairs].astype(jnp.float32).reshape(peers * slab, 2 * HD)
    seen = packed + pltpu.roll(packed, 2 * HD - heads, 1) + pltpu.roll(packed, 2 * HD - 2 * heads, 1)
    sums = pltpu.roll(seen, HD, 1).reshape(peers, slab, 2 * HD)
    seen = seen.reshape(peers, slab, 2 * HD)
    best = jnp.max(seen, axis=0, keepdims=True)
    grow = jnp.exp(seen - best)
    weight_sum = jnp.sum(grow * sums, axis=0, keepdims=True)
    factor = (grow / weight_sum).reshape(peers * slab, 2 * HD)
    factor = jnp.where(lax.broadcasted_iota(jnp.int32, factor.shape, 1) < heads, factor, 0.0)
    column = lax.broadcasted_iota(jnp.int32, (2 * HD, heads * HD), 1)
    row = lax.broadcasted_iota(jnp.int32, (2 * HD, heads * HD), 0)
    spread = jnp.where((column >= row * HD) & (column < row * HD + HD), 1.0, 0.0)
    wide = jnp.dot(
        factor, spread, precision=lax.Precision.HIGHEST, preferred_element_type=jnp.float32
    ).reshape(peers, slab, heads * HD)
    merged = []
    for i in range(pairs):
        weighed = got[:, i].astype(jnp.float32) * wide[:, :, i * 2 * HD : (i + 1) * 2 * HD]
        merged.append(jnp.sum(weighed, axis=0).astype(jnp.bfloat16))
    product = jnp.dot(
        jnp.concatenate(merged, axis=1), w_cross[...], preferred_element_type=jnp.float32
    )
    partial[...] = product.astype(jnp.bfloat16)
    piece = incoming.shape[1]
    divided = piece < slab

    def piece_of(side):
        return rows_at(side * piece, piece, piece) if divided else pl.ds(0, piece)

    def exchange(k, side, origin):
        return side_copy(
            sides, k, partial.at[piece_of(side)], incoming.at[origin], xs.at[k], xr.at[k]
        )

    for k in range(1, sides):
        exchange(k, lax.rem(here + k, sides), here).start()
    incoming[here] = partial[piece_of(here), :]
    for k in range(1, sides):
        exchange(k, lax.rem(here + k, sides), here).wait_send()
        exchange(k, here, lax.rem(here - k + sides, sides)).wait_recv()
    total = incoming[0].astype(jnp.float32)
    for side in range(1, sides):
        total = total + incoming[side].astype(jnp.float32)

    def piece_start(owner, side):
        return slab_start(owner) + (side * piece if divided else 0)

    slot = piece_start(me, here) + lax.broadcasted_iota(jnp.int32, (piece, width), 0)
    limit = jnp.zeros((piece, width), jnp.int32)
    for n in range(target_lengths.shape[0]):
        begun = n * TGT_LEN
        limit = jnp.where(slot >= begun, begun + target_lengths[n], limit)
    decoded[rows_at(piece_start(me, here), piece, piece), :] = (
        mine[piece_of(here), :].astype(jnp.float32) + jnp.where(slot < limit, total, 0.0)
    ).astype(jnp.bfloat16)

    layers = ring // 4

    def block(owner, side):
        return decoded.at[rows_at(piece_start(owner, side), piece, piece)]

    def near(n):
        return flip(me, 2 * n, ring)

    def to_layer(m, owner):
        return seq_copy(flip(me, 4 * m, ring), block(owner, here), block(owner, here), zs.at[m], zr.at[m])

    def to_row(m, owner):
        return seq_copy(flip(me, 2, ring), block(owner, here), block(owner, here), ys.at[m], yr.at[m])

    def to_side(k, n, side):
        return side_copy(
            sides, k, block(near(n), side), block(near(n), side), ws.at[k, n], wr.at[k, n]
        )

    def to_mate(k, owner):
        def at(n):
            side = lax.rem(here - k + sides, sides)
            source = block(flip(owner, 2 * n, ring), side)
            return seq_copy(mate, source, source, hs.at[k, n], hr.at[k, n])

        return at

    given = range(1, sides) if divided else ()

    def pass_block(n):
        for k in given:
            to_side(k, n, here).start()
        to_mate(0, me)(n).start()

    for m in range(layers - 1, 0, -1):
        to_layer(m, me).start()
    to_row(0, me).start()
    pass_block(0)
    for m in range(layers):
        if m:
            to_layer(m, near(2 * m)).wait_recv()
            to_row(m, near(2 * m)).start()
            pass_block(2 * m)
        to_row(m, near(2 * m + 1)).wait_recv()
        pass_block(2 * m + 1)

    def across(n, carry):
        for k in given:
            to_side(k, n, lax.rem(here - k + sides, sides)).wait_recv()
            to_mate(k, me)(n).start()
        return carry

    lax.fori_loop(0, peers, across, 0)
    for m in range(layers):
        if m:
            to_layer(m, me).wait_send()
        to_row(m, near(2 * m)).wait_send()

    def settle(n, carry):
        for k in given:
            to_side(k, n, here).wait_send()
        for k in (0, *given):
            to_mate(k, me)(n).wait_send()
            to_mate(k, mate)(n).wait_recv()
        return carry

    lax.fori_loop(0, peers, settle, 0)


def encoder_block(
    ring, share, sides, back, pad_lengths, target_lengths, tokens, g_ffn, g_final, w_own, w_all,
    ffn_in, ffn_out, w_kv, cross_q, w_cross, targets,
):
    rows, width = tokens.shape
    heads = ring // share
    chunks = rows // math.gcd(rows, 128)
    slab = targets.shape[0] // ring
    piece = slab // sides if slab % (16 * sides) == 0 else slab
    half, lanes = cross_q.shape
    pairs = heads // 2
    peers = ring // 2
    layers = ring // 4
    bf16 = jnp.bfloat16
    vmem = pl.BlockSpec(memory_space=pltpu.VMEM)
    smem = pl.BlockSpec(memory_space=pltpu.SMEM)
    hbm = pl.BlockSpec(memory_space=pltpu.HBM)
    dma = pltpu.SemaphoreType.DMA
    return pl.pallas_call(
        functools.partial(block_kernel, ring, share, sides),
        out_shape=(
            jax.ShapeDtypeStruct((rows, width), bf16),
            jax.ShapeDtypeStruct(targets.shape, bf16),
        ),
        in_specs=[vmem, smem, smem] + [hbm] * 8 + [vmem, hbm, hbm],
        out_specs=(vmem, vmem),
        scratch_shapes=[
            pltpu.VMEM((rows, width), bf16),
            pltpu.VMEM((1, width), jnp.float32),
            pltpu.VMEM((1, width), jnp.float32),
            pltpu.VMEM((sides,) + w_own.shape, bf16),
            pltpu.VMEM((share, sides * heads, HD, rows // share), bf16),
            pltpu.VMEM((rows, width), jnp.float32),
            pltpu.VMEM((rows, width), bf16),
            pltpu.VMEM((sides, rows, width), bf16),
            pltpu.VMEM(ffn_in.shape, bf16),
            pltpu.VMEM(ffn_out.shape, bf16),
            pltpu.VMEM(w_kv.shape, bf16),
            pltpu.VMEM(w_cross.shape, bf16),
            pltpu.VMEM((slab, width), bf16),
            pltpu.VMEM((2, rows, lanes), bf16),
            pltpu.VMEM((2, rows, lanes), bf16),
            pltpu.VMEM((pairs + 1, half, 2 * HD), bf16),
            pltpu.VMEM((half, 2 * HD), jnp.float32),
            pltpu.VMEM((peers, pairs + 1, slab, 2 * HD), bf16),
            pltpu.VMEM((slab, width), bf16),
            pltpu.VMEM((sides, piece, width), bf16),
            dma((9 + sides,)),
            dma((ring,)),
            dma((ring,)),
            dma((ring, sides)),
            dma((ring, sides)),
            dma((chunks, sides)),
            dma((chunks, sides)),
            dma((chunks, 2)),
            dma((chunks, 2)),
            dma((peers, pairs + 1)),
            dma((peers, pairs + 1)),
            dma((sides,)),
            dma((sides,)),
            dma((layers,)),
            dma((layers,)),
            dma((layers,)),
            dma((layers,)),
            dma((sides, peers)),
            dma((sides, peers)),
            dma((sides, peers)),
            dma((sides, peers)),
        ],
        compiler_params=pltpu.CompilerParams(
            collective_id=1, has_side_effects=True, vmem_limit_bytes=50 * 1024 * 1024
        ),
        name="encoder_block",
    )(
        back, pad_lengths, target_lengths, tokens, g_ffn[None, :], g_final[None, :], w_own, w_all,
        ffn_in, ffn_out, w_kv, cross_q, w_cross, targets,
    )


def attend_kernel(lengths, q_ref, kv_ref, o_ref, keys, values, flipped, count):
    blocks, span, lanes = kv_ref.shape
    tile = span
    queries = q_ref.shape[1]
    group = math.gcd(queries, 256)
    ones_rows = flipped.shape[1] - HD
    lane = lax.broadcasted_iota(jnp.int32, (span, lanes), 1)
    row = lax.broadcasted_iota(jnp.int32, (span, lanes), 0)

    @pl.when(pl.program_id(0) == 0)
    def pack():
        def place(j, start):
            block = kv_ref[j]
            dead = jnp.where(row < lengths[j], 0.0, masked_score).astype(jnp.bfloat16)
            at = pl.ds(pl.multiple_of(start, 16), span)
            keys[at, :] = jnp.where(lane < HD, block, dead)
            values[at, :] = jnp.where(lane < HD, jnp.ones_like(block), block)
            return start + ((lengths[j] + 15) // 16) * 16

        stop = lax.fori_loop(0, blocks, place, 0)
        at = pl.ds(pl.multiple_of(stop, 16), span)
        keys[at, :] = jnp.where(lane < HD, 0.0, masked_score).astype(jnp.bfloat16)
        values[at, :] = jnp.zeros((span, lanes), jnp.bfloat16)
        count[0] = (stop + tile - 1) // tile

        def flip(t, carry):
            at = pl.ds(pl.multiple_of(t * tile, tile), tile)
            flipped[t] = values[at, :].T[HD - ones_rows :, :]
            return carry

        lax.fori_loop(0, count[0], flip, 0)

    spare = lax.broadcasted_iota(jnp.int32, (HD, queries), 0)
    pick = jnp.where(spare == 0, 1.0, 0.0).astype(jnp.bfloat16)
    q_wide = jnp.concatenate([q_ref[...], pick], axis=0)
    cuts = [slice(g, g + group) for g in range(0, queries, group)]

    def step(t, state):
        at = pl.ds(pl.multiple_of(t * tile, tile), tile)
        keys_here = keys[at, :]
        values_here = flipped[t]
        all_scores = [
            jnp.dot(keys_here, q_wide[:, cut], preferred_element_type=jnp.float32) for cut in cuts
        ]
        updated = []
        for scores, (top, mixed) in zip(all_scores, state):
            new_top = jnp.maximum(top, jnp.max(scores, axis=0, keepdims=True))
            weights = jnp.exp(scores - new_top).astype(jnp.bfloat16)
            part = jnp.dot(values_here, weights, preferred_element_type=jnp.float32)
            updated.append((new_top, mixed * jnp.exp(top - new_top) + part))
        return tuple(updated)

    start = tuple(
        (
            jnp.full((1, group), masked_score, jnp.float32),
            jnp.zeros((ones_rows + HD, group), jnp.float32),
        )
        for cut in cuts
    )
    ends = lax.fori_loop(0, count[0], step, start)
    for cut, (top, mixed) in zip(cuts, ends):
        o_ref[:, cut] = (mixed[ones_rows:, :] / mixed[0:1, :]).astype(jnp.bfloat16)


def attend(q_all, kv_all, pad_lengths):
    blocks, span, lanes = kv_all.shape
    total = q_all.shape[1]
    width = math.gcd(total, 2048)
    return pl.pallas_call(
        attend_kernel,
        out_shape=jax.ShapeDtypeStruct((HD, total), jnp.bfloat16),
        grid_spec=pltpu.PrefetchScalarGridSpec(
            num_scalar_prefetch=1,
            grid=(total // width,),
            in_specs=[
                pl.BlockSpec((HD, width), lambda i, lengths: (0, i)),
                pl.BlockSpec((blocks, span, lanes), lambda i, lengths: (0, 0, 0)),
            ],
            out_specs=pl.BlockSpec((HD, width), lambda i, lengths: (0, i)),
            scratch_shapes=[
                pltpu.VMEM(((blocks + 1) * span, lanes), jnp.bfloat16),
                pltpu.VMEM(((blocks + 1) * span, lanes), jnp.bfloat16),
                pltpu.VMEM((blocks + 1, HD + 16, span), jnp.bfloat16),
                pltpu.SMEM((1,), jnp.int32),
            ],
        ),
        compiler_params=pltpu.CompilerParams(
            dimension_semantics=("arbitrary",), vmem_limit_bytes=32 * 1024 * 1024
        ),
        name="attend",
    )(pad_lengths, q_all, kv_all)


def local(
    ring,
    sides,
    tokens,
    norm_attn,
    self_qkv,
    self_out,
    norm_ffn,
    ffn_in,
    ffn_out,
    norm_final,
    pad_lengths,
    targets,
    target_lengths,
    norm_cross,
    cross_query,
    cross_kv,
    cross_out,
):
    heads_here = self_qkv.shape[2] // HD
    share = ring // heads_here
    part = tokens.shape[0] // share
    q_got, kv_got, out_all, cross_q = scatter_heads(
        ring, share, sides, tokens, norm_attn, self_qkv, self_out, targets, norm_cross, cross_query
    )
    q_all = q_got.transpose(1, 0, 2).reshape(HD, ring * part)
    mixed_t = attend(q_all, kv_got, pad_lengths)
    back = mixed_t.reshape(HD, ring, part).transpose(1, 0, 2)
    return encoder_block(
        ring,
        share,
        sides,
        back,
        pad_lengths,
        target_lengths,
        tokens,
        norm_ffn,
        norm_final,
        self_out,
        out_all,
        ffn_in,
        ffn_out,
        cross_kv,
        cross_q,
        cross_out,
        targets,
    )


def solution(mesh):
    ring = mesh.shape["seq"]
    sides = mesh.shape["head"]
    placed = (
        P("seq", None),
        P(),
        P(None, None, "head"),
        P("head", None),
        P(),
        P(None, None, "head"),
        P("head", None),
        P(),
        P(),
        P(),
        P(),
        P(),
        P(None, "head"),
        P(None, None, "head"),
        P("head", None),
    )
    return jax.shard_map(
        functools.partial(local, ring, sides),
        mesh=mesh,
        in_specs=placed,
        out_specs=(P("seq", None), P()),
        check_vma=False,
    )
```

```python
import functools
import math

import jax
import jax.numpy as jnp
from jax import lax
from jax.experimental import pallas as pl
from jax.experimental.pallas import tpu as pltpu
from jax.sharding import PartitionSpec as P

HD = 64
TGT_LEN = 128

epsilon = 1e-06
masked_score = -1e30
scaling = HD ** (-0.5) * math.log2(math.e)
MESH = pl.DeviceIdType.MESH


def flip(index, other, count):
    result = 0
    weight = 1
    while weight < count:
        digit = other // weight if isinstance(other, int) else lax.div(other, weight)
        result = result + lax.rem(lax.div(index, weight) + digit, 2) * weight
        weight *= 2
    return result


def rows_at(start, size, align):
    return pl.ds(pl.multiple_of(start, align), size)


def greet_all(ring, sides):
    me = lax.axis_index("seq")
    here = lax.axis_index("head")
    barrier = pltpu.get_barrier_semaphore()

    def greet(i, carry):
        pl.semaphore_signal(
            barrier, inc=1, device_id={"seq": lax.rem(me + i, ring)}, device_id_type=MESH
        )
        return carry

    lax.fori_loop(1, ring, greet, 0)
    for k in range(1, sides):
        pl.semaphore_signal(
            barrier, inc=1, device_id={"head": lax.rem(here + k, sides)}, device_id_type=MESH
        )
    pl.semaphore_wait(barrier, ring - 1 + sides - 1)


def seq_copy(to, source, target, send_sem, recv_sem):
    return pltpu.make_async_remote_copy(
        src_ref=source,
        dst_ref=target,
        send_sem=send_sem,
        recv_sem=recv_sem,
        device_id={"seq": to},
        device_id_type=MESH,
    )


def side_copy(sides, k, source, target, send_sem, recv_sem):
    here = lax.axis_index("head")
    return pltpu.make_async_remote_copy(
        src_ref=source,
        dst_ref=target,
        send_sem=send_sem,
        recv_sem=recv_sem,
        device_id={"head": lax.rem(here + k, sides)},
        device_id_type=MESH,
    )


def in_hbm(array):
    return pltpu.with_memory_space_constraint(array, pltpu.HBM)


def norm_rows(values, gain):
    scale = lax.rsqrt(jnp.mean(values * values, axis=-1, keepdims=True) + epsilon)
    return values * scale * gain


def scatter_kernel(
    ring, share, sides, tokens_hbm, gain_hbm, qkv_hbm, out_hbm, targets_hbm, g_cross_hbm, w_cross_hbm,
    q_out, kv_out, out_all, cross_q,
    tokens, gain, qkv, targets, g_cross, w_cross, normed, q_in, kv_in,
    qs, qr, ks, kr, fs, fr, ls, os, ws, wr,
):
    me = lax.axis_index("seq")
    here = lax.axis_index("head")
    half = targets.shape[0]
    part = kv_in.shape[1]
    heads = ring // share
    slot = lax.rem(me, share)
    mine = rows_at(slot * part, part, part)
    loads = [
        pltpu.make_async_copy(source, target, ls.at[n])
        for n, (source, target) in enumerate(
            [
                (tokens_hbm, tokens),
                (gain_hbm, gain),
                (qkv_hbm.at[1], qkv.at[1]),
                (qkv_hbm.at[2], qkv.at[2]),
                (qkv_hbm.at[0], qkv.at[0]),
                (targets_hbm.at[rows_at(lax.rem(me, 2) * half, half, half)], targets),
                (g_cross_hbm, g_cross),
                (w_cross_hbm, w_cross),
            ]
        )
    ]
    for load in loads:
        load.start()
    greet_all(ring, sides)
    for k in range(1, sides):
        side_copy(sides, k, out_hbm, out_all.at[here], ws.at[k], wr.at[k]).start()

    def q_copy(i):
        to = flip(me, i, ring)
        return seq_copy(to, q_in.at[to], q_out.at[me], qs.at[i], qr.at[i])

    def kv_copy(i):
        to = flip(me, i, ring)
        rows = rows_at(lax.rem(to, share) * part, part, part)
        return seq_copy(to, kv_in.at[to], kv_out.at[me, rows], ks.at[i], kr.at[i])

    def forward(i, k):
        block = kv_out.at[flip(me, i, ring), mine]
        to = me - slot + lax.rem(slot + k, share)
        return seq_copy(to, block, block, fs.at[i, k], fr.at[i, k])

    def arrived(i, k):
        giver = me - slot + lax.rem(slot - k + share, share)
        rows = rows_at(lax.rem(giver, share) * part, part, part)
        block = kv_out.at[flip(giver, i, ring), rows]
        return seq_copy(giver, block, block, fs.at[i, k], fr.at[i, k])

    loads[0].wait()
    loads[1].wait()
    normed[...] = norm_rows(tokens[...].astype(jnp.float32), gain[...]).astype(jnp.bfloat16)
    loads[2].wait()
    loads[3].wait()
    keys = jnp.dot(normed[...], qkv[1], preferred_element_type=jnp.float32).astype(jnp.bfloat16)
    values = jnp.dot(normed[...], qkv[2], preferred_element_type=jnp.float32).astype(jnp.bfloat16)
    for h in range(heads):
        cut = slice(h * HD, (h + 1) * HD)
        both = jnp.concatenate([keys[:, cut], values[:, cut]], axis=1)
        for s in range(share):
            kv_in[h * share + s] = both[s * part : (s + 1) * part, :]

    span = ring // 2
    inner = lax.rem(lax.div(me, span) + lax.div(me, ring // 4), 2)

    def send_half(copy, far):
        def send(n, carry):
            step = far * span + n

            @pl.when(step > 0)
            def away():
                copy(step).start()

            return carry

        lax.fori_loop(0, span, send, 0)

    send_half(kv_copy, inner)
    own_kv = pltpu.make_async_copy(kv_in.at[me], kv_out.at[me, mine], os.at[1])
    own_kv.start()
    loads[4].wait()
    queries = (
        lax.dot_general(
            qkv[0], normed[...], (((0,), (1,)), ((), ())), preferred_element_type=jnp.float32
        )
        * scaling
    ).astype(jnp.bfloat16)
    for h in range(heads):
        for s in range(share):
            q_in[h * share + s] = queries[h * HD : (h + 1) * HD, s * part : (s + 1) * part]

    send_half(q_copy, 0)
    send_half(kv_copy, 1 - inner)
    send_half(q_copy, 1)
    own_q = pltpu.make_async_copy(q_in.at[me], q_out.at[me], os.at[0])
    own_q.start()
    own_kv.wait()
    for k in range(1, share):
        forward(0, k).start()
    for load in loads[5:]:
        load.wait()
    cross_normed = norm_rows(targets[...].astype(jnp.float32), g_cross[...]).astype(jnp.bfloat16)
    cross_q[...] = (
        jnp.dot(cross_normed, w_cross[...], preferred_element_type=jnp.float32) * scaling
    ).astype(jnp.bfloat16)

    def relay(i, carry):
        origin = flip(me, i, ring)
        seq_copy(origin, kv_in.at[0], kv_out.at[origin, mine], ks.at[i], kr.at[i]).wait_recv()
        for k in range(1, share):
            forward(i, k).start()
        return carry

    lax.fori_loop(1, ring, relay, 0)

    def finish(i, carry):
        origin = flip(me, i, ring)
        seq_copy(origin, q_in.at[0], q_out.at[origin], qs.at[i], qr.at[i]).wait_recv()
        q_copy(i).wait_send()
        kv_copy(i).wait_send()
        return carry

    lax.fori_loop(1, ring, finish, 0)

    def drain(i, carry):
        for k in range(1, share):
            arrived(i, k).wait_recv()
            forward(i, k).wait_send()
        return carry

    lax.fori_loop(0, ring, drain, 0)
    for k in range(1, sides):
        origin = lax.rem(here - k + sides, sides)
        side_copy(sides, k, out_hbm, out_all.at[origin], ws.at[k], wr.at[k]).wait()
    own_q.wait()


def scatter_heads(ring, share, sides, tokens, gain, qkv, w_out, targets, g_cross, w_cross):
    rows, width = tokens.shape
    heads = ring // share
    part = rows // share
    half = targets.shape[0] // 2
    bf16 = jnp.bfloat16
    vmem = pl.BlockSpec(memory_space=pltpu.VMEM)
    hbm = pl.BlockSpec(memory_space=pltpu.HBM)
    dma = pltpu.SemaphoreType.DMA
    return pl.pallas_call(
        functools.partial(scatter_kernel, ring, share, sides),
        out_shape=(
            jax.ShapeDtypeStruct((ring, HD, part), bf16),
            jax.ShapeDtypeStruct((ring, rows, 2 * HD), bf16),
            jax.ShapeDtypeStruct((sides,) + w_out.shape, bf16),
            jax.ShapeDtypeStruct((half, w_cross.shape[1]), bf16),
        ),
        in_specs=[hbm] * 7,
        out_specs=(vmem, vmem, hbm, vmem),
        scratch_shapes=[
            pltpu.VMEM((rows, width), bf16),
            pltpu.VMEM((1, width), jnp.float32),
            pltpu.VMEM(qkv.shape, bf16),
            pltpu.VMEM((half, width), bf16),
            pltpu.VMEM((1, width), jnp.float32),
            pltpu.VMEM(w_cross.shape, bf16),
            pltpu.VMEM((rows, width), bf16),
            pltpu.VMEM((heads * share, HD, part), bf16),
            pltpu.VMEM((heads * share, part, 2 * HD), bf16),
            dma((ring,)),
            dma((ring,)),
            dma((ring,)),
            dma((ring,)),
            dma((ring, share)),
            dma((ring, share)),
            dma((8,)),
            dma((2,)),
            dma((sides,)),
            dma((sides,)),
        ],
        compiler_params=pltpu.CompilerParams(
            collective_id=0, has_side_effects=True, vmem_limit_bytes=40 * 1024 * 1024
        ),
        name="scatter_heads",
    )(*map(in_hbm, (tokens, gain[None, :], qkv, w_out, targets, g_cross[None, :], w_cross)))


def block_kernel(
    ring, share, sides, x_in, pad_lengths, target_lengths, tokens_hbm, g_ffn_hbm, g_final_hbm,
    w_own_hbm, w_all_hbm, up_hbm, down_hbm, kv_hbm, cross_q, w_cross_hbm, targets_hbm,
    encoded, decoded,
    tokens, g_ffn, g_final, w_out, context, hidden, normed, parts, up, down, w_kv, w_cross, mine,
    cross_k, cross_v, mixed, stats, got, partial, incoming,
    ls, ss, rs, fs, fr, ps, pr, cs, cr, ms, mr, xs, xr, zs, zr, ws, wr, hs, hr,
):
    me = lax.axis_index("seq")
    here = lax.axis_index("head")
    heads = ring // share
    rows, width = tokens.shape
    slab = mine.shape[0]
    core = lax.rem(me, 2)
    mate = flip(me, 1, ring)

    def slab_start(owner):
        return (lax.rem(owner, 2) * (ring // 2) + lax.div(owner, 2)) * slab

    loads = [
        pltpu.make_async_copy(source, target, ls.at[n])
        for n, (source, target) in enumerate(
            [
                (tokens_hbm, tokens),
                (g_ffn_hbm, g_ffn),
                (w_own_hbm, w_out.at[here]),
                (up_hbm, up),
                (down_hbm, down),
                (g_final_hbm, g_final),
                (kv_hbm, w_kv),
                (w_cross_hbm, w_cross),
                (targets_hbm.at[rows_at(slab_start(me), slab, slab)], mine),
            ]
            + [
                (w_all_hbm.at[lax.rem(here + k, sides)], w_out.at[lax.rem(here + k, sides)])
                for k in range(1, sides)
            ]
        )
    ]
    for load in loads:
        load.start()

    def place(side, origin):
        return context.at[lax.rem(origin, share), side * heads + lax.div(origin, share)]

    own = pltpu.make_async_copy(x_in.at[me], place(here, me), ls.at[len(loads)])
    own.start()
    greet_all(ring, sides)

    def outgoing(i):
        to = flip(me, i, ring)
        return seq_copy(to, x_in.at[to], place(here, me), ss.at[i], rs.at[i])

    def relay(i, k):
        block = place(here, flip(me, i, ring))
        return side_copy(sides, k, block, block, fs.at[i, k], fr.at[i, k])

    def send(i, carry):
        outgoing(i).start()
        return carry

    lax.fori_loop(1, ring, send, 0)
    own.wait()
    for k in range(1, sides):
        relay(0, k).start()

    def pass_on(i, carry):
        origin = flip(me, i, ring)
        seq_copy(origin, x_in.at[0], place(here, origin), ss.at[i], rs.at[i]).wait_recv()
        for k in range(1, sides):
            relay(i, k).start()
        return carry

    lax.fori_loop(1, ring, pass_on, 0)

    def sent(i, carry):
        outgoing(i).wait_send()
        return carry

    lax.fori_loop(1, ring, sent, 0)

    def drain(i, carry):
        for k in range(1, sides):
            relay(i, k).wait_send()
            block = place(lax.rem(here - k + sides, sides), flip(me, i, ring))
            side_copy(sides, k, block, block, fs.at[i, k], fr.at[i, k]).wait_recv()
        return carry

    lax.fori_loop(0, ring, drain, 0)
    for load in loads[:3] + loads[9:]:
        load.wait()
    part = rows // share

    def project(c, carry):
        at = rows_at(c * part, part, part)
        flat = context[c].reshape(sides * heads * HD, part)
        total = tokens[at, :].astype(jnp.float32) + lax.dot_general(
            flat, w_out[...].reshape(sides * heads * HD, width), (((0,), (0,)), ((), ())),
            preferred_element_type=jnp.float32,
        )
        hidden[at, :] = total
        normed[at, :] = norm_rows(total, g_ffn[...]).astype(jnp.bfloat16)
        return carry

    lax.fori_loop(0, share, project, 0)
    for load in loads[3:6]:
        load.wait()
    chunk = math.gcd(rows, 128)
    chunks = rows // chunk

    def span(c):
        return rows_at(c * chunk, chunk, chunk)

    def swap(c, k, side):
        return side_copy(
            sides, k, parts.at[side, span(c)], parts.at[side, span(c)], ps.at[c, k], pr.at[c, k]
        )

    def feed(c, carry):
        x = normed[span(c), :]
        gate = jnp.dot(x, up[0], preferred_element_type=jnp.float32)
        lift = jnp.dot(x, up[1], preferred_element_type=jnp.float32)
        active = (jax.nn.gelu(gate, approximate=True) * lift).astype(jnp.bfloat16)
        parts[here, span(c), :] = jnp.dot(
            active, down[...], preferred_element_type=jnp.float32
        ).astype(jnp.bfloat16)
        for k in range(1, sides):
            swap(c, k, here).start()
        return carry

    lax.fori_loop(0, chunks, feed, 0)
    for load in loads[6:9]:
        load.wait()

    def pair_up(c, slot):
        return (
            seq_copy(mate, cross_k.at[slot, span(c)], cross_k.at[slot, span(c)], cs.at[c, 0], cr.at[c, 0]),
            seq_copy(mate, cross_v.at[slot, span(c)], cross_v.at[slot, span(c)], cs.at[c, 1], cr.at[c, 1]),
        )

    def close(c, carry):
        for k in range(1, sides):
            swap(c, k, here).wait_send()
            swap(c, k, lax.rem(here - k + sides, sides)).wait_recv()
        total = hidden[span(c), :]
        for side in range(sides):
            total = total + parts[side, span(c), :].astype(jnp.float32)
        done = norm_rows(total, g_final[...]).astype(jnp.bfloat16)
        encoded[span(c), :] = done
        cross_k[core, span(c), :] = jnp.dot(
            done, w_kv[0], preferred_element_type=jnp.float32
        ).astype(jnp.bfloat16)
        cross_v[core, span(c), :] = jnp.dot(
            done, w_kv[1], preferred_element_type=jnp.float32
        ).astype(jnp.bfloat16)
        for copy in pair_up(c, core):
            copy.start()
        return carry

    lax.fori_loop(0, chunks, close, 0)

    def paired(c, carry):
        for copy in pair_up(c, core):
            copy.wait_send()
        for copy in pair_up(c, 1 - core):
            copy.wait_recv()
        return carry

    lax.fori_loop(0, chunks, paired, 0)
    half = cross_q.shape[0]
    pairs = heads // 2
    peers = ring // 2
    position = lax.broadcasted_iota(jnp.int32, (2 * rows, 2 * HD), 0)
    first = me - core
    limit = jnp.where(position < rows, pad_lengths[first], rows + pad_lengths[first + 1])
    dead = jnp.where(position < limit, 0.0, masked_score).astype(jnp.bfloat16)
    lane = lax.broadcasted_iota(jnp.int32, (2 * rows, 2 * HD), 1)
    out_lane = lax.broadcasted_iota(jnp.int32, (half, 2 * HD), 1)
    ones = jnp.ones((2 * rows, 2 * HD), jnp.bfloat16)
    stats[...] = jnp.where(out_lane < HD, 0.0, jnp.where(out_lane < HD + heads, 1.0, 0.0))

    def to_peer(i, j):
        to = flip(me, 2 * j, ring)
        source = mixed.at[i, rows_at(lax.div(to, 2) * slab, slab, slab)]
        return seq_copy(to, source, got.at[j, i], ms.at[j, i], mr.at[j, i])

    def to_peers(i):
        def send_one(j, carry):
            to_peer(i, peers - j).start()
            return carry

        lax.fori_loop(1, peers, send_one, 0)

    def cross_pair(i, carry):
        cut = rows_at(i * 2 * HD, 2 * HD, 2 * HD)
        q_here = cross_q[:, cut]
        k_here = cross_k[:, :, cut].reshape(2 * rows, 2 * HD)
        v_here = cross_v[:, :, cut].reshape(2 * rows, 2 * HD)
        pieces = []
        seen = stats[...]
        for h in range(2):
            own = lane < HD if h == 0 else lane >= HD
            keys = jnp.where(own, k_here, dead)
            values = jnp.where(own, v_here, ones)
            pick = jnp.where(out_lane == (HD if h == 0 else 0), 1.0, 0.0).astype(jnp.bfloat16)
            queries = jnp.where(out_lane < HD if h == 0 else out_lane >= HD, q_here, pick)
            scores = lax.dot_general(
                queries, keys, (((1,), (1,)), ((), ())), preferred_element_type=jnp.float32
            )
            top = jnp.max(scores, axis=1, keepdims=True)
            weights = jnp.exp2(scores - top).astype(jnp.bfloat16)
            piece = jnp.dot(weights, values, preferred_element_type=jnp.float32)
            total = piece[:, 2 * HD - 1 :] if h == 0 else piece[:, :1]
            seen = jnp.where(
                out_lane == 2 * i + h, top, jnp.where(out_lane == HD + 2 * i + h, total, seen)
            )
            pieces.append(piece)
        stats[...] = seen
        mixed[i] = jnp.where(out_lane < HD, pieces[0], pieces[1]).astype(jnp.bfloat16)
        to_peers(i)
        return carry

    lax.fori_loop(0, pairs, cross_pair, 0)
    seen = stats[...]
    high = seen.astype(jnp.bfloat16).astype(jnp.float32)
    rest = seen - high
    middle = rest.astype(jnp.bfloat16).astype(jnp.float32)
    mixed[pairs] = (
        high + pltpu.roll(middle, heads, 1) + pltpu.roll(rest - middle, 2 * heads, 1)
    ).astype(jnp.bfloat16)
    to_peers(pairs)
    got[0] = mixed[:, rows_at(lax.div(me, 2) * slab, slab, slab), :]

    def collect(j, carry):
        for i in range(pairs + 1):
            copy = to_peer(i, j)
            copy.wait_send()
            copy.wait_recv()
        return carry

    lax.fori_loop(1, peers, collect, 0)
    packed = got[:, pairs].astype(jnp.float32).reshape(peers * slab, 2 * HD)
    seen = packed + pltpu.roll(packed, 2 * HD - heads, 1) + pltpu.roll(packed, 2 * HD - 2 * heads, 1)
    sums = pltpu.roll(seen, HD, 1).reshape(peers, slab, 2 * HD)
    seen = seen.reshape(peers, slab, 2 * HD)
    best = jnp.max(seen, axis=0, keepdims=True)
    grow = jnp.exp2(seen - best)
    weight_sum = jnp.sum(grow * sums, axis=0, keepdims=True)
    factor = (grow / weight_sum).reshape(peers * slab, 2 * HD)
    factor = jnp.where(lax.broadcasted_iota(jnp.int32, factor.shape, 1) < heads, factor, 0.0)
    column = lax.broadcasted_iota(jnp.int32, (2 * HD, heads * HD), 1)
    row = lax.broadcasted_iota(jnp.int32, (2 * HD, heads * HD), 0)
    spread = jnp.where((column >= row * HD) & (column < row * HD + HD), 1.0, 0.0)
    wide = jnp.dot(
        factor, spread, precision=lax.Precision.HIGHEST, preferred_element_type=jnp.float32
    ).reshape(peers, slab, heads * HD)
    merged = []
    for i in range(pairs):
        weighed = got[:, i].astype(jnp.float32) * wide[:, :, i * 2 * HD : (i + 1) * 2 * HD]
        merged.append(jnp.sum(weighed, axis=0).astype(jnp.bfloat16))
    product = jnp.dot(
        jnp.concatenate(merged, axis=1), w_cross[...], preferred_element_type=jnp.float32
    )
    partial[...] = product.astype(jnp.bfloat16)
    piece = incoming.shape[1]
    divided = piece < slab

    def piece_of(side):
        return rows_at(side * piece, piece, piece) if divided else pl.ds(0, piece)

    def exchange(k, side, origin):
        return side_copy(
            sides, k, partial.at[piece_of(side)], incoming.at[origin], xs.at[k], xr.at[k]
        )

    for k in range(1, sides):
        exchange(k, lax.rem(here + k, sides), here).start()
    incoming[here] = partial[piece_of(here), :]
    for k in range(1, sides):
        exchange(k, lax.rem(here + k, sides), here).wait_send()
        exchange(k, here, lax.rem(here - k + sides, sides)).wait_recv()
    total = incoming[0].astype(jnp.float32)
    for side in range(1, sides):
        total = total + incoming[side].astype(jnp.float32)

    def piece_start(owner, side):
        return slab_start(owner) + (side * piece if divided else 0)

    slot = piece_start(me, here) + lax.broadcasted_iota(jnp.int32, (piece, width), 0)
    limit = jnp.zeros((piece, width), jnp.int32)
    for n in range(target_lengths.shape[0]):
        begun = n * TGT_LEN
        limit = jnp.where(slot >= begun, begun + target_lengths[n], limit)
    decoded[rows_at(piece_start(me, here), piece, piece), :] = (
        mine[piece_of(here), :].astype(jnp.float32) + jnp.where(slot < limit, total, 0.0)
    ).astype(jnp.bfloat16)

    def block(owner, side):
        return decoded.at[rows_at(piece_start(owner, side), piece, piece)]

    def near(n):
        return flip(me, 2 * n, ring)

    def to_near(n, owner):
        return seq_copy(near(n), block(owner, here), block(owner, here), zs.at[n], zr.at[n])

    def to_side(k, n, side):
        return side_copy(
            sides, k, block(near(n), side), block(near(n), side), ws.at[k, n], wr.at[k, n]
        )

    def to_mate(k, n, owner):
        side = lax.rem(here - k + sides, sides)
        source = block(flip(owner, 2 * n, ring), side)
        return seq_copy(mate, source, source, hs.at[k, n], hr.at[k, n])

    given = range(1, sides) if divided else ()

    def share_out(n, carry):
        to_near(n, me).start()
        return carry

    lax.fori_loop(1, peers, share_out, 0)

    def pass_block(n):
        for k in given:
            to_side(k, n, here).start()
        to_mate(0, n, me).start()

    pass_block(0)

    def pass_along(n, carry):
        to_near(n, near(n)).wait_recv()
        pass_block(n)
        return carry

    lax.fori_loop(1, peers, pass_along, 0)

    def across(n, carry):
        for k in given:
            to_side(k, n, lax.rem(here - k + sides, sides)).wait_recv()
            to_mate(k, n, me).start()
        return carry

    lax.fori_loop(0, peers, across, 0)
    def spent(n, carry):
        to_near(n, me).wait_send()
        return carry

    lax.fori_loop(1, peers, spent, 0)

    def settle(n, carry):
        for k in given:
            to_side(k, n, here).wait_send()
        for k in (0, *given):
            to_mate(k, n, me).wait_send()
            to_mate(k, n, mate).wait_recv()
        return carry

    lax.fori_loop(0, peers, settle, 0)


def encoder_block(
    ring, share, sides, back, pad_lengths, target_lengths, tokens, g_ffn, g_final, w_own, w_all,
    ffn_in, ffn_out, w_kv, cross_q, w_cross, targets,
):
    rows, width = tokens.shape
    heads = ring // share
    chunks = rows // math.gcd(rows, 128)
    slab = targets.shape[0] // ring
    piece = slab // sides if slab % (16 * sides) == 0 else slab
    half, lanes = cross_q.shape
    pairs = heads // 2
    peers = ring // 2
    bf16 = jnp.bfloat16
    vmem = pl.BlockSpec(memory_space=pltpu.VMEM)
    smem = pl.BlockSpec(memory_space=pltpu.SMEM)
    hbm = pl.BlockSpec(memory_space=pltpu.HBM)
    dma = pltpu.SemaphoreType.DMA
    return pl.pallas_call(
        functools.partial(block_kernel, ring, share, sides),
        out_shape=(
            jax.ShapeDtypeStruct((rows, width), bf16),
            jax.ShapeDtypeStruct(targets.shape, bf16),
        ),
        in_specs=[vmem, smem, smem] + [hbm] * 8 + [vmem, hbm, hbm],
        out_specs=(vmem, vmem),
        scratch_shapes=[
            pltpu.VMEM((rows, width), bf16),
            pltpu.VMEM((1, width), jnp.float32),
            pltpu.VMEM((1, width), jnp.float32),
            pltpu.VMEM((sides,) + w_own.shape, bf16),
            pltpu.VMEM((share, sides * heads, HD, rows // share), bf16),
            pltpu.VMEM((rows, width), jnp.float32),
            pltpu.VMEM((rows, width), bf16),
            pltpu.VMEM((sides, rows, width), bf16),
            pltpu.VMEM(ffn_in.shape, bf16),
            pltpu.VMEM(ffn_out.shape, bf16),
            pltpu.VMEM(w_kv.shape, bf16),
            pltpu.VMEM(w_cross.shape, bf16),
            pltpu.VMEM((slab, width), bf16),
            pltpu.VMEM((2, rows, lanes), bf16),
            pltpu.VMEM((2, rows, lanes), bf16),
            pltpu.VMEM((pairs + 1, half, 2 * HD), bf16),
            pltpu.VMEM((half, 2 * HD), jnp.float32),
            pltpu.VMEM((peers, pairs + 1, slab, 2 * HD), bf16),
            pltpu.VMEM((slab, width), bf16),
            pltpu.VMEM((sides, piece, width), bf16),
            dma((9 + sides,)),
            dma((ring,)),
            dma((ring,)),
            dma((ring, sides)),
            dma((ring, sides)),
            dma((chunks, sides)),
            dma((chunks, sides)),
            dma((chunks, 2)),
            dma((chunks, 2)),
            dma((peers, pairs + 1)),
            dma((peers, pairs + 1)),
            dma((sides,)),
            dma((sides,)),
            dma((peers,)),
            dma((peers,)),
            dma((sides, peers)),
            dma((sides, peers)),
            dma((sides, peers)),
            dma((sides, peers)),
        ],
        compiler_params=pltpu.CompilerParams(
            collective_id=1, has_side_effects=True, vmem_limit_bytes=50 * 1024 * 1024
        ),
        name="encoder_block",
    )(
        back, pad_lengths, target_lengths, tokens, g_ffn[None, :], g_final[None, :], w_own, w_all,
        ffn_in, ffn_out, w_kv, cross_q, w_cross, targets,
    )


def attend_kernel(lengths, q_ref, kv_ref, o_ref, keys, values, flipped, count):
    blocks, span, lanes = kv_ref.shape
    tile = span
    queries = q_ref.shape[1]
    group = math.gcd(queries, 256)
    ones_rows = flipped.shape[1] - HD
    lane = lax.broadcasted_iota(jnp.int32, (span, lanes), 1)
    row = lax.broadcasted_iota(jnp.int32, (span, lanes), 0)

    @pl.when(pl.program_id(0) == 0)
    def pack():
        def place(j, start):
            block = kv_ref[j]
            dead = jnp.where(row < lengths[j], 0.0, masked_score).astype(jnp.bfloat16)
            at = pl.ds(pl.multiple_of(start, 16), span)
            keys[at, :] = jnp.where(lane < HD, block, dead)
            values[at, :] = jnp.where(lane < HD, jnp.ones_like(block), block)
            return start + ((lengths[j] + 15) // 16) * 16

        stop = lax.fori_loop(0, blocks, place, 0)
        at = pl.ds(pl.multiple_of(stop, 16), span)
        keys[at, :] = jnp.where(lane < HD, 0.0, masked_score).astype(jnp.bfloat16)
        values[at, :] = jnp.zeros((span, lanes), jnp.bfloat16)
        count[0] = (stop + tile - 1) // tile

        def flip(t, carry):
            at = pl.ds(pl.multiple_of(t * tile, tile), tile)
            flipped[t] = values[at, :].T[HD - ones_rows :, :]
            return carry

        lax.fori_loop(0, count[0], flip, 0)

    spare = lax.broadcasted_iota(jnp.int32, (HD, queries), 0)
    pick = jnp.where(spare == 0, 1.0, 0.0).astype(jnp.bfloat16)
    q_wide = jnp.concatenate([q_ref[...], pick], axis=0)
    cuts = [slice(g, g + group) for g in range(0, queries, group)]

    def step(t, state):
        at = pl.ds(pl.multiple_of(t * tile, tile), tile)
        keys_here = keys[at, :]
        values_here = flipped[t]
        all_scores = [
            jnp.dot(keys_here, q_wide[:, cut], preferred_element_type=jnp.float32) for cut in cuts
        ]
        updated = []
        for scores, (top, mixed) in zip(all_scores, state):
            new_top = jnp.maximum(top, jnp.max(scores, axis=0, keepdims=True))
            weights = jnp.exp2(scores - new_top).astype(jnp.bfloat16)
            part = jnp.dot(values_here, weights, preferred_element_type=jnp.float32)
            updated.append((new_top, mixed * jnp.exp2(top - new_top) + part))
        return tuple(updated)

    start = tuple(
        (
            jnp.full((1, group), masked_score, jnp.float32),
            jnp.zeros((ones_rows + HD, group), jnp.float32),
        )
        for cut in cuts
    )
    ends = lax.fori_loop(0, count[0], step, start)
    for cut, (top, mixed) in zip(cuts, ends):
        o_ref[:, cut] = (mixed[ones_rows:, :] / mixed[0:1, :]).astype(jnp.bfloat16)


def attend(q_all, kv_all, pad_lengths):
    blocks, span, lanes = kv_all.shape
    total = q_all.shape[1]
    width = math.gcd(total, 4096)
    return pl.pallas_call(
        attend_kernel,
        out_shape=jax.ShapeDtypeStruct((HD, total), jnp.bfloat16),
        grid_spec=pltpu.PrefetchScalarGridSpec(
            num_scalar_prefetch=1,
            grid=(total // width,),
            in_specs=[
                pl.BlockSpec((HD, width), lambda i, lengths: (0, i)),
                pl.BlockSpec((blocks, span, lanes), lambda i, lengths: (0, 0, 0)),
            ],
            out_specs=pl.BlockSpec((HD, width), lambda i, lengths: (0, i)),
            scratch_shapes=[
                pltpu.VMEM(((blocks + 1) * span, lanes), jnp.bfloat16),
                pltpu.VMEM(((blocks + 1) * span, lanes), jnp.bfloat16),
                pltpu.VMEM((blocks + 1, HD + 16, span), jnp.bfloat16),
                pltpu.SMEM((1,), jnp.int32),
            ],
        ),
        compiler_params=pltpu.CompilerParams(
            dimension_semantics=("arbitrary",), vmem_limit_bytes=32 * 1024 * 1024
        ),
        name="attend",
    )(pad_lengths, q_all, kv_all)


def local(
    ring,
    sides,
    tokens,
    norm_attn,
    self_qkv,
    self_out,
    norm_ffn,
    ffn_in,
    ffn_out,
    norm_final,
    pad_lengths,
    targets,
    target_lengths,
    norm_cross,
    cross_query,
    cross_kv,
    cross_out,
):
    heads_here = self_qkv.shape[2] // HD
    share = ring // heads_here
    part = tokens.shape[0] // share
    q_got, kv_got, out_all, cross_q = scatter_heads(
        ring, share, sides, tokens, norm_attn, self_qkv, self_out, targets, norm_cross, cross_query
    )
    q_all = q_got.transpose(1, 0, 2).reshape(HD, ring * part)
    mixed_t = attend(q_all, kv_got, pad_lengths)
    back = mixed_t.reshape(HD, ring, part).transpose(1, 0, 2)
    return encoder_block(
        ring,
        share,
        sides,
        back,
        pad_lengths,
        target_lengths,
        tokens,
        norm_ffn,
        norm_final,
        self_out,
        out_all,
        ffn_in,
        ffn_out,
        cross_kv,
        cross_q,
        cross_out,
        targets,
    )


def solution(mesh):
    ring = mesh.shape["seq"]
    sides = mesh.shape["head"]
    placed = (
        P("seq", None),
        P(),
        P(None, None, "head"),
        P("head", None),
        P(),
        P(None, None, "head"),
        P("head", None),
        P(),
        P(),
        P(),
        P(),
        P(),
        P(None, "head"),
        P(None, None, "head"),
        P("head", None),
    )
    return jax.shard_map(
        functools.partial(local, ring, sides),
        mesh=mesh,
        in_specs=placed,
        out_specs=(P("seq", None), P()),
        check_vma=False,
    )
```

```python
import functools
import math

import jax
import jax.numpy as jnp
from jax import lax
from jax.experimental import pallas as pl
from jax.experimental.pallas import tpu as pltpu
from jax.sharding import PartitionSpec as P

HD = 64
TGT_LEN = 128

epsilon = 1e-06
masked_score = -1e30
scaling = HD ** (-0.5) * math.log2(math.e)
MESH = pl.DeviceIdType.MESH


def flip(index, other, count):
    result = 0
    weight = 1
    while weight < count:
        digit = other // weight if isinstance(other, int) else lax.div(other, weight)
        result = result + lax.rem(lax.div(index, weight) + digit, 2) * weight
        weight *= 2
    return result


def rows_at(start, size, align):
    return pl.ds(pl.multiple_of(start, align), size)


def greet_all(ring, sides):
    me = lax.axis_index("seq")
    here = lax.axis_index("head")
    barrier = pltpu.get_barrier_semaphore()

    def greet(i, carry):
        pl.semaphore_signal(
            barrier, inc=1, device_id={"seq": lax.rem(me + i, ring)}, device_id_type=MESH
        )
        return carry

    lax.fori_loop(1, ring, greet, 0)
    for k in range(1, sides):
        pl.semaphore_signal(
            barrier, inc=1, device_id={"head": lax.rem(here + k, sides)}, device_id_type=MESH
        )
    pl.semaphore_wait(barrier, ring - 1 + sides - 1)


def seq_copy(to, source, target, send_sem, recv_sem):
    return pltpu.make_async_remote_copy(
        src_ref=source,
        dst_ref=target,
        send_sem=send_sem,
        recv_sem=recv_sem,
        device_id={"seq": to},
        device_id_type=MESH,
    )


def side_copy(sides, k, source, target, send_sem, recv_sem):
    here = lax.axis_index("head")
    return pltpu.make_async_remote_copy(
        src_ref=source,
        dst_ref=target,
        send_sem=send_sem,
        recv_sem=recv_sem,
        device_id={"head": lax.rem(here + k, sides)},
        device_id_type=MESH,
    )


def in_hbm(array):
    return pltpu.with_memory_space_constraint(array, pltpu.HBM)


def norm_rows(values, gain):
    scale = lax.rsqrt(jnp.mean(values * values, axis=-1, keepdims=True) + epsilon)
    return values * scale * gain


def scatter_kernel(
    ring, share, sides, tokens_hbm, gain_hbm, qkv_hbm, out_hbm, targets_hbm, g_cross_hbm, w_cross_hbm,
    w_kv_hbm, q_out, kv_out, out_all, w_kv_all, cross_q,
    tokens, gain, qkv, targets, g_cross, w_cross, normed, q_in, kv_in,
    qs, qr, ks, kr, fs, fr, ls, os, ws, wr, vs, vr,
):
    me = lax.axis_index("seq")
    here = lax.axis_index("head")
    half = targets.shape[0]
    part = kv_in.shape[1]
    heads = ring // share
    slot = lax.rem(me, share)
    mine = rows_at(slot * part, part, part)
    loads = [
        pltpu.make_async_copy(source, target, ls.at[n])
        for n, (source, target) in enumerate(
            [
                (tokens_hbm, tokens),
                (gain_hbm, gain),
                (qkv_hbm.at[1], qkv.at[1]),
                (qkv_hbm.at[2], qkv.at[2]),
                (qkv_hbm.at[0], qkv.at[0]),
                (targets_hbm.at[rows_at(lax.rem(me, 2) * half, half, half)], targets),
                (g_cross_hbm, g_cross),
                (w_cross_hbm, w_cross),
            ]
        )
    ]
    for load in loads:
        load.start()
    greet_all(ring, sides)
    core = lax.rem(me, 2)
    out_rows = out_hbm.shape[0] // 2

    def out_half(which):
        return rows_at(which * out_rows, out_rows, out_rows)

    def weight_copy(k, n, side):
        source = (out_hbm.at[out_half(core)], w_kv_hbm.at[core])[n]
        target = (out_all.at[side, out_half(core)], w_kv_all.at[side, core])[n]
        return side_copy(sides, k, source, target, ws.at[k, n], wr.at[k, n])

    def weight_forward(k, n, which):
        side = lax.rem(here - k + sides, sides)
        block = (out_all.at[side, out_half(which)], w_kv_all.at[side, which])[n]
        return seq_copy(flip(me, 1, ring), block, block, vs.at[k, n], vr.at[k, n])

    def query_copy(k, side):
        return side_copy(sides, k, cross_q.at[here], cross_q.at[side], ws.at[k, 2], wr.at[k, 2])

    for k in range(1, sides):
        for n in range(2):
            weight_copy(k, n, here).start()

    def q_copy(i):
        to = flip(me, i, ring)
        return seq_copy(to, q_in.at[to], q_out.at[me], qs.at[i], qr.at[i])

    def kv_copy(i):
        to = flip(me, i, ring)
        rows = rows_at(lax.rem(to, share) * part, part, part)
        return seq_copy(to, kv_in.at[to], kv_out.at[me, rows], ks.at[i], kr.at[i])

    def forward(i, k):
        block = kv_out.at[flip(me, i, ring), mine]
        to = me - slot + lax.rem(slot + k, share)
        return seq_copy(to, block, block, fs.at[i, k], fr.at[i, k])

    def arrived(i, k):
        giver = me - slot + lax.rem(slot - k + share, share)
        rows = rows_at(lax.rem(giver, share) * part, part, part)
        block = kv_out.at[flip(giver, i, ring), rows]
        return seq_copy(giver, block, block, fs.at[i, k], fr.at[i, k])

    loads[0].wait()
    loads[1].wait()
    normed[...] = norm_rows(tokens[...].astype(jnp.float32), gain[...]).astype(jnp.bfloat16)
    loads[2].wait()
    loads[3].wait()
    keys = jnp.dot(normed[...], qkv[1], preferred_element_type=jnp.float32).astype(jnp.bfloat16)
    values = jnp.dot(normed[...], qkv[2], preferred_element_type=jnp.float32).astype(jnp.bfloat16)
    for h in range(heads):
        cut = slice(h * HD, (h + 1) * HD)
        both = jnp.concatenate([keys[:, cut], values[:, cut]], axis=1)
        for s in range(share):
            kv_in[h * share + s] = both[s * part : (s + 1) * part, :]

    span = ring // 2
    inner = lax.rem(lax.div(me, span) + lax.div(me, ring // 4), 2)

    def send_half(copy, far):
        def send(n, carry):
            step = far * span + n

            @pl.when(step > 0)
            def away():
                copy(step).start()

            return carry

        lax.fori_loop(0, span, send, 0)

    send_half(kv_copy, inner)
    own_kv = pltpu.make_async_copy(kv_in.at[me], kv_out.at[me, mine], os.at[1])
    own_kv.start()
    loads[4].wait()
    queries = (
        lax.dot_general(
            qkv[0], normed[...], (((0,), (1,)), ((), ())), preferred_element_type=jnp.float32
        )
        * scaling
    ).astype(jnp.bfloat16)
    for h in range(heads):
        for s in range(share):
            q_in[h * share + s] = queries[h * HD : (h + 1) * HD, s * part : (s + 1) * part]

    send_half(q_copy, 0)
    send_half(kv_copy, 1 - inner)
    send_half(q_copy, 1)
    own_q = pltpu.make_async_copy(q_in.at[me], q_out.at[me], os.at[0])
    own_q.start()
    own_kv.wait()
    for k in range(1, share):
        forward(0, k).start()
    for load in loads[5:]:
        load.wait()
    cross_normed = norm_rows(targets[...].astype(jnp.float32), g_cross[...]).astype(jnp.bfloat16)
    cross_q[here] = (
        jnp.dot(cross_normed, w_cross[...], preferred_element_type=jnp.float32) * scaling
    ).astype(jnp.bfloat16)
    for k in range(1, sides):
        query_copy(k, here).start()

    def relay(i, carry):
        origin = flip(me, i, ring)
        seq_copy(origin, kv_in.at[0], kv_out.at[origin, mine], ks.at[i], kr.at[i]).wait_recv()
        for k in range(1, share):
            forward(i, k).start()
        return carry

    lax.fori_loop(1, ring, relay, 0)

    def finish(i, carry):
        origin = flip(me, i, ring)
        seq_copy(origin, q_in.at[0], q_out.at[origin], qs.at[i], qr.at[i]).wait_recv()
        q_copy(i).wait_send()
        kv_copy(i).wait_send()
        return carry

    lax.fori_loop(1, ring, finish, 0)

    def drain(i, carry):
        for k in range(1, share):
            arrived(i, k).wait_recv()
            forward(i, k).wait_send()
        return carry

    lax.fori_loop(0, ring, drain, 0)
    for n in range(2):
        for k in range(1, sides):
            weight_copy(k, n, lax.rem(here - k + sides, sides)).wait_recv()
            weight_forward(k, n, core).start()
    for k in range(1, sides):
        query_copy(k, lax.rem(here - k + sides, sides)).wait_recv()
        query_copy(k, here).wait_send()
        for n in range(2):
            weight_copy(k, n, here).wait_send()
            weight_forward(k, n, core).wait_send()
            weight_forward(k, n, 1 - core).wait_recv()
    own_q.wait()


def scatter_heads(ring, share, sides, tokens, gain, qkv, w_out, targets, g_cross, w_cross, w_kv):
    rows, width = tokens.shape
    heads = ring // share
    part = rows // share
    half = targets.shape[0] // 2
    bf16 = jnp.bfloat16
    vmem = pl.BlockSpec(memory_space=pltpu.VMEM)
    hbm = pl.BlockSpec(memory_space=pltpu.HBM)
    dma = pltpu.SemaphoreType.DMA
    return pl.pallas_call(
        functools.partial(scatter_kernel, ring, share, sides),
        out_shape=(
            jax.ShapeDtypeStruct((ring, HD, part), bf16),
            jax.ShapeDtypeStruct((ring, rows, 2 * HD), bf16),
            jax.ShapeDtypeStruct((sides,) + w_out.shape, bf16),
            jax.ShapeDtypeStruct((sides,) + w_kv.shape, bf16),
            jax.ShapeDtypeStruct((sides, half, w_cross.shape[1]), bf16),
        ),
        in_specs=[hbm] * 8,
        out_specs=(vmem, vmem, hbm, hbm, vmem),
        scratch_shapes=[
            pltpu.VMEM((rows, width), bf16),
            pltpu.VMEM((1, width), jnp.float32),
            pltpu.VMEM(qkv.shape, bf16),
            pltpu.VMEM((half, width), bf16),
            pltpu.VMEM((1, width), jnp.float32),
            pltpu.VMEM(w_cross.shape, bf16),
            pltpu.VMEM((rows, width), bf16),
            pltpu.VMEM((heads * share, HD, part), bf16),
            pltpu.VMEM((heads * share, part, 2 * HD), bf16),
            dma((ring,)),
            dma((ring,)),
            dma((ring,)),
            dma((ring,)),
            dma((ring, share)),
            dma((ring, share)),
            dma((8,)),
            dma((2,)),
            dma((sides, 3)),
            dma((sides, 3)),
            dma((sides, 2)),
            dma((sides, 2)),
        ],
        compiler_params=pltpu.CompilerParams(
            collective_id=0, has_side_effects=True, vmem_limit_bytes=40 * 1024 * 1024
        ),
        name="scatter_heads",
    )(*map(in_hbm, (tokens, gain[None, :], qkv, w_out, targets, g_cross[None, :], w_cross, w_kv)))


def block_kernel(
    ring, share, sides, x_in, pad_lengths, target_lengths, tokens_hbm, g_ffn_hbm, g_final_hbm,
    w_own_hbm, w_all_hbm, up_hbm, down_hbm, kv_hbm, kv_all_hbm, cross_q, w_cross_hbm, targets_hbm,
    encoded, decoded,
    tokens, g_ffn, g_final, w_out, context, hidden, normed, parts, landed, up, down, w_kv, w_cross,
    mine, cross_k, cross_v, given, taken, mixed, stats, got, partial, incoming,
    ls, ss, rs, fs, fr, ps, pr, cs, cr, es, er, ts, tr, ms, mr, xs, xr, zs, zr, ws, wr, hs, hr,
):
    me = lax.axis_index("seq")
    here = lax.axis_index("head")
    heads = ring // share
    rows, width = tokens.shape
    slab = mine.shape[0]
    core = lax.rem(me, 2)
    mate = flip(me, 1, ring)

    def slab_start(owner):
        return (lax.rem(owner, 2) * (ring // 2) + lax.div(owner, 2)) * slab

    loads = [
        pltpu.make_async_copy(source, target, ls.at[n])
        for n, (source, target) in enumerate(
            [
                (tokens_hbm, tokens),
                (g_ffn_hbm, g_ffn),
                (w_own_hbm, w_out.at[here]),
                (up_hbm, up),
                (down_hbm, down),
                (g_final_hbm, g_final),
                (kv_hbm, w_kv.at[here]),
                (w_cross_hbm, w_cross),
                (targets_hbm.at[rows_at(slab_start(me), slab, slab)], mine),
            ]
            + [
                (w_all_hbm.at[lax.rem(here + k, sides)], w_out.at[lax.rem(here + k, sides)])
                for k in range(1, sides)
            ]
            + [
                (kv_all_hbm.at[lax.rem(here + k, sides)], w_kv.at[lax.rem(here + k, sides)])
                for k in range(1, sides)
            ]
        )
    ]
    for load in loads:
        load.start()

    def place(side, origin):
        return context.at[lax.rem(origin, share), side * heads + lax.div(origin, share)]

    own = pltpu.make_async_copy(x_in.at[me], place(here, me), ls.at[len(loads)])
    own.start()
    greet_all(ring, sides)

    def outgoing(i):
        to = flip(me, i, ring)
        return seq_copy(to, x_in.at[to], place(here, me), ss.at[i], rs.at[i])

    def relay(i, k):
        block = place(here, flip(me, i, ring))
        return side_copy(sides, k, block, block, fs.at[i, k], fr.at[i, k])

    def send(i, carry):
        outgoing(i).start()
        return carry

    lax.fori_loop(1, ring, send, 0)
    own.wait()
    for k in range(1, sides):
        relay(0, k).start()

    def pass_on(i, carry):
        origin = flip(me, i, ring)
        seq_copy(origin, x_in.at[0], place(here, origin), ss.at[i], rs.at[i]).wait_recv()
        for k in range(1, sides):
            relay(i, k).start()
        return carry

    lax.fori_loop(1, ring, pass_on, 0)

    def sent(i, carry):
        outgoing(i).wait_send()
        return carry

    lax.fori_loop(1, ring, sent, 0)

    def drain(i, carry):
        for k in range(1, sides):
            relay(i, k).wait_send()
            block = place(lax.rem(here - k + sides, sides), flip(me, i, ring))
            side_copy(sides, k, block, block, fs.at[i, k], fr.at[i, k]).wait_recv()
        return carry

    lax.fori_loop(0, ring, drain, 0)
    for load in loads[:3] + loads[9 : 8 + sides]:
        load.wait()
    part = rows // share

    def project(c, carry):
        at = rows_at(c * part, part, part)
        flat = context[c].reshape(sides * heads * HD, part)
        total = tokens[at, :].astype(jnp.float32) + lax.dot_general(
            flat, w_out[...].reshape(sides * heads * HD, width), (((0,), (0,)), ((), ())),
            preferred_element_type=jnp.float32,
        )
        hidden[at, :] = total
        normed[at, :] = norm_rows(total, g_ffn[...]).astype(jnp.bfloat16)
        return carry

    lax.fori_loop(0, share, project, 0)
    for load in loads[3:6]:
        load.wait()
    lot = rows // sides
    chunk = math.gcd(lot, 128)
    chunks = lot // chunk

    def span(c):
        return rows_at(c * chunk, chunk, chunk)

    def hand_over(c, k, side, origin):
        return side_copy(
            sides, k, parts.at[side, span(c)], landed.at[origin, span(c)], ps.at[c, k], pr.at[c, k]
        )

    def feed(n, carry):
        k = lax.div(n, chunks) + 1
        c = lax.rem(n, chunks)
        side = lax.rem(here + k, sides)
        x = normed[rows_at(side * lot + c * chunk, chunk, chunk), :]
        gate = jnp.dot(x, up[0], preferred_element_type=jnp.float32)
        lift = jnp.dot(x, up[1], preferred_element_type=jnp.float32)
        active = (jax.nn.gelu(gate, approximate=True) * lift).astype(jnp.bfloat16)
        parts[side, span(c), :] = jnp.dot(
            active, down[...], preferred_element_type=jnp.float32
        ).astype(jnp.bfloat16)

        @pl.when(k < sides)
        def away():
            hand_over(c, k, side, here).start()

        return carry

    lax.fori_loop(0, sides * chunks, feed, 0)
    for load in loads[6:9] + loads[8 + sides :]:
        load.wait()

    def pair_up(c, slot):
        return [
            seq_copy(
                mate, whole.at[slot, side, span(c)], whole.at[slot, side, span(c)],
                cs.at[c, side, n], cr.at[c, side, n],
            )
            for n, whole in enumerate((cross_k, cross_v))
            for side in range(sides)
        ]

    def close(c, carry):
        at = rows_at(here * lot + c * chunk, chunk, chunk)
        total = hidden[at, :] + parts[here, span(c), :].astype(jnp.float32)
        for k in range(1, sides):
            origin = lax.rem(here - k + sides, sides)
            hand_over(c, k, lax.rem(here + k, sides), here).wait_send()
            hand_over(c, k, here, origin).wait_recv()
            total = total + landed[origin, span(c), :].astype(jnp.float32)
        done = norm_rows(total, g_final[...]).astype(jnp.bfloat16)
        encoded[at, :] = done
        for n, whole in enumerate((cross_k, cross_v)):
            for side in range(sides):
                whole[core, side, span(c), :] = jnp.dot(
                    done, w_kv[side, n], preferred_element_type=jnp.float32
                ).astype(jnp.bfloat16)
        for copy in pair_up(c, core):
            copy.start()
        return carry

    lax.fori_loop(0, chunks, close, 0)

    def paired(c, carry):
        for copy in pair_up(c, core):
            copy.wait_send()
        for copy in pair_up(c, 1 - core):
            copy.wait_recv()
        return carry

    lax.fori_loop(0, chunks, paired, 0)
    half = cross_q.shape[1]
    pairs = heads // 2
    peers = ring // 2
    position = lax.broadcasted_iota(jnp.int32, (2 * lot, 2 * HD), 0)
    first = me - core
    limit = jnp.where(position < lot, pad_lengths[first], lot + pad_lengths[first + 1]) - here * lot
    dead = jnp.where(position < limit, 0.0, masked_score).astype(jnp.bfloat16)
    lane = lax.broadcasted_iota(jnp.int32, (2 * lot, 2 * HD), 1)
    out_lane = lax.broadcasted_iota(jnp.int32, (half, 2 * HD), 1)
    ones = jnp.ones((2 * lot, 2 * HD), jnp.bfloat16)

    def pack(seen):
        high = seen.astype(jnp.bfloat16).astype(jnp.float32)
        rest = seen - high
        middle = rest.astype(jnp.bfloat16).astype(jnp.float32)
        return (
            high + pltpu.roll(middle, heads, 1) + pltpu.roll(rest - middle, 2 * heads, 1)
        ).astype(jnp.bfloat16)

    def unpack(packed):
        return (
            packed
            + pltpu.roll(packed, 2 * HD - heads, 1)
            + pltpu.roll(packed, 2 * HD - 2 * heads, 1)
        )

    def to_owner(k, i, side, origin):
        return side_copy(sides, k, given.at[side, i], taken.at[origin, i], ts.at[k, i], tr.at[k, i])

    def attend_side(k, carry):
        side = lax.rem(here + k, sides)
        stats[...] = jnp.where(out_lane < HD, 0.0, jnp.where(out_lane < HD + heads, 1.0, 0.0))

        def cross_pair(i, carry):
            cut = rows_at(i * 2 * HD, 2 * HD, 2 * HD)
            q_here = cross_q[side, :, cut]
            k_here = cross_k[:, side, :, cut].reshape(2 * lot, 2 * HD)
            v_here = cross_v[:, side, :, cut].reshape(2 * lot, 2 * HD)
            pieces = []
            seen = stats[...]
            for h in range(2):
                own = lane < HD if h == 0 else lane >= HD
                keys = jnp.where(own, k_here, dead)
                values = jnp.where(own, v_here, ones)
                pick = jnp.where(out_lane == (HD if h == 0 else 0), 1.0, 0.0).astype(jnp.bfloat16)
                queries = jnp.where(out_lane < HD if h == 0 else out_lane >= HD, q_here, pick)
                scores = lax.dot_general(
                    queries, keys, (((1,), (1,)), ((), ())), preferred_element_type=jnp.float32
                )
                top = jnp.max(scores, axis=1, keepdims=True)
                weights = jnp.exp2(scores - top).astype(jnp.bfloat16)
                piece = jnp.dot(weights, values, preferred_element_type=jnp.float32)
                total = piece[:, 2 * HD - 1 :] if h == 0 else piece[:, :1]
                seen = jnp.where(
                    out_lane == 2 * i + h, top, jnp.where(out_lane == HD + 2 * i + h, total, seen)
                )
                pieces.append(piece)
            stats[...] = seen
            given[side, i] = jnp.where(out_lane < HD, pieces[0], pieces[1]).astype(jnp.bfloat16)

            @pl.when(k < sides)
            def away():
                to_owner(k, i, side, here).start()

            return carry

        lax.fori_loop(0, pairs, cross_pair, 0)

        @pl.when(k < sides)
        def summary():
            given[side, pairs] = pack(stats[...])
            to_owner(k, pairs, side, here).start()

        return carry

    lax.fori_loop(1, sides + 1, attend_side, 0)

    def publish(k, side):
        rows_of = encoded.at[rows_at(side * lot, lot, lot)]
        return side_copy(sides, k, rows_of, rows_of, es.at[k], er.at[k])

    for k in range(1, sides):
        publish(k, here).start()
    for k in range(1, sides):
        for i in range(pairs + 1):
            to_owner(k, i, here, lax.rem(here - k + sides, sides)).wait_recv()
    origins = [lax.rem(here - k + sides, sides) for k in range(1, sides)]
    views = [stats[...]] + [unpack(taken[o, pairs].astype(jnp.float32)) for o in origins]
    best = functools.reduce(jnp.maximum, views)
    grows = [jnp.where(out_lane < heads, jnp.exp2(view - best), 0.0) for view in views]
    weight_sum = sum(grow * pltpu.roll(view, HD, 1) for grow, view in zip(grows, views))
    column = lax.broadcasted_iota(jnp.int32, (2 * HD, heads * HD), 1)
    row = lax.broadcasted_iota(jnp.int32, (2 * HD, heads * HD), 0)
    spread = jnp.where((column >= row * HD) & (column < row * HD + HD), 1.0, 0.0)
    scales = jnp.dot(
        jnp.concatenate(grows, axis=0), spread, precision=lax.Precision.HIGHEST,
        preferred_element_type=jnp.float32,
    )

    def to_peer(i, j):
        to = flip(me, 2 * j, ring)
        source = mixed.at[i, rows_at(lax.div(to, 2) * slab, slab, slab)]
        return seq_copy(to, source, got.at[j, i], ms.at[j, i], mr.at[j, i])

    def to_peers(i):
        def send_one(j, carry):
            to_peer(i, peers - j).start()
            return carry

        lax.fori_loop(1, peers, send_one, 0)

    for i in range(pairs):
        cut = slice(i * 2 * HD, (i + 1) * 2 * HD)
        total = given[here, i].astype(jnp.float32) * scales[:half, cut]
        for n, origin in enumerate(origins):
            scale = scales[(n + 1) * half : (n + 2) * half, cut]
            total = total + taken[origin, i].astype(jnp.float32) * scale
        mixed[i] = total.astype(jnp.bfloat16)
        to_peers(i)
    mixed[pairs] = pack(
        jnp.where(
            out_lane < heads,
            best,
            jnp.where(
                (out_lane >= HD) & (out_lane < HD + heads), pltpu.roll(weight_sum, HD, 1), 0.0
            ),
        )
    )
    to_peers(pairs)
    got[0] = mixed[:, rows_at(lax.div(me, 2) * slab, slab, slab), :]

    def collect(j, carry):
        for i in range(pairs + 1):
            copy = to_peer(i, j)
            copy.wait_send()
            copy.wait_recv()
        return carry

    lax.fori_loop(1, peers, collect, 0)
    seen = unpack(got[:, pairs].astype(jnp.float32).reshape(peers * slab, 2 * HD))
    sums = pltpu.roll(seen, HD, 1).reshape(peers, slab, 2 * HD)
    seen = seen.reshape(peers, slab, 2 * HD)
    best = jnp.max(seen, axis=0, keepdims=True)
    grow = jnp.exp2(seen - best)
    weight_sum = jnp.sum(grow * sums, axis=0, keepdims=True)
    factor = (grow / weight_sum).reshape(peers * slab, 2 * HD)
    factor = jnp.where(lax.broadcasted_iota(jnp.int32, factor.shape, 1) < heads, factor, 0.0)
    wide = jnp.dot(
        factor, spread, precision=lax.Precision.HIGHEST, preferred_element_type=jnp.float32
    ).reshape(peers, slab, heads * HD)
    merged = []
    for i in range(pairs):
        weighed = got[:, i].astype(jnp.float32) * wide[:, :, i * 2 * HD : (i + 1) * 2 * HD]
        merged.append(jnp.sum(weighed, axis=0).astype(jnp.bfloat16))
    product = jnp.dot(
        jnp.concatenate(merged, axis=1), w_cross[...], preferred_element_type=jnp.float32
    )
    partial[...] = product.astype(jnp.bfloat16)
    piece = incoming.shape[1]
    divided = piece < slab

    def piece_of(side):
        return rows_at(side * piece, piece, piece) if divided else pl.ds(0, piece)

    def exchange(k, side, origin):
        return side_copy(
            sides, k, partial.at[piece_of(side)], incoming.at[origin], xs.at[k], xr.at[k]
        )

    for k in range(1, sides):
        exchange(k, lax.rem(here + k, sides), here).start()
    incoming[here] = partial[piece_of(here), :]
    for k in range(1, sides):
        exchange(k, lax.rem(here + k, sides), here).wait_send()
        exchange(k, here, lax.rem(here - k + sides, sides)).wait_recv()
    total = incoming[0].astype(jnp.float32)
    for side in range(1, sides):
        total = total + incoming[side].astype(jnp.float32)

    def piece_start(owner, side):
        return slab_start(owner) + (side * piece if divided else 0)

    slot = piece_start(me, here) + lax.broadcasted_iota(jnp.int32, (piece, width), 0)
    limit = jnp.zeros((piece, width), jnp.int32)
    for n in range(target_lengths.shape[0]):
        begun = n * TGT_LEN
        limit = jnp.where(slot >= begun, begun + target_lengths[n], limit)
    decoded[rows_at(piece_start(me, here), piece, piece), :] = (
        mine[piece_of(here), :].astype(jnp.float32) + jnp.where(slot < limit, total, 0.0)
    ).astype(jnp.bfloat16)

    def block(owner, side):
        return decoded.at[rows_at(piece_start(owner, side), piece, piece)]

    def near(n):
        return flip(me, 2 * n, ring)

    def to_near(n, owner):
        return seq_copy(near(n), block(owner, here), block(owner, here), zs.at[n], zr.at[n])

    def to_side(k, n, side):
        return side_copy(
            sides, k, block(near(n), side), block(near(n), side), ws.at[k, n], wr.at[k, n]
        )

    def to_mate(k, n, owner):
        side = lax.rem(here - k + sides, sides)
        source = block(flip(owner, 2 * n, ring), side)
        return seq_copy(mate, source, source, hs.at[k, n], hr.at[k, n])

    beside = range(1, sides) if divided else ()

    def share_out(n, carry):
        to_near(n, me).start()
        return carry

    lax.fori_loop(1, peers, share_out, 0)

    def pass_block(n):
        for k in beside:
            to_side(k, n, here).start()
        to_mate(0, n, me).start()

    pass_block(0)

    def pass_along(n, carry):
        to_near(n, near(n)).wait_recv()
        pass_block(n)
        return carry

    lax.fori_loop(1, peers, pass_along, 0)

    def across(n, carry):
        for k in beside:
            to_side(k, n, lax.rem(here - k + sides, sides)).wait_recv()
            to_mate(k, n, me).start()
        return carry

    lax.fori_loop(0, peers, across, 0)
    def spent(n, carry):
        to_near(n, me).wait_send()
        return carry

    lax.fori_loop(1, peers, spent, 0)

    def settle(n, carry):
        for k in beside:
            to_side(k, n, here).wait_send()
        for k in (0, *beside):
            to_mate(k, n, me).wait_send()
            to_mate(k, n, mate).wait_recv()
        return carry

    lax.fori_loop(0, peers, settle, 0)
    for k in range(1, sides):
        publish(k, here).wait_send()
        publish(k, lax.rem(here - k + sides, sides)).wait_recv()
        for i in range(pairs + 1):
            to_owner(k, i, lax.rem(here + k, sides), here).wait_send()


def encoder_block(
    ring, share, sides, back, pad_lengths, target_lengths, tokens, g_ffn, g_final, w_own, w_all,
    ffn_in, ffn_out, w_kv, w_kv_all, cross_q, w_cross, targets,
):
    rows, width = tokens.shape
    heads = ring // share
    lot = rows // sides
    chunks = lot // math.gcd(lot, 128)
    slab = targets.shape[0] // ring
    piece = slab // sides if slab % (16 * sides) == 0 else slab
    half, lanes = cross_q.shape[1:]
    pairs = heads // 2
    peers = ring // 2
    bf16 = jnp.bfloat16
    vmem = pl.BlockSpec(memory_space=pltpu.VMEM)
    smem = pl.BlockSpec(memory_space=pltpu.SMEM)
    hbm = pl.BlockSpec(memory_space=pltpu.HBM)
    dma = pltpu.SemaphoreType.DMA
    return pl.pallas_call(
        functools.partial(block_kernel, ring, share, sides),
        out_shape=(
            jax.ShapeDtypeStruct((rows, width), bf16),
            jax.ShapeDtypeStruct(targets.shape, bf16),
        ),
        in_specs=[vmem, smem, smem] + [hbm] * 9 + [vmem, hbm, hbm],
        out_specs=(vmem, vmem),
        scratch_shapes=[
            pltpu.VMEM((rows, width), bf16),
            pltpu.VMEM((1, width), jnp.float32),
            pltpu.VMEM((1, width), jnp.float32),
            pltpu.VMEM((sides,) + w_own.shape, bf16),
            pltpu.VMEM((share, sides * heads, HD, rows // share), bf16),
            pltpu.VMEM((rows, width), jnp.float32),
            pltpu.VMEM((rows, width), bf16),
            pltpu.VMEM((sides, lot, width), bf16),
            pltpu.VMEM((sides, lot, width), bf16),
            pltpu.VMEM(ffn_in.shape, bf16),
            pltpu.VMEM(ffn_out.shape, bf16),
            pltpu.VMEM((sides,) + w_kv.shape, bf16),
            pltpu.VMEM(w_cross.shape, bf16),
            pltpu.VMEM((slab, width), bf16),
            pltpu.VMEM((2, sides, lot, lanes), bf16),
            pltpu.VMEM((2, sides, lot, lanes), bf16),
            pltpu.VMEM((sides, pairs + 1, half, 2 * HD), bf16),
            pltpu.VMEM((sides, pairs + 1, half, 2 * HD), bf16),
            pltpu.VMEM((pairs + 1, half, 2 * HD), bf16),
            pltpu.VMEM((half, 2 * HD), jnp.float32),
            pltpu.VMEM((peers, pairs + 1, slab, 2 * HD), bf16),
            pltpu.VMEM((slab, width), bf16),
            pltpu.VMEM((sides, piece, width), bf16),
            dma((8 + 2 * sides,)),
            dma((ring,)),
            dma((ring,)),
            dma((ring, sides)),
            dma((ring, sides)),
            dma((chunks, sides)),
            dma((chunks, sides)),
            dma((chunks, sides, 2)),
            dma((chunks, sides, 2)),
            dma((sides,)),
            dma((sides,)),
            dma((sides, pairs + 1)),
            dma((sides, pairs + 1)),
            dma((peers, pairs + 1)),
            dma((peers, pairs + 1)),
            dma((sides,)),
            dma((sides,)),
            dma((peers,)),
            dma((peers,)),
            dma((sides, peers)),
            dma((sides, peers)),
            dma((sides, peers)),
            dma((sides, peers)),
        ],
        compiler_params=pltpu.CompilerParams(
            collective_id=1, has_side_effects=True, vmem_limit_bytes=50 * 1024 * 1024
        ),
        name="encoder_block",
    )(
        back, pad_lengths, target_lengths, tokens, g_ffn[None, :], g_final[None, :], w_own, w_all,
        ffn_in, ffn_out, w_kv, w_kv_all, cross_q, w_cross, targets,
    )


def attend_kernel(lengths, q_ref, kv_ref, o_ref, keys, values, flipped, count):
    blocks, span, lanes = kv_ref.shape
    tile = span
    queries = q_ref.shape[1]
    group = math.gcd(queries, 256)
    ones_rows = flipped.shape[1] - HD
    lane = lax.broadcasted_iota(jnp.int32, (span, lanes), 1)
    row = lax.broadcasted_iota(jnp.int32, (span, lanes), 0)

    @pl.when(pl.program_id(0) == 0)
    def pack():
        def place(j, start):
            block = kv_ref[j]
            dead = jnp.where(row < lengths[j], 0.0, masked_score).astype(jnp.bfloat16)
            at = pl.ds(pl.multiple_of(start, 16), span)
            keys[at, :] = jnp.where(lane < HD, block, dead)
            values[at, :] = jnp.where(lane < HD, jnp.ones_like(block), block)
            return start + ((lengths[j] + 15) // 16) * 16

        stop = lax.fori_loop(0, blocks, place, 0)
        at = pl.ds(pl.multiple_of(stop, 16), span)
        keys[at, :] = jnp.where(lane < HD, 0.0, masked_score).astype(jnp.bfloat16)
        values[at, :] = jnp.zeros((span, lanes), jnp.bfloat16)
        count[0] = (stop + tile - 1) // tile

        def flip(t, carry):
            at = pl.ds(pl.multiple_of(t * tile, tile), tile)
            flipped[t] = values[at, :].T[HD - ones_rows :, :]
            return carry

        lax.fori_loop(0, count[0], flip, 0)

    spare = lax.broadcasted_iota(jnp.int32, (HD, queries), 0)
    pick = jnp.where(spare == 0, 1.0, 0.0).astype(jnp.bfloat16)
    q_wide = jnp.concatenate([q_ref[...], pick], axis=0)
    cuts = [slice(g, g + group) for g in range(0, queries, group)]

    def step(t, state):
        at = pl.ds(pl.multiple_of(t * tile, tile), tile)
        keys_here = keys[at, :]
        values_here = flipped[t]
        all_scores = [
            jnp.dot(keys_here, q_wide[:, cut], preferred_element_type=jnp.float32) for cut in cuts
        ]
        updated = []
        for scores, (top, mixed) in zip(all_scores, state):
            new_top = jnp.maximum(top, jnp.max(scores, axis=0, keepdims=True))
            weights = jnp.exp2(scores - new_top).astype(jnp.bfloat16)
            part = jnp.dot(values_here, weights, preferred_element_type=jnp.float32)
            updated.append((new_top, mixed * jnp.exp2(top - new_top) + part))
        return tuple(updated)

    start = tuple(
        (
            jnp.full((1, group), masked_score, jnp.float32),
            jnp.zeros((ones_rows + HD, group), jnp.float32),
        )
        for cut in cuts
    )
    ends = lax.fori_loop(0, count[0], step, start)
    for cut, (top, mixed) in zip(cuts, ends):
        o_ref[:, cut] = (mixed[ones_rows:, :] / mixed[0:1, :]).astype(jnp.bfloat16)


def attend(q_all, kv_all, pad_lengths):
    blocks, span, lanes = kv_all.shape
    total = q_all.shape[1]
    width = math.gcd(total, 4096)
    return pl.pallas_call(
        attend_kernel,
        out_shape=jax.ShapeDtypeStruct((HD, total), jnp.bfloat16),
        grid_spec=pltpu.PrefetchScalarGridSpec(
            num_scalar_prefetch=1,
            grid=(total // width,),
            in_specs=[
                pl.BlockSpec((HD, width), lambda i, lengths: (0, i)),
                pl.BlockSpec((blocks, span, lanes), lambda i, lengths: (0, 0, 0)),
            ],
            out_specs=pl.BlockSpec((HD, width), lambda i, lengths: (0, i)),
            scratch_shapes=[
                pltpu.VMEM(((blocks + 1) * span, lanes), jnp.bfloat16),
                pltpu.VMEM(((blocks + 1) * span, lanes), jnp.bfloat16),
                pltpu.VMEM((blocks + 1, HD + 16, span), jnp.bfloat16),
                pltpu.SMEM((1,), jnp.int32),
            ],
        ),
        compiler_params=pltpu.CompilerParams(
            dimension_semantics=("arbitrary",), vmem_limit_bytes=32 * 1024 * 1024
        ),
        name="attend",
    )(pad_lengths, q_all, kv_all)


def local(
    ring,
    sides,
    tokens,
    norm_attn,
    self_qkv,
    self_out,
    norm_ffn,
    ffn_in,
    ffn_out,
    norm_final,
    pad_lengths,
    targets,
    target_lengths,
    norm_cross,
    cross_query,
    cross_kv,
    cross_out,
):
    heads_here = self_qkv.shape[2] // HD
    share = ring // heads_here
    part = tokens.shape[0] // share
    q_got, kv_got, out_all, cross_kv_all, cross_q = scatter_heads(
        ring, share, sides, tokens, norm_attn, self_qkv, self_out, targets, norm_cross, cross_query,
        cross_kv,
    )
    q_all = q_got.transpose(1, 0, 2).reshape(HD, ring * part)
    mixed_t = attend(q_all, kv_got, pad_lengths)
    back = mixed_t.reshape(HD, ring, part).transpose(1, 0, 2)
    return encoder_block(
        ring,
        share,
        sides,
        back,
        pad_lengths,
        target_lengths,
        tokens,
        norm_ffn,
        norm_final,
        self_out,
        out_all,
        ffn_in,
        ffn_out,
        cross_kv,
        cross_kv_all,
        cross_q,
        cross_out,
        targets,
    )


def solution(mesh):
    ring = mesh.shape["seq"]
    sides = mesh.shape["head"]
    placed = (
        P("seq", None),
        P(),
        P(None, None, "head"),
        P("head", None),
        P(),
        P(None, None, "head"),
        P("head", None),
        P(),
        P(),
        P(),
        P(),
        P(),
        P(None, "head"),
        P(None, None, "head"),
        P("head", None),
    )
    return jax.shard_map(
        functools.partial(local, ring, sides),
        mesh=mesh,
        in_specs=placed,
        out_specs=(P("seq", None), P()),
        check_vma=False,
    )
```

```python
import functools
import math

import jax
import jax.numpy as jnp
from jax import lax
from jax.experimental import pallas as pl
from jax.experimental.pallas import tpu as pltpu
from jax.sharding import PartitionSpec as P

HD = 64
TGT_LEN = 128

epsilon = 1e-06
masked_score = -1e30
scaling = HD ** (-0.5) * math.log2(math.e)
MESH = pl.DeviceIdType.MESH


def flip(index, other, count):
    result = 0
    weight = 1
    while weight < count:
        digit = other // weight if isinstance(other, int) else lax.div(other, weight)
        result = result + lax.rem(lax.div(index, weight) + digit, 2) * weight
        weight *= 2
    return result


def rows_at(start, size, align):
    return pl.ds(pl.multiple_of(start, align), size)


def greet_all(ring, sides):
    me = lax.axis_index("seq")
    here = lax.axis_index("head")
    barrier = pltpu.get_barrier_semaphore()

    def greet(i, carry):
        pl.semaphore_signal(
            barrier, inc=1, device_id={"seq": lax.rem(me + i, ring)}, device_id_type=MESH
        )
        return carry

    lax.fori_loop(1, ring, greet, 0)
    for k in range(1, sides):
        pl.semaphore_signal(
            barrier, inc=1, device_id={"head": lax.rem(here + k, sides)}, device_id_type=MESH
        )
    pl.semaphore_wait(barrier, ring - 1 + sides - 1)


def seq_copy(to, source, target, send_sem, recv_sem):
    return pltpu.make_async_remote_copy(
        src_ref=source,
        dst_ref=target,
        send_sem=send_sem,
        recv_sem=recv_sem,
        device_id={"seq": to},
        device_id_type=MESH,
    )


def side_copy(sides, k, source, target, send_sem, recv_sem):
    here = lax.axis_index("head")
    return pltpu.make_async_remote_copy(
        src_ref=source,
        dst_ref=target,
        send_sem=send_sem,
        recv_sem=recv_sem,
        device_id={"head": lax.rem(here + k, sides)},
        device_id_type=MESH,
    )


def in_hbm(array):
    return pltpu.with_memory_space_constraint(array, pltpu.HBM)


def norm_rows(values, gain):
    scale = lax.rsqrt(jnp.mean(values * values, axis=-1, keepdims=True) + epsilon)
    return values * scale * gain


def scatter_kernel(
    ring, share, sides, tokens_hbm, gain_hbm, qkv_hbm, out_hbm, targets_hbm, g_cross_hbm, w_cross_hbm,
    q_out, kv_out, out_all, cross_q,
    tokens, gain, qkv, targets, g_cross, w_cross, normed, q_in, kv_in,
    qs, qr, ks, kr, fs, fr, ls, os, ws, wr,
):
    me = lax.axis_index("seq")
    here = lax.axis_index("head")
    half = targets.shape[0]
    part = kv_in.shape[1]
    heads = ring // share
    slot = lax.rem(me, share)
    mine = rows_at(slot * part, part, part)
    loads = [
        pltpu.make_async_copy(source, target, ls.at[n])
        for n, (source, target) in enumerate(
            [
                (tokens_hbm, tokens),
                (gain_hbm, gain),
                (qkv_hbm.at[1], qkv.at[1]),
                (qkv_hbm.at[2], qkv.at[2]),
                (qkv_hbm.at[0], qkv.at[0]),
                (targets_hbm.at[rows_at(lax.rem(me, 2) * half, half, half)], targets),
                (g_cross_hbm, g_cross),
                (w_cross_hbm, w_cross),
            ]
        )
    ]
    for load in loads:
        load.start()
    greet_all(ring, sides)
    for k in range(1, sides):
        side_copy(sides, k, out_hbm, out_all.at[here], ws.at[k], wr.at[k]).start()

    def q_copy(i):
        to = flip(me, i, ring)
        return seq_copy(to, q_in.at[to], q_out.at[me], qs.at[i], qr.at[i])

    def kv_copy(i):
        to = flip(me, i, ring)
        rows = rows_at(lax.rem(to, share) * part, part, part)
        return seq_copy(to, kv_in.at[to], kv_out.at[me, rows], ks.at[i], kr.at[i])

    def forward(i, k):
        block = kv_out.at[flip(me, i, ring), mine]
        to = me - slot + lax.rem(slot + k, share)
        return seq_copy(to, block, block, fs.at[i, k], fr.at[i, k])

    def arrived(i, k):
        giver = me - slot + lax.rem(slot - k + share, share)
        rows = rows_at(lax.rem(giver, share) * part, part, part)
        block = kv_out.at[flip(giver, i, ring), rows]
        return seq_copy(giver, block, block, fs.at[i, k], fr.at[i, k])

    loads[0].wait()
    loads[1].wait()
    normed[...] = norm_rows(tokens[...].astype(jnp.float32), gain[...]).astype(jnp.bfloat16)
    loads[2].wait()
    loads[3].wait()
    keys = jnp.dot(normed[...], qkv[1], preferred_element_type=jnp.float32).astype(jnp.bfloat16)
    values = jnp.dot(normed[...], qkv[2], preferred_element_type=jnp.float32).astype(jnp.bfloat16)
    for h in range(heads):
        cut = slice(h * HD, (h + 1) * HD)
        both = jnp.concatenate([keys[:, cut], values[:, cut]], axis=1)
        for s in range(share):
            kv_in[h * share + s] = both[s * part : (s + 1) * part, :]

    span = ring // 2
    inner = lax.rem(lax.div(me, span) + lax.div(me, ring // 4), 2)

    def send_half(copy, far):
        def send(n, carry):
            step = far * span + n

            @pl.when(step > 0)
            def away():
                copy(step).start()

            return carry

        lax.fori_loop(0, span, send, 0)

    send_half(kv_copy, inner)
    own_kv = pltpu.make_async_copy(kv_in.at[me], kv_out.at[me, mine], os.at[1])
    own_kv.start()
    loads[4].wait()
    queries = (
        lax.dot_general(
            qkv[0], normed[...], (((0,), (1,)), ((), ())), preferred_element_type=jnp.float32
        )
        * scaling
    ).astype(jnp.bfloat16)
    for h in range(heads):
        for s in range(share):
            q_in[h * share + s] = queries[h * HD : (h + 1) * HD, s * part : (s + 1) * part]

    send_half(q_copy, 0)
    send_half(kv_copy, 1 - inner)
    send_half(q_copy, 1)
    own_q = pltpu.make_async_copy(q_in.at[me], q_out.at[me], os.at[0])
    own_q.start()
    own_kv.wait()
    for k in range(1, share):
        forward(0, k).start()
    for load in loads[5:]:
        load.wait()
    cross_normed = norm_rows(targets[...].astype(jnp.float32), g_cross[...]).astype(jnp.bfloat16)
    cross_q[...] = (
        jnp.dot(cross_normed, w_cross[...], preferred_element_type=jnp.float32) * scaling
    ).astype(jnp.bfloat16)

    def relay(i, carry):
        origin = flip(me, i, ring)
        seq_copy(origin, kv_in.at[0], kv_out.at[origin, mine], ks.at[i], kr.at[i]).wait_recv()
        for k in range(1, share):
            forward(i, k).start()
        return carry

    lax.fori_loop(1, ring, relay, 0)

    def finish(i, carry):
        origin = flip(me, i, ring)
        seq_copy(origin, q_in.at[0], q_out.at[origin], qs.at[i], qr.at[i]).wait_recv()
        q_copy(i).wait_send()
        kv_copy(i).wait_send()
        return carry

    lax.fori_loop(1, ring, finish, 0)

    def drain(i, carry):
        for k in range(1, share):
            arrived(i, k).wait_recv()
            forward(i, k).wait_send()
        return carry

    lax.fori_loop(0, ring, drain, 0)
    for k in range(1, sides):
        origin = lax.rem(here - k + sides, sides)
        side_copy(sides, k, out_hbm, out_all.at[origin], ws.at[k], wr.at[k]).wait()
    own_q.wait()


def scatter_heads(ring, share, sides, tokens, gain, qkv, w_out, targets, g_cross, w_cross):
    rows, width = tokens.shape
    heads = ring // share
    part = rows // share
    half = targets.shape[0] // 2
    bf16 = jnp.bfloat16
    vmem = pl.BlockSpec(memory_space=pltpu.VMEM)
    hbm = pl.BlockSpec(memory_space=pltpu.HBM)
    dma = pltpu.SemaphoreType.DMA
    return pl.pallas_call(
        functools.partial(scatter_kernel, ring, share, sides),
        out_shape=(
            jax.ShapeDtypeStruct((ring, HD, part), bf16),
            jax.ShapeDtypeStruct((ring, rows, 2 * HD), bf16),
            jax.ShapeDtypeStruct((sides,) + w_out.shape, bf16),
            jax.ShapeDtypeStruct((half, w_cross.shape[1]), bf16),
        ),
        in_specs=[hbm] * 7,
        out_specs=(vmem, vmem, hbm, vmem),
        scratch_shapes=[
            pltpu.VMEM((rows, width), bf16),
            pltpu.VMEM((1, width), jnp.float32),
            pltpu.VMEM(qkv.shape, bf16),
            pltpu.VMEM((half, width), bf16),
            pltpu.VMEM((1, width), jnp.float32),
            pltpu.VMEM(w_cross.shape, bf16),
            pltpu.VMEM((rows, width), bf16),
            pltpu.VMEM((heads * share, HD, part), bf16),
            pltpu.VMEM((heads * share, part, 2 * HD), bf16),
            dma((ring,)),
            dma((ring,)),
            dma((ring,)),
            dma((ring,)),
            dma((ring, share)),
            dma((ring, share)),
            dma((8,)),
            dma((2,)),
            dma((sides,)),
            dma((sides,)),
        ],
        compiler_params=pltpu.CompilerParams(
            collective_id=0, has_side_effects=True, vmem_limit_bytes=40 * 1024 * 1024
        ),
        name="scatter_heads",
    )(*map(in_hbm, (tokens, gain[None, :], qkv, w_out, targets, g_cross[None, :], w_cross)))


def block_kernel(
    ring, share, sides, x_in, pad_lengths, target_lengths, tokens_hbm, g_ffn_hbm, g_final_hbm,
    w_own_hbm, w_all_hbm, up_hbm, down_hbm, kv_hbm, cross_q, w_cross_hbm, targets_hbm,
    encoded, decoded,
    tokens, g_ffn, g_final, w_out, context, hidden, normed, parts, up, down, w_kv, w_cross, mine,
    cross_k, cross_v, held, tops, mixed, stats, got, partial, incoming,
    ls, ss, rs, fs, fr, ps, pr, cs, cr, ms, mr, xs, xr, zs, zr, ws, wr, hs, hr,
):
    me = lax.axis_index("seq")
    here = lax.axis_index("head")
    heads = ring // share
    rows, width = tokens.shape
    slab = mine.shape[0]
    core = lax.rem(me, 2)
    mate = flip(me, 1, ring)

    def slab_start(owner):
        return (lax.rem(owner, 2) * (ring // 2) + lax.div(owner, 2)) * slab

    loads = [
        pltpu.make_async_copy(source, target, ls.at[n])
        for n, (source, target) in enumerate(
            [
                (tokens_hbm, tokens),
                (g_ffn_hbm, g_ffn),
                (w_own_hbm, w_out.at[here]),
                (up_hbm, up),
                (down_hbm, down),
                (g_final_hbm, g_final),
                (kv_hbm, w_kv),
                (w_cross_hbm, w_cross),
                (targets_hbm.at[rows_at(slab_start(me), slab, slab)], mine),
            ]
            + [
                (w_all_hbm.at[lax.rem(here + k, sides)], w_out.at[lax.rem(here + k, sides)])
                for k in range(1, sides)
            ]
        )
    ]
    for load in loads:
        load.start()

    def place(side, origin):
        return context.at[lax.rem(origin, share), side * heads + lax.div(origin, share)]

    own = pltpu.make_async_copy(x_in.at[me], place(here, me), ls.at[len(loads)])
    own.start()
    greet_all(ring, sides)

    def outgoing(i):
        to = flip(me, i, ring)
        return seq_copy(to, x_in.at[to], place(here, me), ss.at[i], rs.at[i])

    def relay(i, k):
        block = place(here, flip(me, i, ring))
        return side_copy(sides, k, block, block, fs.at[i, k], fr.at[i, k])

    def send(i, carry):
        outgoing(i).start()
        return carry

    lax.fori_loop(1, ring, send, 0)
    own.wait()
    for k in range(1, sides):
        relay(0, k).start()

    def pass_on(i, carry):
        origin = flip(me, i, ring)
        seq_copy(origin, x_in.at[0], place(here, origin), ss.at[i], rs.at[i]).wait_recv()
        for k in range(1, sides):
            relay(i, k).start()
        return carry

    lax.fori_loop(1, ring, pass_on, 0)

    def sent(i, carry):
        outgoing(i).wait_send()
        return carry

    lax.fori_loop(1, ring, sent, 0)

    def drain(i, carry):
        for k in range(1, sides):
            relay(i, k).wait_send()
            block = place(lax.rem(here - k + sides, sides), flip(me, i, ring))
            side_copy(sides, k, block, block, fs.at[i, k], fr.at[i, k]).wait_recv()
        return carry

    lax.fori_loop(0, ring, drain, 0)
    for load in loads[:3] + loads[9:]:
        load.wait()
    part = rows // share

    def project(c, carry):
        at = rows_at(c * part, part, part)
        flat = context[c].reshape(sides * heads * HD, part)
        total = tokens[at, :].astype(jnp.float32) + lax.dot_general(
            flat, w_out[...].reshape(sides * heads * HD, width), (((0,), (0,)), ((), ())),
            preferred_element_type=jnp.float32,
        )
        hidden[at, :] = total
        normed[at, :] = norm_rows(total, g_ffn[...]).astype(jnp.bfloat16)
        return carry

    lax.fori_loop(0, share, project, 0)
    for load in loads[3:6]:
        load.wait()
    chunk = math.gcd(rows, 128)
    chunks = rows // chunk

    def span(c):
        return rows_at(c * chunk, chunk, chunk)

    def swap(c, k, side):
        return side_copy(
            sides, k, parts.at[side, span(c)], parts.at[side, span(c)], ps.at[c, k], pr.at[c, k]
        )

    def feed(c, carry):
        x = normed[span(c), :]
        gate = jnp.dot(x, up[0], preferred_element_type=jnp.float32)
        lift = jnp.dot(x, up[1], preferred_element_type=jnp.float32)
        active = (jax.nn.gelu(gate, approximate=True) * lift).astype(jnp.bfloat16)
        parts[here, span(c), :] = jnp.dot(
            active, down[...], preferred_element_type=jnp.float32
        ).astype(jnp.bfloat16)
        for k in range(1, sides):
            swap(c, k, here).start()
        return carry

    lax.fori_loop(0, chunks, feed, 0)
    for load in loads[6:9]:
        load.wait()

    def pair_up(c, slot):
        return (
            seq_copy(mate, cross_k.at[slot, span(c)], cross_k.at[slot, span(c)], cs.at[c, 0], cr.at[c, 0]),
            seq_copy(mate, cross_v.at[slot, span(c)], cross_v.at[slot, span(c)], cs.at[c, 1], cr.at[c, 1]),
        )

    def close(c, carry):
        for k in range(1, sides):
            swap(c, k, here).wait_send()
            swap(c, k, lax.rem(here - k + sides, sides)).wait_recv()
        total = hidden[span(c), :]
        for side in range(sides):
            total = total + parts[side, span(c), :].astype(jnp.float32)
        done = norm_rows(total, g_final[...]).astype(jnp.bfloat16)
        encoded[span(c), :] = done
        cross_k[core, span(c), :] = jnp.dot(
            done, w_kv[0], preferred_element_type=jnp.float32
        ).astype(jnp.bfloat16)
        cross_v[core, span(c), :] = jnp.dot(
            done, w_kv[1], preferred_element_type=jnp.float32
        ).astype(jnp.bfloat16)
        for copy in pair_up(c, core):
            copy.start()
        return carry

    lax.fori_loop(0, chunks, close, 0)

    def paired(c, carry):
        for copy in pair_up(c, core):
            copy.wait_send()
        for copy in pair_up(c, 1 - core):
            copy.wait_recv()
        return carry

    lax.fori_loop(0, chunks, paired, 0)
    half = cross_q.shape[0]
    pairs = heads // 2
    peers = ring // 2
    position = lax.broadcasted_iota(jnp.int32, (2 * rows, 2 * HD), 0)
    first = me - core
    limit = jnp.where(position < rows, pad_lengths[first], rows + pad_lengths[first + 1])
    dead = jnp.where(position < limit, 0.0, masked_score).astype(jnp.bfloat16)
    lane = lax.broadcasted_iota(jnp.int32, (2 * rows, 2 * HD), 1)
    out_lane = lax.broadcasted_iota(jnp.int32, (half, 2 * HD), 1)
    ones = jnp.ones((2 * rows, 2 * HD), jnp.bfloat16)
    stats[...] = jnp.where(out_lane < HD, 0.0, jnp.where(out_lane < HD + heads, 1.0, 0.0))

    def to_peer(i, j):
        to = flip(me, 2 * j, ring)
        source = mixed.at[i, rows_at(lax.div(to, 2) * slab, slab, slab)]
        return seq_copy(to, source, got.at[j, i], ms.at[j, i], mr.at[j, i])

    def to_peers(i):
        def send_one(j, carry):
            to_peer(i, peers - j).start()
            return carry

        lax.fori_loop(1, peers, send_one, 0)

    def score(i, h):
        cut = rows_at(i * 2 * HD, 2 * HD, 2 * HD)
        keys = cross_k[:, :, cut].reshape(2 * rows, 2 * HD)
        keys = jnp.where(lane < HD if h == 0 else lane >= HD, keys, dead)
        pick = jnp.where(out_lane == (HD if h == 0 else 0), 1.0, 0.0).astype(jnp.bfloat16)
        queries = jnp.where(out_lane < HD if h == 0 else out_lane >= HD, cross_q[:, cut], pick)
        return lax.dot_general(
            queries, keys, (((1,), (1,)), ((), ())), preferred_element_type=jnp.float32
        )

    def hold(h, scores):
        held[h] = scores
        tops[h] = jnp.max(scores, axis=1, keepdims=True)

    for h in range(2):
        hold(h, score(0, h))

    def cross_pair(i, carry):
        following = [score(lax.rem(i + 1, pairs), h) for h in range(2)]
        v_here = cross_v[:, :, rows_at(i * 2 * HD, 2 * HD, 2 * HD)].reshape(2 * rows, 2 * HD)
        pieces = []
        seen = stats[...]
        for h in range(2):
            values = jnp.where(lane < HD if h == 0 else lane >= HD, v_here, ones)
            top = tops[h]
            weights = jnp.exp2(held[h] - top).astype(jnp.bfloat16)
            piece = jnp.dot(weights, values, preferred_element_type=jnp.float32)
            total = piece[:, 2 * HD - 1 :] if h == 0 else piece[:, :1]
            seen = jnp.where(
                out_lane == 2 * i + h, top, jnp.where(out_lane == HD + 2 * i + h, total, seen)
            )
            pieces.append(piece)
            hold(h, following[h])
        stats[...] = seen
        mixed[i] = jnp.where(out_lane < HD, pieces[0], pieces[1]).astype(jnp.bfloat16)
        to_peers(i)
        return carry

    lax.fori_loop(0, pairs, cross_pair, 0)
    seen = stats[...]
    high = seen.astype(jnp.bfloat16).astype(jnp.float32)
    rest = seen - high
    middle = rest.astype(jnp.bfloat16).astype(jnp.float32)
    mixed[pairs] = (
        high + pltpu.roll(middle, heads, 1) + pltpu.roll(rest - middle, 2 * heads, 1)
    ).astype(jnp.bfloat16)
    to_peers(pairs)
    got[0] = mixed[:, rows_at(lax.div(me, 2) * slab, slab, slab), :]

    def collect(j, carry):
        for i in range(pairs + 1):
            copy = to_peer(i, j)
            copy.wait_send()
            copy.wait_recv()
        return carry

    lax.fori_loop(1, peers, collect, 0)
    packed = got[:, pairs].astype(jnp.float32).reshape(peers * slab, 2 * HD)
    seen = packed + pltpu.roll(packed, 2 * HD - heads, 1) + pltpu.roll(packed, 2 * HD - 2 * heads, 1)
    sums = pltpu.roll(seen, HD, 1).reshape(peers, slab, 2 * HD)
    seen = seen.reshape(peers, slab, 2 * HD)
    best = jnp.max(seen, axis=0, keepdims=True)
    grow = jnp.exp2(seen - best)
    weight_sum = jnp.sum(grow * sums, axis=0, keepdims=True)
    factor = (grow / weight_sum).reshape(peers * slab, 2 * HD)
    factor = jnp.where(lax.broadcasted_iota(jnp.int32, factor.shape, 1) < heads, factor, 0.0)
    column = lax.broadcasted_iota(jnp.int32, (2 * HD, heads * HD), 1)
    row = lax.broadcasted_iota(jnp.int32, (2 * HD, heads * HD), 0)
    spread = jnp.where((column >= row * HD) & (column < row * HD + HD), 1.0, 0.0)
    spread = spread.astype(jnp.bfloat16)
    high = factor.astype(jnp.bfloat16)
    low = (factor - high.astype(jnp.float32)).astype(jnp.bfloat16)
    wide = jnp.dot(
        jnp.concatenate([high, low], axis=1), jnp.concatenate([spread, spread], axis=0),
        preferred_element_type=jnp.float32,
    ).reshape(peers, slab, heads * HD)
    merged = []
    for i in range(pairs):
        weighed = got[:, i].astype(jnp.float32) * wide[:, :, i * 2 * HD : (i + 1) * 2 * HD]
        merged.append(jnp.sum(weighed, axis=0).astype(jnp.bfloat16))
    product = jnp.dot(
        jnp.concatenate(merged, axis=1), w_cross[...], preferred_element_type=jnp.float32
    )
    partial[...] = product.astype(jnp.bfloat16)
    piece = incoming.shape[1]
    divided = piece < slab

    def piece_of(side):
        return rows_at(side * piece, piece, piece) if divided else pl.ds(0, piece)

    def exchange(k, side, origin):
        return side_copy(
            sides, k, partial.at[piece_of(side)], incoming.at[origin], xs.at[k], xr.at[k]
        )

    for k in range(1, sides):
        exchange(k, lax.rem(here + k, sides), here).start()
    incoming[here] = partial[piece_of(here), :]
    for k in range(1, sides):
        exchange(k, lax.rem(here + k, sides), here).wait_send()
        exchange(k, here, lax.rem(here - k + sides, sides)).wait_recv()
    total = incoming[0].astype(jnp.float32)
    for side in range(1, sides):
        total = total + incoming[side].astype(jnp.float32)

    def piece_start(owner, side):
        return slab_start(owner) + (side * piece if divided else 0)

    slot = piece_start(me, here) + lax.broadcasted_iota(jnp.int32, (piece, width), 0)
    limit = jnp.zeros((piece, width), jnp.int32)
    for n in range(target_lengths.shape[0]):
        begun = n * TGT_LEN
        limit = jnp.where(slot >= begun, begun + target_lengths[n], limit)
    decoded[rows_at(piece_start(me, here), piece, piece), :] = (
        mine[piece_of(here), :].astype(jnp.float32) + jnp.where(slot < limit, total, 0.0)
    ).astype(jnp.bfloat16)

    def block(owner, side):
        return decoded.at[rows_at(piece_start(owner, side), piece, piece)]

    def near(n):
        return flip(me, 2 * n, ring)

    def to_near(n, owner):
        return seq_copy(near(n), block(owner, here), block(owner, here), zs.at[n], zr.at[n])

    def to_side(k, n, side):
        return side_copy(
            sides, k, block(near(n), side), block(near(n), side), ws.at[k, n], wr.at[k, n]
        )

    def to_mate(k, n, owner):
        side = lax.rem(here - k + sides, sides)
        source = block(flip(owner, 2 * n, ring), side)
        return seq_copy(mate, source, source, hs.at[k, n], hr.at[k, n])

    given = range(1, sides) if divided else ()

    def share_out(n, carry):
        to_near(n, me).start()
        return carry

    lax.fori_loop(1, peers, share_out, 0)

    def pass_block(n):
        for k in given:
            to_side(k, n, here).start()
        to_mate(0, n, me).start()

    pass_block(0)

    def pass_along(n, carry):
        to_near(n, near(n)).wait_recv()
        pass_block(n)
        return carry

    lax.fori_loop(1, peers, pass_along, 0)

    def across(n, carry):
        for k in given:
            to_side(k, n, lax.rem(here - k + sides, sides)).wait_recv()
            to_mate(k, n, me).start()
        return carry

    lax.fori_loop(0, peers, across, 0)
    def spent(n, carry):
        to_near(n, me).wait_send()
        return carry

    lax.fori_loop(1, peers, spent, 0)

    def settle(n, carry):
        for k in given:
            to_side(k, n, here).wait_send()
        for k in (0, *given):
            to_mate(k, n, me).wait_send()
            to_mate(k, n, mate).wait_recv()
        return carry

    lax.fori_loop(0, peers, settle, 0)


def encoder_block(
    ring, share, sides, back, pad_lengths, target_lengths, tokens, g_ffn, g_final, w_own, w_all,
    ffn_in, ffn_out, w_kv, cross_q, w_cross, targets,
):
    rows, width = tokens.shape
    heads = ring // share
    chunks = rows // math.gcd(rows, 128)
    slab = targets.shape[0] // ring
    piece = slab // sides if slab % (16 * sides) == 0 else slab
    half, lanes = cross_q.shape
    pairs = heads // 2
    peers = ring // 2
    bf16 = jnp.bfloat16
    vmem = pl.BlockSpec(memory_space=pltpu.VMEM)
    smem = pl.BlockSpec(memory_space=pltpu.SMEM)
    hbm = pl.BlockSpec(memory_space=pltpu.HBM)
    dma = pltpu.SemaphoreType.DMA
    return pl.pallas_call(
        functools.partial(block_kernel, ring, share, sides),
        out_shape=(
            jax.ShapeDtypeStruct((rows, width), bf16),
            jax.ShapeDtypeStruct(targets.shape, bf16),
        ),
        in_specs=[vmem, smem, smem] + [hbm] * 8 + [vmem, hbm, hbm],
        out_specs=(vmem, vmem),
        scratch_shapes=[
            pltpu.VMEM((rows, width), bf16),
            pltpu.VMEM((1, width), jnp.float32),
            pltpu.VMEM((1, width), jnp.float32),
            pltpu.VMEM((sides,) + w_own.shape, bf16),
            pltpu.VMEM((share, sides * heads, HD, rows // share), bf16),
            pltpu.VMEM((rows, width), jnp.float32),
            pltpu.VMEM((rows, width), bf16),
            pltpu.VMEM((sides, rows, width), bf16),
            pltpu.VMEM(ffn_in.shape, bf16),
            pltpu.VMEM(ffn_out.shape, bf16),
            pltpu.VMEM(w_kv.shape, bf16),
            pltpu.VMEM(w_cross.shape, bf16),
            pltpu.VMEM((slab, width), bf16),
            pltpu.VMEM((2, rows, lanes), bf16),
            pltpu.VMEM((2, rows, lanes), bf16),
            pltpu.VMEM((2, half, 2 * rows), jnp.float32),
            pltpu.VMEM((2, half, 1), jnp.float32),
            pltpu.VMEM((pairs + 1, half, 2 * HD), bf16),
            pltpu.VMEM((half, 2 * HD), jnp.float32),
            pltpu.VMEM((peers, pairs + 1, slab, 2 * HD), bf16),
            pltpu.VMEM((slab, width), bf16),
            pltpu.VMEM((sides, piece, width), bf16),
            dma((9 + sides,)),
            dma((ring,)),
            dma((ring,)),
            dma((ring, sides)),
            dma((ring, sides)),
            dma((chunks, sides)),
            dma((chunks, sides)),
            dma((chunks, 2)),
            dma((chunks, 2)),
            dma((peers, pairs + 1)),
            dma((peers, pairs + 1)),
            dma((sides,)),
            dma((sides,)),
            dma((peers,)),
            dma((peers,)),
            dma((sides, peers)),
            dma((sides, peers)),
            dma((sides, peers)),
            dma((sides, peers)),
        ],
        compiler_params=pltpu.CompilerParams(
            collective_id=1, has_side_effects=True, vmem_limit_bytes=50 * 1024 * 1024
        ),
        name="encoder_block",
    )(
        back, pad_lengths, target_lengths, tokens, g_ffn[None, :], g_final[None, :], w_own, w_all,
        ffn_in, ffn_out, w_kv, cross_q, w_cross, targets,
    )


def attend_kernel(
    lengths, q_ref, kv_ref, o_ref, keys, values, flipped, count, held, tops, reach, mixed
):
    blocks, span, lanes = kv_ref.shape
    tile = span
    queries = q_ref.shape[1]
    group = math.gcd(queries, 256)
    ones_rows = flipped.shape[1] - HD
    lane = lax.broadcasted_iota(jnp.int32, (span, lanes), 1)
    row = lax.broadcasted_iota(jnp.int32, (span, lanes), 0)

    @pl.when(pl.program_id(0) == 0)
    def pack():
        def place(j, start):
            block = kv_ref[j]
            dead = jnp.where(row < lengths[j], 0.0, masked_score).astype(jnp.bfloat16)
            at = pl.ds(pl.multiple_of(start, 16), span)
            keys[at, :] = jnp.where(lane < HD, block, dead)
            values[at, :] = jnp.where(lane < HD, jnp.ones_like(block), block)
            return start + ((lengths[j] + 15) // 16) * 16

        stop = lax.fori_loop(0, blocks, place, 0)
        at = pl.ds(pl.multiple_of(stop, 16), span)
        keys[at, :] = jnp.where(lane < HD, 0.0, masked_score).astype(jnp.bfloat16)
        values[at, :] = jnp.zeros((span, lanes), jnp.bfloat16)
        count[0] = (stop + tile - 1) // tile

        def flip(t, carry):
            at = pl.ds(pl.multiple_of(t * tile, tile), tile)
            flipped[t] = values[at, :].T[HD - ones_rows :, :]
            return carry

        lax.fori_loop(0, count[0], flip, 0)

    spare = lax.broadcasted_iota(jnp.int32, (HD, queries), 0)
    pick = jnp.where(spare == 0, 1.0, 0.0).astype(jnp.bfloat16)
    q_wide = jnp.concatenate([q_ref[...], pick], axis=0)
    cuts = [slice(g, g + group) for g in range(0, queries, group)]

    def score(t, cut):
        at = pl.ds(pl.multiple_of(t * tile, tile), tile)
        return jnp.dot(keys[at, :], q_wide[:, cut], preferred_element_type=jnp.float32)

    def hold(n, scores):
        held[n] = scores
        tops[n] = jnp.max(scores, axis=0, keepdims=True)

    for n, cut in enumerate(cuts):
        hold(n, score(0, cut))
        reach[n] = jnp.full((1, group), masked_score, jnp.float32)
        mixed[n] = jnp.zeros((ones_rows + HD, group), jnp.float32)

    def step(t, carry):
        values_here = flipped[t]
        for n, cut in enumerate(cuts):
            following = score(t + 1, cut)
            top = jnp.maximum(reach[n], tops[n])
            weights = jnp.exp2(held[n] - top).astype(jnp.bfloat16)
            mixed[n] = mixed[n] * jnp.exp2(reach[n] - top) + jnp.dot(
                values_here, weights, preferred_element_type=jnp.float32
            )
            reach[n] = top
            hold(n, following)
        return carry

    lax.fori_loop(0, count[0], step, 0)
    for n, cut in enumerate(cuts):
        o_ref[:, cut] = (mixed[n, ones_rows:, :] / mixed[n, 0:1, :]).astype(jnp.bfloat16)


def attend(q_all, kv_all, pad_lengths):
    blocks, span, lanes = kv_all.shape
    total = q_all.shape[1]
    width = math.gcd(total, 4096)
    group = math.gcd(width, 256)
    groups = width // group
    return pl.pallas_call(
        attend_kernel,
        out_shape=jax.ShapeDtypeStruct((HD, total), jnp.bfloat16),
        grid_spec=pltpu.PrefetchScalarGridSpec(
            num_scalar_prefetch=1,
            grid=(total // width,),
            in_specs=[
                pl.BlockSpec((HD, width), lambda i, lengths: (0, i)),
                pl.BlockSpec((blocks, span, lanes), lambda i, lengths: (0, 0, 0)),
            ],
            out_specs=pl.BlockSpec((HD, width), lambda i, lengths: (0, i)),
            scratch_shapes=[
                pltpu.VMEM(((blocks + 1) * span, lanes), jnp.bfloat16),
                pltpu.VMEM(((blocks + 1) * span, lanes), jnp.bfloat16),
                pltpu.VMEM((blocks + 1, HD + 16, span), jnp.bfloat16),
                pltpu.SMEM((1,), jnp.int32),
                pltpu.VMEM((groups, span, group), jnp.float32),
                pltpu.VMEM((groups, 1, group), jnp.float32),
                pltpu.VMEM((groups, 1, group), jnp.float32),
                pltpu.VMEM((groups, HD + 16, group), jnp.float32),
            ],
        ),
        compiler_params=pltpu.CompilerParams(
            dimension_semantics=("arbitrary",), vmem_limit_bytes=32 * 1024 * 1024
        ),
        name="attend",
    )(pad_lengths, q_all, kv_all)


def local(
    ring,
    sides,
    tokens,
    norm_attn,
    self_qkv,
    self_out,
    norm_ffn,
    ffn_in,
    ffn_out,
    norm_final,
    pad_lengths,
    targets,
    target_lengths,
    norm_cross,
    cross_query,
    cross_kv,
    cross_out,
):
    heads_here = self_qkv.shape[2] // HD
    share = ring // heads_here
    part = tokens.shape[0] // share
    q_got, kv_got, out_all, cross_q = scatter_heads(
        ring, share, sides, tokens, norm_attn, self_qkv, self_out, targets, norm_cross, cross_query
    )
    q_all = q_got.transpose(1, 0, 2).reshape(HD, ring * part)
    mixed_t = attend(q_all, kv_got, pad_lengths)
    back = mixed_t.reshape(HD, ring, part).transpose(1, 0, 2)
    return encoder_block(
        ring,
        share,
        sides,
        back,
        pad_lengths,
        target_lengths,
        tokens,
        norm_ffn,
        norm_final,
        self_out,
        out_all,
        ffn_in,
        ffn_out,
        cross_kv,
        cross_q,
        cross_out,
        targets,
    )


def solution(mesh):
    ring = mesh.shape["seq"]
    sides = mesh.shape["head"]
    placed = (
        P("seq", None),
        P(),
        P(None, None, "head"),
        P("head", None),
        P(),
        P(None, None, "head"),
        P("head", None),
        P(),
        P(),
        P(),
        P(),
        P(),
        P(None, "head"),
        P(None, None, "head"),
        P("head", None),
    )
    return jax.shard_map(
        functools.partial(local, ring, sides),
        mesh=mesh,
        in_specs=placed,
        out_specs=(P("seq", None), P()),
        check_vma=False,
    )
```

```python
import functools
import math

import jax
import jax.numpy as jnp
from jax import lax
from jax.experimental import pallas as pl
from jax.experimental.pallas import tpu as pltpu
from jax.sharding import PartitionSpec as P

HD = 64
TGT_LEN = 128

epsilon = 1e-06
masked_score = -1e30
scaling = HD ** (-0.5) * math.log2(math.e)
MESH = pl.DeviceIdType.MESH


def flip(index, other, count):
    result = 0
    weight = 1
    while weight < count:
        digit = other // weight if isinstance(other, int) else lax.div(other, weight)
        result = result + lax.rem(lax.div(index, weight) + digit, 2) * weight
        weight *= 2
    return result


def rows_at(start, size, align):
    return pl.ds(pl.multiple_of(start, align), size)


def greet_all(ring, sides):
    me = lax.axis_index("seq")
    here = lax.axis_index("head")
    barrier = pltpu.get_barrier_semaphore()

    def greet(i, carry):
        pl.semaphore_signal(
            barrier, inc=1, device_id={"seq": lax.rem(me + i, ring)}, device_id_type=MESH
        )
        return carry

    lax.fori_loop(1, ring, greet, 0)
    for k in range(1, sides):
        pl.semaphore_signal(
            barrier, inc=1, device_id={"head": lax.rem(here + k, sides)}, device_id_type=MESH
        )
    pl.semaphore_wait(barrier, ring - 1 + sides - 1)


def seq_copy(to, source, target, send_sem, recv_sem):
    return pltpu.make_async_remote_copy(
        src_ref=source,
        dst_ref=target,
        send_sem=send_sem,
        recv_sem=recv_sem,
        device_id={"seq": to},
        device_id_type=MESH,
    )


def side_copy(sides, k, source, target, send_sem, recv_sem):
    here = lax.axis_index("head")
    return pltpu.make_async_remote_copy(
        src_ref=source,
        dst_ref=target,
        send_sem=send_sem,
        recv_sem=recv_sem,
        device_id={"head": lax.rem(here + k, sides)},
        device_id_type=MESH,
    )


def in_hbm(array):
    return pltpu.with_memory_space_constraint(array, pltpu.HBM)


def norm_rows(values, gain):
    scale = lax.rsqrt(jnp.mean(values * values, axis=-1, keepdims=True) + epsilon)
    return values * scale * gain


def scatter_kernel(
    ring, share, sides, tokens_hbm, gain_hbm, qkv_hbm, out_hbm, targets_hbm, g_cross_hbm, w_cross_hbm,
    q_out, kv_out, out_all, cross_q,
    tokens, gain, qkv, targets, g_cross, w_cross, normed, q_in, kv_in,
    qs, qr, ks, kr, fs, fr, ls, os, ws, wr,
):
    me = lax.axis_index("seq")
    here = lax.axis_index("head")
    half = targets.shape[0]
    part = kv_in.shape[1]
    heads = ring // share
    slot = lax.rem(me, share)
    mine = rows_at(slot * part, part, part)
    loads = [
        pltpu.make_async_copy(source, target, ls.at[n])
        for n, (source, target) in enumerate(
            [
                (tokens_hbm, tokens),
                (gain_hbm, gain),
                (qkv_hbm.at[1], qkv.at[1]),
                (qkv_hbm.at[2], qkv.at[2]),
                (qkv_hbm.at[0], qkv.at[0]),
                (targets_hbm.at[rows_at(lax.rem(me, 2) * half, half, half)], targets),
                (g_cross_hbm, g_cross),
                (w_cross_hbm, w_cross),
            ]
        )
    ]
    for load in loads:
        load.start()
    greet_all(ring, sides)
    for k in range(1, sides):
        side_copy(sides, k, out_hbm, out_all.at[here], ws.at[k], wr.at[k]).start()

    def q_copy(i):
        to = flip(me, i, ring)
        return seq_copy(to, q_in.at[to], q_out.at[me], qs.at[i], qr.at[i])

    def kv_copy(i):
        to = flip(me, i, ring)
        rows = rows_at(lax.rem(to, share) * part, part, part)
        return seq_copy(to, kv_in.at[to], kv_out.at[me, rows], ks.at[i], kr.at[i])

    def forward(i, k):
        block = kv_out.at[flip(me, i, ring), mine]
        to = me - slot + lax.rem(slot + k, share)
        return seq_copy(to, block, block, fs.at[i, k], fr.at[i, k])

    def arrived(i, k):
        giver = me - slot + lax.rem(slot - k + share, share)
        rows = rows_at(lax.rem(giver, share) * part, part, part)
        block = kv_out.at[flip(giver, i, ring), rows]
        return seq_copy(giver, block, block, fs.at[i, k], fr.at[i, k])

    loads[0].wait()
    loads[1].wait()
    normed[...] = norm_rows(tokens[...].astype(jnp.float32), gain[...]).astype(jnp.bfloat16)
    loads[2].wait()
    loads[3].wait()
    keys = jnp.dot(normed[...], qkv[1], preferred_element_type=jnp.float32).astype(jnp.bfloat16)
    values = jnp.dot(normed[...], qkv[2], preferred_element_type=jnp.float32).astype(jnp.bfloat16)
    for h in range(heads):
        cut = slice(h * HD, (h + 1) * HD)
        both = jnp.concatenate([keys[:, cut], values[:, cut]], axis=1)
        for s in range(share):
            kv_in[h * share + s] = both[s * part : (s + 1) * part, :]

    span = ring // 2
    inner = lax.rem(lax.div(me, span) + lax.div(me, ring // 4), 2)

    def send_half(copy, far):
        def send(n, carry):
            step = far * span + n

            @pl.when(step > 0)
            def away():
                copy(step).start()

            return carry

        lax.fori_loop(0, span, send, 0)

    send_half(kv_copy, inner)
    own_kv = pltpu.make_async_copy(kv_in.at[me], kv_out.at[me, mine], os.at[1])
    own_kv.start()
    loads[4].wait()
    queries = (
        lax.dot_general(
            qkv[0], normed[...], (((0,), (1,)), ((), ())), preferred_element_type=jnp.float32
        )
        * scaling
    ).astype(jnp.bfloat16)
    for h in range(heads):
        for s in range(share):
            q_in[h * share + s] = queries[h * HD : (h + 1) * HD, s * part : (s + 1) * part]

    send_half(q_copy, 0)
    send_half(kv_copy, 1 - inner)
    send_half(q_copy, 1)
    own_q = pltpu.make_async_copy(q_in.at[me], q_out.at[me], os.at[0])
    own_q.start()
    own_kv.wait()
    for k in range(1, share):
        forward(0, k).start()
    for load in loads[5:]:
        load.wait()
    cross_normed = norm_rows(targets[...].astype(jnp.float32), g_cross[...]).astype(jnp.bfloat16)
    cross_q[...] = (
        jnp.dot(cross_normed, w_cross[...], preferred_element_type=jnp.float32) * scaling
    ).astype(jnp.bfloat16)

    def relay(i, carry):
        origin = flip(me, i, ring)
        seq_copy(origin, kv_in.at[0], kv_out.at[origin, mine], ks.at[i], kr.at[i]).wait_recv()
        for k in range(1, share):
            forward(i, k).start()
        return carry

    lax.fori_loop(1, ring, relay, 0)

    def finish(i, carry):
        origin = flip(me, i, ring)
        seq_copy(origin, q_in.at[0], q_out.at[origin], qs.at[i], qr.at[i]).wait_recv()
        q_copy(i).wait_send()
        kv_copy(i).wait_send()
        return carry

    lax.fori_loop(1, ring, finish, 0)

    def drain(i, carry):
        for k in range(1, share):
            arrived(i, k).wait_recv()
            forward(i, k).wait_send()
        return carry

    lax.fori_loop(0, ring, drain, 0)
    for k in range(1, sides):
        origin = lax.rem(here - k + sides, sides)
        side_copy(sides, k, out_hbm, out_all.at[origin], ws.at[k], wr.at[k]).wait()
    own_q.wait()


def scatter_heads(ring, share, sides, tokens, gain, qkv, w_out, targets, g_cross, w_cross):
    rows, width = tokens.shape
    heads = ring // share
    part = rows // share
    half = targets.shape[0] // 2
    bf16 = jnp.bfloat16
    vmem = pl.BlockSpec(memory_space=pltpu.VMEM)
    hbm = pl.BlockSpec(memory_space=pltpu.HBM)
    dma = pltpu.SemaphoreType.DMA
    return pl.pallas_call(
        functools.partial(scatter_kernel, ring, share, sides),
        out_shape=(
            jax.ShapeDtypeStruct((ring, HD, part), bf16),
            jax.ShapeDtypeStruct((ring, rows, 2 * HD), bf16),
            jax.ShapeDtypeStruct((sides,) + w_out.shape, bf16),
            jax.ShapeDtypeStruct((half, w_cross.shape[1]), bf16),
        ),
        in_specs=[hbm] * 7,
        out_specs=(vmem, vmem, hbm, vmem),
        scratch_shapes=[
            pltpu.VMEM((rows, width), bf16),
            pltpu.VMEM((1, width), jnp.float32),
            pltpu.VMEM(qkv.shape, bf16),
            pltpu.VMEM((half, width), bf16),
            pltpu.VMEM((1, width), jnp.float32),
            pltpu.VMEM(w_cross.shape, bf16),
            pltpu.VMEM((rows, width), bf16),
            pltpu.VMEM((heads * share, HD, part), bf16),
            pltpu.VMEM((heads * share, part, 2 * HD), bf16),
            dma((ring,)),
            dma((ring,)),
            dma((ring,)),
            dma((ring,)),
            dma((ring, share)),
            dma((ring, share)),
            dma((8,)),
            dma((2,)),
            dma((sides,)),
            dma((sides,)),
        ],
        compiler_params=pltpu.CompilerParams(
            collective_id=0, has_side_effects=True, vmem_limit_bytes=40 * 1024 * 1024
        ),
        name="scatter_heads",
    )(*map(in_hbm, (tokens, gain[None, :], qkv, w_out, targets, g_cross[None, :], w_cross)))


def block_kernel(
    ring, share, sides, x_in, pad_lengths, target_lengths, tokens_hbm, g_ffn_hbm, g_final_hbm,
    w_own_hbm, w_all_hbm, up_hbm, down_hbm, kv_hbm, cross_q, w_cross_hbm, targets_hbm,
    encoded, decoded,
    tokens, g_ffn, g_final, w_out, context, hidden, normed, parts, up, down, w_kv, w_cross, mine,
    cross_k, cross_v, held, tops, mixed, stats, got, partial, incoming,
    ls, ss, rs, fs, fr, ps, pr, cs, cr, ms, mr, xs, xr, zs, zr, ws, wr, hs, hr,
):
    me = lax.axis_index("seq")
    here = lax.axis_index("head")
    heads = ring // share
    rows, width = tokens.shape
    slab = mine.shape[0]
    core = lax.rem(me, 2)
    mate = flip(me, 1, ring)

    def slab_start(owner):
        return (lax.rem(owner, 2) * (ring // 2) + lax.div(owner, 2)) * slab

    loads = [
        pltpu.make_async_copy(source, target, ls.at[n])
        for n, (source, target) in enumerate(
            [
                (tokens_hbm, tokens),
                (g_ffn_hbm, g_ffn),
                (w_own_hbm, w_out.at[here]),
                (up_hbm, up),
                (down_hbm, down),
                (g_final_hbm, g_final),
                (kv_hbm, w_kv),
                (w_cross_hbm, w_cross),
                (targets_hbm.at[rows_at(slab_start(me), slab, slab)], mine),
            ]
            + [
                (w_all_hbm.at[lax.rem(here + k, sides)], w_out.at[lax.rem(here + k, sides)])
                for k in range(1, sides)
            ]
        )
    ]
    for load in loads:
        load.start()

    def place(side, origin):
        return context.at[lax.rem(origin, share), side * heads + lax.div(origin, share)]

    own = pltpu.make_async_copy(x_in.at[me], place(here, me), ls.at[len(loads)])
    own.start()
    greet_all(ring, sides)

    def outgoing(i):
        to = flip(me, i, ring)
        return seq_copy(to, x_in.at[to], place(here, me), ss.at[i], rs.at[i])

    def relay(i, k):
        block = place(here, flip(me, i, ring))
        return side_copy(sides, k, block, block, fs.at[i, k], fr.at[i, k])

    def send(i, carry):
        outgoing(i).start()
        return carry

    lax.fori_loop(1, ring, send, 0)
    own.wait()
    for k in range(1, sides):
        relay(0, k).start()

    def pass_on(i, carry):
        origin = flip(me, i, ring)
        seq_copy(origin, x_in.at[0], place(here, origin), ss.at[i], rs.at[i]).wait_recv()
        for k in range(1, sides):
            relay(i, k).start()
        return carry

    lax.fori_loop(1, ring, pass_on, 0)

    def sent(i, carry):
        outgoing(i).wait_send()
        return carry

    lax.fori_loop(1, ring, sent, 0)

    def drain(i, carry):
        for k in range(1, sides):
            relay(i, k).wait_send()
            block = place(lax.rem(here - k + sides, sides), flip(me, i, ring))
            side_copy(sides, k, block, block, fs.at[i, k], fr.at[i, k]).wait_recv()
        return carry

    lax.fori_loop(0, ring, drain, 0)
    for load in loads[:3] + loads[9:]:
        load.wait()
    part = rows // share

    chunk = math.gcd(rows, 128)
    chunks = rows // chunk
    unit = math.gcd(part, chunk)

    def project(u):
        at = rows_at(u * unit, unit, unit)
        block = context.at[lax.div(u * unit, part)]
        if unit < part:
            block = block.at[:, :, rows_at(lax.rem(u * unit, part), unit, unit)]
        total = tokens[at, :].astype(jnp.float32) + lax.dot_general(
            block[...].reshape(sides * heads * HD, unit),
            w_out[...].reshape(sides * heads * HD, width), (((0,), (0,)), ((), ())),
            preferred_element_type=jnp.float32,
        )
        hidden[at, :] = total
        normed[at, :] = norm_rows(total, g_ffn[...]).astype(jnp.bfloat16)

    for load in loads[3:6]:
        load.wait()

    def span(c):
        return rows_at(c * chunk, chunk, chunk)

    def swap(c, k, side):
        return side_copy(
            sides, k, parts.at[side, span(c)], parts.at[side, span(c)], ps.at[c, k], pr.at[c, k]
        )

    def feed(c, carry):
        for n in range(chunk // unit):
            project(c * (chunk // unit) + n)
        x = normed[span(c), :]
        gate = jnp.dot(x, up[0], preferred_element_type=jnp.float32)
        lift = jnp.dot(x, up[1], preferred_element_type=jnp.float32)
        active = (jax.nn.gelu(gate, approximate=True) * lift).astype(jnp.bfloat16)
        parts[here, span(c), :] = jnp.dot(
            active, down[...], preferred_element_type=jnp.float32
        ).astype(jnp.bfloat16)
        for k in range(1, sides):
            swap(c, k, here).start()
        return carry

    lax.fori_loop(0, chunks, feed, 0)
    for load in loads[6:9]:
        load.wait()

    def pair_up(c, slot):
        return (
            seq_copy(mate, cross_k.at[slot, span(c)], cross_k.at[slot, span(c)], cs.at[c, 0], cr.at[c, 0]),
            seq_copy(mate, cross_v.at[slot, span(c)], cross_v.at[slot, span(c)], cs.at[c, 1], cr.at[c, 1]),
        )

    def close(c, carry):
        for k in range(1, sides):
            swap(c, k, here).wait_send()
            swap(c, k, lax.rem(here - k + sides, sides)).wait_recv()
        total = hidden[span(c), :]
        for side in range(sides):
            total = total + parts[side, span(c), :].astype(jnp.float32)
        done = norm_rows(total, g_final[...]).astype(jnp.bfloat16)
        encoded[span(c), :] = done
        cross_k[core, span(c), :] = jnp.dot(
            done, w_kv[0], preferred_element_type=jnp.float32
        ).astype(jnp.bfloat16)
        cross_v[core, span(c), :] = jnp.dot(
            done, w_kv[1], preferred_element_type=jnp.float32
        ).astype(jnp.bfloat16)
        for copy in pair_up(c, core):
            copy.start()
        return carry

    lax.fori_loop(0, chunks, close, 0)

    def paired(c, carry):
        for copy in pair_up(c, core):
            copy.wait_send()
        for copy in pair_up(c, 1 - core):
            copy.wait_recv()
        return carry

    lax.fori_loop(0, chunks, paired, 0)
    half = cross_q.shape[0]
    pairs = heads // 2
    peers = ring // 2
    position = lax.broadcasted_iota(jnp.int32, (2 * rows, 2 * HD), 0)
    first = me - core
    limit = jnp.where(position < rows, pad_lengths[first], rows + pad_lengths[first + 1])
    dead = jnp.where(position < limit, 0.0, masked_score).astype(jnp.bfloat16)
    lane = lax.broadcasted_iota(jnp.int32, (2 * rows, 2 * HD), 1)
    out_lane = lax.broadcasted_iota(jnp.int32, (half, 2 * HD), 1)
    ones = jnp.ones((2 * rows, 2 * HD), jnp.bfloat16)
    stats[...] = jnp.where(out_lane < HD, 0.0, jnp.where(out_lane < HD + heads, 1.0, 0.0))

    def to_peer(i, j):
        to = flip(me, 2 * j, ring)
        source = mixed.at[i, rows_at(lax.div(to, 2) * slab, slab, slab)]
        return seq_copy(to, source, got.at[j, i], ms.at[j, i], mr.at[j, i])

    def to_peers(i):
        def send_one(j, carry):
            to_peer(i, peers - j).start()
            return carry

        lax.fori_loop(1, peers, send_one, 0)

    def score(i, h):
        cut = rows_at(i * 2 * HD, 2 * HD, 2 * HD)
        keys = cross_k[:, :, cut].reshape(2 * rows, 2 * HD)
        keys = jnp.where(lane < HD if h == 0 else lane >= HD, keys, dead)
        pick = jnp.where(out_lane == (HD if h == 0 else 0), 1.0, 0.0).astype(jnp.bfloat16)
        queries = jnp.where(out_lane < HD if h == 0 else out_lane >= HD, cross_q[:, cut], pick)
        return lax.dot_general(
            queries, keys, (((1,), (1,)), ((), ())), preferred_element_type=jnp.float32
        )

    def hold(h, scores):
        held[h] = scores
        tops[h] = jnp.max(scores, axis=1, keepdims=True)

    for h in range(2):
        hold(h, score(0, h))

    def cross_pair(i, carry):
        following = [score(lax.rem(i + 1, pairs), h) for h in range(2)]
        v_here = cross_v[:, :, rows_at(i * 2 * HD, 2 * HD, 2 * HD)].reshape(2 * rows, 2 * HD)
        pieces = []
        seen = stats[...]
        for h in range(2):
            values = jnp.where(lane < HD if h == 0 else lane >= HD, v_here, ones)
            top = tops[h]
            weights = jnp.exp2(held[h] - top).astype(jnp.bfloat16)
            piece = jnp.dot(weights, values, preferred_element_type=jnp.float32)
            total = piece[:, 2 * HD - 1 :] if h == 0 else piece[:, :1]
            seen = jnp.where(
                out_lane == 2 * i + h, top, jnp.where(out_lane == HD + 2 * i + h, total, seen)
            )
            pieces.append(piece)
            hold(h, following[h])
        stats[...] = seen
        mixed[i] = jnp.where(out_lane < HD, pieces[0], pieces[1]).astype(jnp.bfloat16)
        to_peers(i)
        return carry

    lax.fori_loop(0, pairs, cross_pair, 0)
    seen = stats[...]
    high = seen.astype(jnp.bfloat16).astype(jnp.float32)
    rest = seen - high
    middle = rest.astype(jnp.bfloat16).astype(jnp.float32)
    mixed[pairs] = (
        high + pltpu.roll(middle, heads, 1) + pltpu.roll(rest - middle, 2 * heads, 1)
    ).astype(jnp.bfloat16)
    to_peers(pairs)
    got[0] = mixed[:, rows_at(lax.div(me, 2) * slab, slab, slab), :]

    def collect(j, carry):
        for i in range(pairs + 1):
            copy = to_peer(i, j)
            copy.wait_send()
            copy.wait_recv()
        return carry

    lax.fori_loop(1, peers, collect, 0)
    packed = got[:, pairs].astype(jnp.float32).reshape(peers * slab, 2 * HD)
    seen = packed + pltpu.roll(packed, 2 * HD - heads, 1) + pltpu.roll(packed, 2 * HD - 2 * heads, 1)
    sums = pltpu.roll(seen, HD, 1).reshape(peers, slab, 2 * HD)
    seen = seen.reshape(peers, slab, 2 * HD)
    best = jnp.max(seen, axis=0, keepdims=True)
    grow = jnp.exp2(seen - best)
    weight_sum = jnp.sum(grow * sums, axis=0, keepdims=True)
    factor = (grow / weight_sum).reshape(peers * slab, 2 * HD)
    factor = jnp.where(lax.broadcasted_iota(jnp.int32, factor.shape, 1) < heads, factor, 0.0)
    column = lax.broadcasted_iota(jnp.int32, (2 * HD, heads * HD), 1)
    row = lax.broadcasted_iota(jnp.int32, (2 * HD, heads * HD), 0)
    spread = jnp.where((column >= row * HD) & (column < row * HD + HD), 1.0, 0.0)
    spread = spread.astype(jnp.bfloat16)
    high = factor.astype(jnp.bfloat16)
    low = (factor - high.astype(jnp.float32)).astype(jnp.bfloat16)
    wide = jnp.dot(
        jnp.concatenate([high, low], axis=1), jnp.concatenate([spread, spread], axis=0),
        preferred_element_type=jnp.float32,
    ).reshape(peers, slab, heads * HD)
    merged = []
    for i in range(pairs):
        weighed = got[:, i].astype(jnp.float32) * wide[:, :, i * 2 * HD : (i + 1) * 2 * HD]
        merged.append(jnp.sum(weighed, axis=0).astype(jnp.bfloat16))
    product = jnp.dot(
        jnp.concatenate(merged, axis=1), w_cross[...], preferred_element_type=jnp.float32
    )
    partial[...] = product.astype(jnp.bfloat16)
    piece = incoming.shape[1]
    divided = piece < slab

    def piece_of(side):
        return rows_at(side * piece, piece, piece) if divided else pl.ds(0, piece)

    def exchange(k, side, origin):
        return side_copy(
            sides, k, partial.at[piece_of(side)], incoming.at[origin], xs.at[k], xr.at[k]
        )

    for k in range(1, sides):
        exchange(k, lax.rem(here + k, sides), here).start()
    incoming[here] = partial[piece_of(here), :]
    for k in range(1, sides):
        exchange(k, lax.rem(here + k, sides), here).wait_send()
        exchange(k, here, lax.rem(here - k + sides, sides)).wait_recv()
    total = incoming[0].astype(jnp.float32)
    for side in range(1, sides):
        total = total + incoming[side].astype(jnp.float32)

    def piece_start(owner, side):
        return slab_start(owner) + (side * piece if divided else 0)

    slot = piece_start(me, here) + lax.broadcasted_iota(jnp.int32, (piece, width), 0)
    limit = jnp.zeros((piece, width), jnp.int32)
    for n in range(target_lengths.shape[0]):
        begun = n * TGT_LEN
        limit = jnp.where(slot >= begun, begun + target_lengths[n], limit)
    decoded[rows_at(piece_start(me, here), piece, piece), :] = (
        mine[piece_of(here), :].astype(jnp.float32) + jnp.where(slot < limit, total, 0.0)
    ).astype(jnp.bfloat16)

    def block(owner, side):
        return decoded.at[rows_at(piece_start(owner, side), piece, piece)]

    def near(n):
        return flip(me, 2 * n, ring)

    def to_near(n, owner):
        return seq_copy(near(n), block(owner, here), block(owner, here), zs.at[n], zr.at[n])

    def to_side(k, n, side):
        return side_copy(
            sides, k, block(near(n), side), block(near(n), side), ws.at[k, n], wr.at[k, n]
        )

    def to_mate(k, n, owner):
        side = lax.rem(here - k + sides, sides)
        source = block(flip(owner, 2 * n, ring), side)
        return seq_copy(mate, source, source, hs.at[k, n], hr.at[k, n])

    given = range(1, sides) if divided else ()

    def share_out(n, carry):
        to_near(n, me).start()
        return carry

    lax.fori_loop(1, peers, share_out, 0)

    def pass_block(n):
        for k in given:
            to_side(k, n, here).start()
        to_mate(0, n, me).start()

    pass_block(0)

    def pass_along(n, carry):
        to_near(n, near(n)).wait_recv()
        pass_block(n)
        return carry

    lax.fori_loop(1, peers, pass_along, 0)

    def across(n, carry):
        for k in given:
            to_side(k, n, lax.rem(here - k + sides, sides)).wait_recv()
            to_mate(k, n, me).start()
        return carry

    lax.fori_loop(0, peers, across, 0)
    def spent(n, carry):
        to_near(n, me).wait_send()
        return carry

    lax.fori_loop(1, peers, spent, 0)

    def settle(n, carry):
        for k in given:
            to_side(k, n, here).wait_send()
        for k in (0, *given):
            to_mate(k, n, me).wait_send()
            to_mate(k, n, mate).wait_recv()
        return carry

    lax.fori_loop(0, peers, settle, 0)


def encoder_block(
    ring, share, sides, back, pad_lengths, target_lengths, tokens, g_ffn, g_final, w_own, w_all,
    ffn_in, ffn_out, w_kv, cross_q, w_cross, targets,
):
    rows, width = tokens.shape
    heads = ring // share
    chunks = rows // math.gcd(rows, 128)
    slab = targets.shape[0] // ring
    piece = slab // sides if slab % (16 * sides) == 0 else slab
    half, lanes = cross_q.shape
    pairs = heads // 2
    peers = ring // 2
    bf16 = jnp.bfloat16
    vmem = pl.BlockSpec(memory_space=pltpu.VMEM)
    smem = pl.BlockSpec(memory_space=pltpu.SMEM)
    hbm = pl.BlockSpec(memory_space=pltpu.HBM)
    dma = pltpu.SemaphoreType.DMA
    return pl.pallas_call(
        functools.partial(block_kernel, ring, share, sides),
        out_shape=(
            jax.ShapeDtypeStruct((rows, width), bf16),
            jax.ShapeDtypeStruct(targets.shape, bf16),
        ),
        in_specs=[vmem, smem, smem] + [hbm] * 8 + [vmem, hbm, hbm],
        out_specs=(vmem, vmem),
        scratch_shapes=[
            pltpu.VMEM((rows, width), bf16),
            pltpu.VMEM((1, width), jnp.float32),
            pltpu.VMEM((1, width), jnp.float32),
            pltpu.VMEM((sides,) + w_own.shape, bf16),
            pltpu.VMEM((share, sides * heads, HD, rows // share), bf16),
            pltpu.VMEM((rows, width), jnp.float32),
            pltpu.VMEM((rows, width), bf16),
            pltpu.VMEM((sides, rows, width), bf16),
            pltpu.VMEM(ffn_in.shape, bf16),
            pltpu.VMEM(ffn_out.shape, bf16),
            pltpu.VMEM(w_kv.shape, bf16),
            pltpu.VMEM(w_cross.shape, bf16),
            pltpu.VMEM((slab, width), bf16),
            pltpu.VMEM((2, rows, lanes), bf16),
            pltpu.VMEM((2, rows, lanes), bf16),
            pltpu.VMEM((2, half, 2 * rows), jnp.float32),
            pltpu.VMEM((2, half, 1), jnp.float32),
            pltpu.VMEM((pairs + 1, half, 2 * HD), bf16),
            pltpu.VMEM((half, 2 * HD), jnp.float32),
            pltpu.VMEM((peers, pairs + 1, slab, 2 * HD), bf16),
            pltpu.VMEM((slab, width), bf16),
            pltpu.VMEM((sides, piece, width), bf16),
            dma((9 + sides,)),
            dma((ring,)),
            dma((ring,)),
            dma((ring, sides)),
            dma((ring, sides)),
            dma((chunks, sides)),
            dma((chunks, sides)),
            dma((chunks, 2)),
            dma((chunks, 2)),
            dma((peers, pairs + 1)),
            dma((peers, pairs + 1)),
            dma((sides,)),
            dma((sides,)),
            dma((peers,)),
            dma((peers,)),
            dma((sides, peers)),
            dma((sides, peers)),
            dma((sides, peers)),
            dma((sides, peers)),
        ],
        compiler_params=pltpu.CompilerParams(
            collective_id=1, has_side_effects=True, vmem_limit_bytes=50 * 1024 * 1024
        ),
        name="encoder_block",
    )(
        back, pad_lengths, target_lengths, tokens, g_ffn[None, :], g_final[None, :], w_own, w_all,
        ffn_in, ffn_out, w_kv, cross_q, w_cross, targets,
    )


def attend_kernel(
    lengths, q_ref, kv_ref, o_ref, keys, values, flipped, count, held, tops, reach, mixed
):
    blocks, span, lanes = kv_ref.shape
    tile = span
    queries = q_ref.shape[1]
    group = math.gcd(queries, 256)
    ones_rows = flipped.shape[1] - HD
    lane = lax.broadcasted_iota(jnp.int32, (span, lanes), 1)
    row = lax.broadcasted_iota(jnp.int32, (span, lanes), 0)

    @pl.when(pl.program_id(0) == 0)
    def pack():
        def place(j, start):
            block = kv_ref[j]
            dead = jnp.where(row < lengths[j], 0.0, masked_score).astype(jnp.bfloat16)
            at = pl.ds(pl.multiple_of(start, 16), span)
            keys[at, :] = jnp.where(lane < HD, block, dead)
            values[at, :] = jnp.where(lane < HD, jnp.ones_like(block), block)
            return start + ((lengths[j] + 15) // 16) * 16

        stop = lax.fori_loop(0, blocks, place, 0)
        at = pl.ds(pl.multiple_of(stop, 16), span)
        keys[at, :] = jnp.where(lane < HD, 0.0, masked_score).astype(jnp.bfloat16)
        values[at, :] = jnp.zeros((span, lanes), jnp.bfloat16)
        count[0] = (stop + tile - 1) // tile

        def flip(t, carry):
            at = pl.ds(pl.multiple_of(t * tile, tile), tile)
            flipped[t] = values[at, :].T[HD - ones_rows :, :]
            return carry

        lax.fori_loop(0, count[0], flip, 0)

    spare = lax.broadcasted_iota(jnp.int32, (HD, queries), 0)
    pick = jnp.where(spare == 0, 1.0, 0.0).astype(jnp.bfloat16)
    q_wide = jnp.concatenate([q_ref[...], pick], axis=0)
    cuts = [slice(g, g + group) for g in range(0, queries, group)]

    def score(t, cut):
        at = pl.ds(pl.multiple_of(t * tile, tile), tile)
        return jnp.dot(keys[at, :], q_wide[:, cut], preferred_element_type=jnp.float32)

    def hold(n, scores):
        held[n] = scores
        tops[n] = jnp.max(scores, axis=0, keepdims=True)

    for n, cut in enumerate(cuts):
        hold(n, score(0, cut))
        reach[n] = jnp.full((1, group), masked_score, jnp.float32)
        mixed[n] = jnp.zeros((ones_rows + HD, group), jnp.float32)

    def step(t, carry):
        values_here = flipped[t]
        for n, cut in enumerate(cuts):
            following = score(t + 1, cut)
            top = jnp.maximum(reach[n], tops[n])
            weights = jnp.exp2(held[n] - top).astype(jnp.bfloat16)
            mixed[n] = mixed[n] * jnp.exp2(reach[n] - top) + jnp.dot(
                values_here, weights, preferred_element_type=jnp.float32
            )
            reach[n] = top
            hold(n, following)
        return carry

    lax.fori_loop(0, count[0], step, 0)
    for n, cut in enumerate(cuts):
        o_ref[:, cut] = (mixed[n, ones_rows:, :] / mixed[n, 0:1, :]).astype(jnp.bfloat16)


def attend(q_all, kv_all, pad_lengths):
    blocks, span, lanes = kv_all.shape
    total = q_all.shape[1]
    width = math.gcd(total, 4096)
    group = math.gcd(width, 256)
    groups = width // group
    return pl.pallas_call(
        attend_kernel,
        out_shape=jax.ShapeDtypeStruct((HD, total), jnp.bfloat16),
        grid_spec=pltpu.PrefetchScalarGridSpec(
            num_scalar_prefetch=1,
            grid=(total // width,),
            in_specs=[
                pl.BlockSpec((HD, width), lambda i, lengths: (0, i)),
                pl.BlockSpec((blocks, span, lanes), lambda i, lengths: (0, 0, 0)),
            ],
            out_specs=pl.BlockSpec((HD, width), lambda i, lengths: (0, i)),
            scratch_shapes=[
                pltpu.VMEM(((blocks + 1) * span, lanes), jnp.bfloat16),
                pltpu.VMEM(((blocks + 1) * span, lanes), jnp.bfloat16),
                pltpu.VMEM((blocks + 1, HD + 16, span), jnp.bfloat16),
                pltpu.SMEM((1,), jnp.int32),
                pltpu.VMEM((groups, span, group), jnp.float32),
                pltpu.VMEM((groups, 1, group), jnp.float32),
                pltpu.VMEM((groups, 1, group), jnp.float32),
                pltpu.VMEM((groups, HD + 16, group), jnp.float32),
            ],
        ),
        compiler_params=pltpu.CompilerParams(
            dimension_semantics=("arbitrary",), vmem_limit_bytes=32 * 1024 * 1024
        ),
        name="attend",
    )(pad_lengths, q_all, kv_all)


def local(
    ring,
    sides,
    tokens,
    norm_attn,
    self_qkv,
    self_out,
    norm_ffn,
    ffn_in,
    ffn_out,
    norm_final,
    pad_lengths,
    targets,
    target_lengths,
    norm_cross,
    cross_query,
    cross_kv,
    cross_out,
):
    heads_here = self_qkv.shape[2] // HD
    share = ring // heads_here
    part = tokens.shape[0] // share
    q_got, kv_got, out_all, cross_q = scatter_heads(
        ring, share, sides, tokens, norm_attn, self_qkv, self_out, targets, norm_cross, cross_query
    )
    q_all = q_got.transpose(1, 0, 2).reshape(HD, ring * part)
    mixed_t = attend(q_all, kv_got, pad_lengths)
    back = mixed_t.reshape(HD, ring, part).transpose(1, 0, 2)
    return encoder_block(
        ring,
        share,
        sides,
        back,
        pad_lengths,
        target_lengths,
        tokens,
        norm_ffn,
        norm_final,
        self_out,
        out_all,
        ffn_in,
        ffn_out,
        cross_kv,
        cross_q,
        cross_out,
        targets,
    )


def solution(mesh):
    ring = mesh.shape["seq"]
    sides = mesh.shape["head"]
    placed = (
        P("seq", None),
        P(),
        P(None, None, "head"),
        P("head", None),
        P(),
        P(None, None, "head"),
        P("head", None),
        P(),
        P(),
        P(),
        P(),
        P(),
        P(None, "head"),
        P(None, None, "head"),
        P("head", None),
    )
    return jax.shard_map(
        functools.partial(local, ring, sides),
        mesh=mesh,
        in_specs=placed,
        out_specs=(P("seq", None), P()),
        check_vma=False,
    )
```
